32 devices in a mesh: fsdp: 2 (over core), ctx: 4 (over y, x), tensor: 4 (over z).
Axes of the slice: x: 2, y: 2, z: 4, core: 2. Of those that a mesh axis runs over, the one named last changes fastest.
Arguments:
- tokens: bfloat16 [4, 1024, 2048], P('fsdp', ('ctx', 'tensor')), may hold values from -6 to 6
- segments: int32 [4, 1024], P('fsdp'), may hold values from 0 to 6, as said below
- positions: int32 [4, 1024], P('fsdp'), may hold values from 0 to 1226, as said below
- query_weight: bfloat16 [2048, 2048], P(('fsdp', 'ctx'), 'tensor'), may hold values from -0.125 to 0.125
- key_weight: bfloat16 [2048, 2048], P(('fsdp', 'ctx'), 'tensor'), may hold values from -0.125 to 0.125
- value_weight: bfloat16 [2048, 2048], P(('fsdp', 'ctx'), 'tensor'), may hold values from -0.125 to 0.125
- output_weight: bfloat16 [2048, 2048], P(('fsdp', 'ctx'), 'tensor'), may hold values from -0.125 to 0.125
- gate_weight: bfloat16 [2048, 8192], P(('fsdp', 'ctx'), 'tensor'), may hold values from -0.125 to 0.125
- up_projection_weight: bfloat16 [2048, 8192], P(('fsdp', 'ctx'), 'tensor'), may hold values from -0.125 to 0.125
- down_weight: bfloat16 [2048, 8192], P(('fsdp', 'ctx'), 'tensor'), may hold values from -0.0625 to 0.0625
- query_gain: float32 [2048], replicated, may hold values from 0.5 to 1.5
- key_gain: float32 [2048], replicated, may hold values from 0.5 to 1.5
- attention_gain: float32 [2048], replicated, may hold values from 0.5 to 1.5
- feedforward_gain: float32 [2048], replicated, may hold values from 0.5 to 1.5
- cotangent: bfloat16 [4, 1024, 2048], P('fsdp', ('ctx', 'tensor')), may hold values from -6 to 6
Outputs:
- block_out: bfloat16 [4, 1024, 2048], P('fsdp', ('ctx', 'tensor'))
- input_grad: float32 [4, 1024, 2048], P('fsdp', ('ctx', 'tensor'))
- query_weight_grad: float32 [2048, 2048], P(('fsdp', 'ctx'), 'tensor')
- key_weight_grad: float32 [2048, 2048], P(('fsdp', 'ctx'), 'tensor')
- value_weight_grad: float32 [2048, 2048], P(('fsdp', 'ctx'), 'tensor')
- output_weight_grad: float32 [2048, 2048], P(('fsdp', 'ctx'), 'tensor')
- gate_weight_grad: float32 [2048, 8192], P(('fsdp', 'ctx'), 'tensor')
- up_weight_grad: float32 [2048, 8192], P(('fsdp', 'ctx'), 'tensor')
- down_weight_grad: float32 [2048, 8192], P(('fsdp', 'ctx'), 'tensor')
- query_gain_grad: float32 [2048], replicated
- key_gain_grad: float32 [2048], replicated
- attention_gain_grad: float32 [2048], replicated
- feedforward_gain_grad: float32 [2048], replicated
The draws below stay inside these ranges and needn't reach their ends.
Inputs may be any that keep to these rules, and one draw needn't show every extreme that they name: `segments`: in each sequence the numbers start at 0 and rise by one where a new document begins; documents hold a fifth of 1024 (rounded down) to 2047 tokens, and the first may have begun before the sequence. `positions`: each token's index in its document; it rises by one from token to token within a document and is 0 where a document begins inside the sequence.
All inputs are finite; a program needn't handle non-finite values.
Results may differ from the reference program's by a relative error of at most 0.017.
Values may be sent and summed in bfloat16 or wider, within the bound.
A program may use at most 256 MiB of HBM per device.

```python
import jax
import jax.numpy as jnp
from jax import lax

D = 2048
H = 16
HD = 128
FF = 8192
SEQ_LEN = 1024
SEQS = 4


def document_layout(key):
    folded_key = jax.random.fold_in(key, 11)
    length_key, offset_key, first_key, second_key = jax.random.split(folded_key, 4)
    least = SEQ_LEN // 5
    doc_lengths = jax.random.randint(length_key, (SEQS, 8), least, 2 * SEQ_LEN)
    offsets = jax.random.randint(offset_key, (SEQS, 1), 0, least)
    first_row = jax.random.randint(first_key, (), 0, SEQS)
    second_row = (first_row + jax.random.randint(second_key, (), 1, SEQS)) % SEQS
    row_index = jnp.arange(SEQS, dtype=jnp.int32)[:, None]
    column_index = jnp.arange(8, dtype=jnp.int32)[None, :]
    doc_lengths = jnp.where(row_index == first_row, least, doc_lengths)
    doc_lengths = jnp.where((row_index == second_row) & (column_index == 0), 2 * SEQ_LEN - 1, doc_lengths)
    offsets = jnp.where((row_index == first_row) | (row_index == second_row), least - 1, offsets)
    doc_ends = jnp.cumsum(doc_lengths, axis=1) - offsets
    doc_begins = jnp.concatenate([-offsets, doc_ends[:, :-1]], axis=1)
    token_index = jnp.arange(SEQ_LEN, dtype=jnp.int32)
    seg_ids = jnp.sum((token_index[None, :, None] >= doc_ends[:, None, :]).astype(jnp.int32), axis=2)
    onehot = (seg_ids[:, :, None] == jnp.arange(8, dtype=jnp.int32)[None, None, :]).astype(jnp.int32)
    begin_tok = jnp.sum(onehot * doc_begins[:, None, :], axis=2)
    return (seg_ids.astype(jnp.int32), (token_index[None, :] - begin_tok).astype(jnp.int32))


def draw_segments(key, part):
    return document_layout(key)[0]


def draw_positions(key, part):
    return document_layout(key)[1]


def gain_values(folded_key):
    return jax.random.uniform(folded_key, (D,), jnp.float32, 0.5, 1.5)


def draw_query_gain(key, part):
    return gain_values(jax.random.fold_in(key, 21))


def draw_key_gain(key, part):
    return gain_values(jax.random.fold_in(key, 22))


def shard_levels(rng, extent, cuts, smallest, largest):
    gain, own = 1.0, jax.random.fold_in(rng, 6)
    for axis_at, parts in cuts:
        draws = jnp.exp(jax.random.uniform(jax.random.fold_in(own, axis_at), (parts,), jnp.float32, smallest / len(cuts), largest / len(cuts)))
        gain = gain * jnp.repeat(draws, extent[axis_at] // parts).reshape([-1 if axis == axis_at else 1 for axis in range(len(extent))])
    return gain


def centred(own_key, extent, scale, most, cuts=(), held_as=jnp.bfloat16):
    values = jax.random.normal(own_key, extent, jnp.float32) * scale
    if len(cuts) > 0:
        values = shard_levels(own_key, extent, cuts, -0.22, 0.18) * values
    return jnp.clip(values, min=-most, max=most).astype(held_as)


def setup_inputs(seed: int = 0) -> dict:
    streams_of = jax.random.split(jax.random.key(seed), 16)
    return {
        "tokens": centred(streams_of[0], (SEQS, SEQ_LEN, D), 1.0, 6.0, ((0, 2), (1, 16))),
        "segments": draw_segments(jax.random.fold_in(streams_of[15], 71), 0),
        "positions": draw_positions(jax.random.fold_in(streams_of[15], 71), 0),
        "query_weight": centred(streams_of[3], (D, D), D ** -0.5, 0.125, ((0, 8), (1, 4))),
        "key_weight": centred(streams_of[4], (D, D), D ** -0.5, 0.125, ((0, 8), (1, 4))),
        "value_weight": centred(streams_of[5], (D, D), D ** -0.5, 0.125, ((0, 8), (1, 4))),
        "output_weight": centred(streams_of[6], (D, D), D ** -0.5, 0.125, ((0, 8), (1, 4))),
        "gate_weight": centred(streams_of[7], (D, FF), D ** -0.5, 0.125, ((0, 8), (1, 4))),
        "up_projection_weight": centred(streams_of[8], (D, FF), D ** -0.5, 0.125, ((0, 8), (1, 4))),
        "down_weight": centred(streams_of[9], (D, FF), FF ** -0.5, 0.0625, ((0, 8), (1, 4))),
        "query_gain": draw_query_gain(jax.random.fold_in(streams_of[15], 71), 0),
        "key_gain": draw_key_gain(jax.random.fold_in(streams_of[15], 71), 0),
        "attention_gain": jnp.clip(1.0 + 0.1 * jax.random.normal(streams_of[12], (D,), jnp.float32), 0.5, 1.5),
        "feedforward_gain": jnp.clip(1.0 + 0.1 * jax.random.normal(streams_of[13], (D,), jnp.float32), 0.5, 1.5),
        "cotangent": centred(streams_of[14], (SEQS, SEQ_LEN, D), 1.0, 6.0, ((0, 2), (1, 16))),
    }


epsilon = 1e-06
rope_theta = 500000.0
masked_score = -1e+30

def dot_float(left, right):
    return jnp.dot(left, right, preferred_element_type=jnp.float32)

def root_mean_square_scale(values):
    return lax.rsqrt(lax.optimization_barrier(jnp.mean(values * values, axis=-1, keepdims=True)) + epsilon)

def norm_back(grad_unit, unit, scale):
    return scale * (grad_unit - unit * lax.optimization_barrier(jnp.mean(grad_unit * unit, axis=-1, keepdims=True)))

def rope_tables(position_ids):
    freq_index = jnp.arange(HD // 2, dtype=jnp.float32)
    inverse = rope_theta ** (-2.0 * freq_index / HD)
    angles = position_ids.astype(jnp.float32)[..., None] * inverse
    return (jnp.cos(angles), jnp.sin(angles))

def rotate(values, cosine, sine):
    half = values.shape[-1] // 2
    first_half = values[..., :half]
    second_half = values[..., half:]
    cos_wide = cosine[..., None, :]
    sin_wide = sine[..., None, :]
    return jnp.concatenate([first_half * cos_wide - second_half * sin_wide, second_half * cos_wide + first_half * sin_wide], axis=-1)

def unrotate(values, cosine, sine):
    half = values.shape[-1] // 2
    first_half = values[..., :half]
    second_half = values[..., half:]
    cos_wide = cosine[..., None, :]
    sin_wide = sine[..., None, :]
    return jnp.concatenate([first_half * cos_wide + second_half * sin_wide, second_half * cos_wide - first_half * sin_wide], axis=-1)

def reference(tokens, segments, positions, query_weight, key_weight, value_weight, output_weight, gate_weight, up_projection_weight, down_weight, query_gain, key_gain, attention_gain, feedforward_gain, cotangent):
    score_scale = HD ** (-0.5)

    def one_sequence(carry, inputs):
        row_tokens, row_segs, row_pos, row_cot = inputs
        query_lin = dot_float(row_tokens, query_weight)
        key_lin = dot_float(row_tokens, key_weight)
        value_lin = dot_float(row_tokens, value_weight)
        query_scale = root_mean_square_scale(query_lin)
        key_scale = root_mean_square_scale(key_lin)
        query_unit = query_lin * query_scale
        key_unit = key_lin * key_scale
        cosine, sine = rope_tables(row_pos)
        query_rot = rotate((query_unit * query_gain).reshape(SEQ_LEN, H, HD), cosine, sine).astype(jnp.bfloat16)
        key_rot = rotate((key_unit * key_gain).reshape(SEQ_LEN, H, HD), cosine, sine).astype(jnp.bfloat16)
        value_b = value_lin.astype(jnp.bfloat16).reshape(SEQ_LEN, H, HD)
        token_index = jnp.arange(SEQ_LEN, dtype=jnp.int32)
        allowed = (row_segs[:, None] == row_segs[None, :]) & (token_index[:, None] >= token_index[None, :])
        raw_scores = jnp.einsum('qhd,khd->hqk', query_rot.astype(jnp.float32), key_rot.astype(jnp.float32)) * score_scale
        scores = jnp.where(allowed[None], raw_scores, masked_score)
        top_score = lax.optimization_barrier(jnp.max(scores, axis=-1, keepdims=True))
        log_total = top_score + jnp.log(lax.optimization_barrier(jnp.sum(jnp.exp(scores - top_score), axis=-1, keepdims=True)))
        probs_full = jnp.exp(scores - log_total)
        probs_b = probs_full.astype(jnp.bfloat16)
        attended = jnp.einsum('hqk,khd->qhd', probs_b.astype(jnp.float32), value_b.astype(jnp.float32)).astype(jnp.bfloat16)
        attended_flat = attended.reshape(SEQ_LEN, D)
        attention_out = dot_float(attended_flat, output_weight.T)
        attention_scale = root_mean_square_scale(attention_out)
        attention_unit = attention_out * attention_scale
        hidden_state = row_tokens.astype(jnp.float32) + attention_unit * attention_gain
        hidden_b = hidden_state.astype(jnp.bfloat16)
        gate_lin = dot_float(hidden_b, gate_weight)
        up_lin = dot_float(hidden_b, up_projection_weight)
        gate_sig = jax.nn.sigmoid(gate_lin)
        gate_act = gate_lin * gate_sig
        mixed = (gate_act * up_lin).astype(jnp.bfloat16)
        mixed_out = dot_float(mixed, down_weight.T)
        mixed_scale = root_mean_square_scale(mixed_out)
        mixed_unit = mixed_out * mixed_scale
        block_row = (hidden_state + mixed_unit * feedforward_gain).astype(jnp.bfloat16)
        upstream = row_cot.astype(jnp.float32)
        ffn_gain_grad = lax.optimization_barrier(jnp.sum(upstream * mixed_unit, axis=0))
        mixed_grad = norm_back(upstream * feedforward_gain, mixed_unit, mixed_scale).astype(jnp.bfloat16)
        down_grad = dot_float(mixed_grad.T, mixed)
        inner_grad = dot_float(mixed_grad, down_weight)
        gate_lin_grad = (inner_grad * up_lin * gate_sig * (1.0 + gate_lin * (1.0 - gate_sig))).astype(jnp.bfloat16)
        up_lin_grad = (inner_grad * gate_act).astype(jnp.bfloat16)
        gate_grad = dot_float(hidden_b.T, gate_lin_grad)
        up_grad = dot_float(hidden_b.T, up_lin_grad)
        hidden_grad = upstream + dot_float(gate_lin_grad, gate_weight.T) + dot_float(up_lin_grad, up_projection_weight.T)
        attn_gain_grad = lax.optimization_barrier(jnp.sum(hidden_grad * attention_unit, axis=0))
        attention_grad = norm_back(hidden_grad * attention_gain, attention_unit, attention_scale).astype(jnp.bfloat16)
        output_grad = dot_float(attention_grad.T, attended_flat)
        attended_output_gradient = dot_float(attention_grad, output_weight).astype(jnp.bfloat16).reshape(SEQ_LEN, H, HD)
        value_grad = jnp.einsum('hqk,qhd->khd', probs_b.astype(jnp.float32), attended_output_gradient.astype(jnp.float32)).astype(jnp.bfloat16)
        prob_grad = jnp.einsum('qhd,khd->hqk', attended_output_gradient.astype(jnp.float32), value_b.astype(jnp.float32))
        delta_rows = jnp.einsum('qhd,qhd->hq', attended_output_gradient.astype(jnp.float32), attended.astype(jnp.float32))
        score_grad = (probs_full * (prob_grad - delta_rows[..., None])).astype(jnp.bfloat16)
        query_grad = (jnp.einsum('hqk,khd->qhd', score_grad.astype(jnp.float32), key_rot.astype(jnp.float32)) * score_scale).astype(jnp.bfloat16)
        key_grad = (jnp.einsum('hqk,qhd->khd', score_grad.astype(jnp.float32), query_rot.astype(jnp.float32)) * score_scale).astype(jnp.bfloat16)
        query_grad_n = unrotate(query_grad.astype(jnp.float32), cosine, sine).reshape(SEQ_LEN, D)
        key_grad_n = unrotate(key_grad.astype(jnp.float32), cosine, sine).reshape(SEQ_LEN, D)
        q_gain_grad = lax.optimization_barrier(jnp.sum(query_grad_n * query_unit, axis=0))
        k_gain_grad = lax.optimization_barrier(jnp.sum(key_grad_n * key_unit, axis=0))
        query_pre = norm_back(query_grad_n * query_gain, query_unit, query_scale).astype(jnp.bfloat16)
        key_pre = norm_back(key_grad_n * key_gain, key_unit, key_scale).astype(jnp.bfloat16)
        value_pre = value_grad.reshape(SEQ_LEN, D)
        input_row = hidden_grad + dot_float(query_pre, query_weight.T) + dot_float(key_pre, key_weight.T) + dot_float(value_pre, value_weight.T)
        query_grad_w = dot_float(row_tokens.T, query_pre)
        key_grad_w = dot_float(row_tokens.T, key_pre)
        value_grad_w = dot_float(row_tokens.T, value_pre)
        terms = (query_grad_w, key_grad_w, value_grad_w, output_grad, gate_grad, up_grad, down_grad, q_gain_grad, k_gain_grad, attn_gain_grad, ffn_gain_grad)
        new_carry = jax.tree.map(lambda total, term: total + term, carry, terms)
        return (new_carry, (block_row, input_row))
    start = (jnp.zeros((D, D), jnp.float32), jnp.zeros((D, D), jnp.float32), jnp.zeros((D, D), jnp.float32), jnp.zeros((D, D), jnp.float32), jnp.zeros((D, FF), jnp.float32), jnp.zeros((D, FF), jnp.float32), jnp.zeros((D, FF), jnp.float32), jnp.zeros((D,), jnp.float32), jnp.zeros((D,), jnp.float32), jnp.zeros((D,), jnp.float32), jnp.zeros((D,), jnp.float32))
    totals, stacked = lax.scan(one_sequence, start, (tokens, segments, positions, cotangent))
    block_out, input_grad = stacked
    return (block_out, input_grad, totals[0], totals[1], totals[2], totals[3], totals[4], totals[5], totals[6], totals[7], totals[8], totals[9], totals[10])
```

```python
import functools

import jax
import jax.numpy as jnp
from jax import lax
from jax.experimental import pallas as pl
from jax.experimental.pallas import tpu as pltpu
from jax.sharding import PartitionSpec as P

D = 2048
HD = 128


epsilon = 1e-06
rope_theta = 500000.0
masked_score = -1e30


def rope_tables(position_ids):
    freq_index = jnp.arange(HD // 2, dtype=jnp.float32)
    inverse = rope_theta ** (-2.0 * freq_index / HD)
    angles = position_ids.astype(jnp.float32)[..., None] * inverse
    return (jnp.cos(angles), jnp.sin(angles))


MESH = pl.DeviceIdType.MESH
BF = jnp.bfloat16
F32 = jnp.float32
VMEM_SPEC = pl.BlockSpec(memory_space=pltpu.VMEM)
HBM_SPEC = pl.BlockSpec(memory_space=pltpu.HBM)
NN = (((1,), (0,)), ((), ()))
NT = (((1,), (1,)), ((), ()))
TN = (((0,), (0,)), ((), ()))


def dot(a, b, dims):
    return lax.dot_general(a, b, dims, preferred_element_type=F32)


def loop(count, step):
    def run(i, carry):
        step(i)
        return carry

    lax.fori_loop(0, count, run, 0)


def cut(i, size):
    return pl.ds(pl.multiple_of(i * size, size), size)


def both(*conds):
    out = True
    for cond in conds:
        if isinstance(cond, bool):
            if not cond:
                return False
        elif isinstance(out, bool):
            out = cond
        else:
            out = jnp.logical_and(out, cond)
    return out


def when(cond, step):
    if isinstance(cond, bool):
        if cond:
            step()
    else:
        pl.when(cond)(step)


class Place:
    def __init__(self, fsdp_size, ctx_size, tensor_size):
        self.nf, self.nc, self.nt = fsdp_size, ctx_size, tensor_size
        self.f = lax.axis_index("fsdp")
        self.c = lax.axis_index("ctx")
        self.t = lax.axis_index("tensor")
        self.p = lax.rem(self.f, 2)
        self.group = self.f - self.p
        self.mate = self.group + 1 - self.p

    def at(self, f=None, c=None, t=None):
        return {
            "fsdp": self.f if f is None else f,
            "ctx": self.c if c is None else c,
            "tensor": self.t if t is None else t,
        }

    def plane(self):
        out = []
        for dg in range(self.nf // 2):
            for dc in (3, 1, 2, 0) if self.nc == 4 else range(self.nc):
                for dp in (0, 1):
                    if dg or dc or dp:
                        out.append((dg, dc, dp))
        return out

    def peer(self, off):
        dg, dc, dp = off
        group = lax.rem(self.group + 2 * dg, self.nf)
        core = self.p + dp - 2 * self.p * dp
        return group + core, core, jnp.bitwise_xor(self.c, dc)

    def barrier(self):
        sem = pltpu.get_barrier_semaphore()

        def signal(**place):
            pl.semaphore_signal(sem, inc=1, device_id=self.at(**place), device_id_type=MESH)

        offs = self.plane()
        for off in offs:
            f, _, c = self.peer(off)
            signal(f=f, c=c)
        for dt in range(1, self.nt):
            for core in range(2):
                signal(f=self.group + core, t=lax.rem(self.t + dt, self.nt))
        pl.semaphore_wait(sem, len(offs) + 2 * (self.nt - 1))


def remote(src, dst, send, recv, device):
    return pltpu.make_async_remote_copy(
        src_ref=src, dst_ref=dst, send_sem=send, recv_sem=recv, device_id=device, device_id_type=MESH
    )


def wait_bytes(ref, sem):
    pltpu.make_async_copy(ref, ref, sem).wait()


class Reduce:
    def __init__(self, e, part, pair, right, left, sems, rows):
        self.e, self.part, self.pair, self.right, self.left, self.rows = e, part, pair, right, left, rows
        self.sems = sems

    def half(self, p):
        n = self.e.nt * self.rows
        return self.part.at[pl.ds(pl.multiple_of(p * n, n), n), :]

    def block(self, b):
        return self.part.at[cut(self.e.p * self.e.nt + b, self.rows), :]

    def _pair(self):
        return remote(
            self.half(1 - self.e.p), self.pair, self.sems.at[0, 0], self.sems.at[1, 0],
            self.e.at(f=self.e.mate),
        )

    def _side(self, b, k, up):
        e = self.e
        buf, row = (self.right, 0) if up else (self.left, 2)
        return remote(
            self.block(b), buf.at[k], self.sems.at[row, 1 + k], self.sems.at[row + 1, 1 + k],
            e.at(t=e.t + 1 if up else e.t - 1),
        )

    def pair_send(self):
        self._pair().start()

    def pair_add(self):
        self._pair().wait_recv()
        mine = self.half(self.e.p)

        def step(i):
            sl = cut(i, self.rows)
            mine[sl, :] = (mine[sl, :].astype(F32) + self.pair[sl, :].astype(F32)).astype(BF)

        loop(self.e.nt, step)

    def slot(self, j):
        e, n = self.e, self.e.nt
        for up in (True, False):
            b = e.t + (n - 2) - j if up else e.t - (n - 2) + j
            near = e.t > 0 if up else e.t < n - 1
            far = e.t < n - 1 if up else e.t > 0
            inside = b <= n - 1 if up else b >= 0
            buf = self.right if up else self.left

            def take(b=b, buf=buf, up=up):
                self._side(b, j, up).wait_recv()

                def add():
                    blk = self.block(b)
                    blk[...] = (blk[...].astype(F32) + buf[j].astype(F32)).astype(BF)

                when(j < n - 2, add)

            when(both(j >= 0, j <= n - 2, near, inside), take)
            when(both(j < n - 2, far, inside), lambda b=b, up=up: self._side(b, j + 1, up).start())

    def result(self, out):
        e, n = self.e, self.e.nt
        out[...] = self.block(e.t)[...].astype(F32)

        def add_right():
            out[...] += self.right[n - 2].astype(F32)

        def add_left():
            out[...] += self.left[n - 2].astype(F32)

        when(e.t > 0, add_right)
        when(e.t < n - 1, add_left)

    def drain(self):
        e, n = self.e, self.e.nt
        self._pair().wait_send()

        def step(i):
            j = i - 1
            for up in (True, False):
                b = e.t + (n - 2) - j if up else e.t - (n - 2) + j
                far = e.t < n - 1 if up else e.t > 0
                inside = b <= n - 1 if up else b >= 0
                when(both(far, inside), lambda b=b, up=up: self._side(b, j + 1, up).wait_send())

        for i in range(n - 1):
            step(i)


class Gather:
    def __init__(self, e, full, sems, rows):
        self.e, self.full, self.sems, self.rows = e, full, sems, rows

    def block(self, p, b):
        return self.full.at[cut(p * self.e.nt + b, self.rows), :]

    def _side(self, b, k, up):
        e = self.e
        row = 0 if up else 2
        ref = self.block(e.p, b)
        return remote(
            ref, ref, self.sems.at[row, k], self.sems.at[row + 1, k],
            e.at(t=e.t + 1 if up else e.t - 1),
        )

    def _pair(self, b, k, incoming):
        e = self.e
        ref = self.block(1 - e.p if incoming else e.p, b)
        return remote(ref, ref, self.sems.at[4, k], self.sems.at[5, k], e.at(f=e.mate))

    def init(self):
        e, n = self.e, self.e.nt
        when(e.t < n - 1, lambda: self._side(e.t, 0, True).start())
        when(e.t > 0, lambda: self._side(e.t, 0, False).start())
        self._pair(e.t, 0, False).start()

    def slot(self, j):
        e, n = self.e, self.e.nt
        for up in (True, False):
            b = e.t - 1 - j if up else e.t + 1 + j
            inside = b >= 0 if up else b <= n - 1
            far = e.t < n - 1 if up else e.t > 0
            k = 1 + j if up else n + j

            def take(b=b, up=up, far=far, k=k):
                self._side(b, j, up).wait_recv()
                when(both(far, j < n - 2), lambda: self._side(b, j + 1, up).start())
                self._pair(b, k, False).start()

            when(both(j >= 0, j <= n - 2, inside), take)

    def _rest(self, step_pair):
        e, n = self.e, self.e.nt
        step_pair(e.t, 0)
        for j in range(n - 1):
            when(e.t - 1 - j >= 0, lambda j=j: step_pair(e.t - 1 - j, 1 + j))
            when(e.t + 1 + j <= n - 1, lambda j=j: step_pair(e.t + 1 + j, n + j))

    def done(self):
        self._rest(lambda b, k: self._pair(b, k, True).wait_recv())

    def drain(self):
        e, n = self.e, self.e.nt
        self._rest(lambda b, k: self._pair(b, k, False).wait_send())
        when(e.t < n - 1, lambda: self._side(e.t, 0, True).wait_send())
        when(e.t > 0, lambda: self._side(e.t, 0, False).wait_send())
        for j in range(n - 2):
            when(
                both(e.t - 1 - j >= 0, e.t < n - 1),
                lambda j=j: self._side(e.t - 1 - j, j + 1, True).wait_send(),
            )
            when(
                both(e.t + 1 + j <= n - 1, e.t > 0),
                lambda j=j: self._side(e.t + 1 + j, j + 1, False).wait_send(),
            )


class Weight:
    def __init__(self, e, shard, full, send, recv):
        self.e, self.shard, self.full, self.send, self.recv = e, shard, full, send, recv
        self.rows, self.half = shard.shape[0], full.shape[1]

    def start(self):
        e = self.e
        dst = self.full.at[cut(e.f * e.nc + e.c, self.rows), :]
        for off in e.plane():
            f, core, c = e.peer(off)
            remote(
                self.shard.at[:, cut(core, self.half)], dst, self.send, self.recv, e.at(f=f, c=c)
            ).start()
        pltpu.make_async_copy(self.shard.at[:, cut(e.p, self.half)], dst, self.recv).start()

    def wait(self):
        wait_bytes(self.full, self.recv)

    def drain(self):
        count = len(self.e.plane()) * self.rows
        wait_bytes(self.full.at[pl.ds(0, count), :], self.send)


def ffn_kernel(
    sizes, seqs, rows,
    att, wo_sh, gate_sh, up_sh, down_sh, tokens, cot, again, fgain,
    block_out, hidden_grad, agh, wo_part, gate_part, up_part, down_part, gains,
    wo_v, g_v, u_v, d_v, part, pair, right, left, hid, mgr, agr, aa, bb, mixed,
    unit1, hid32, scale1, scratch_y, agx,
    wsem, rsem, gsem, xsend, xrecv, osem,
):
    e = Place(*sizes)
    dm = tokens.shape[2]
    half = g_v.shape[1]
    wide = att.shape[2]
    heads = wide // HD
    weights = [
        Weight(e, sh, full, wsem.at[i, 0], wsem.at[i, 1])
        for i, (sh, full) in enumerate(
            ((wo_sh, wo_v), (gate_sh, g_v), (up_sh, u_v), (down_sh, d_v))
        )
    ]
    w_o, w_g, w_u, w_d = weights

    def reduce(k, s):
        return Reduce(e, part.at[s], pair.at[s], right.at[s], left.at[s], rsem.at[k, s], rows)

    def gather(k, s):
        return Gather(e, (hid, mgr, agr)[k].at[s], gsem.at[k, s], rows)

    red = [[reduce(k, s) for s in range(seqs)] for k in range(3)]
    gat = [[gather(k, s) for s in range(seqs)] for k in range(3)]

    e.barrier()
    for w in weights:
        w.start()
    gains[...] = jnp.zeros_like(gains)

    tile = 512

    def out_tiles(s):
        def step(i):
            sl = cut(i, tile)
            part[s, :, sl] = dot(att[s], wo_v[sl, :], NT).astype(BF)

        loop(dm // tile, step)

    def norm1(s):
        y = scratch_y
        red[0][s].result(y)
        v = y[...]
        scale = lax.rsqrt(jnp.mean(v * v, axis=-1, keepdims=True) + epsilon)
        unit = v * scale
        unit1[s] = unit
        scale1[s] = jnp.broadcast_to(scale, scale1.shape[1:])
        h = tokens[s].astype(F32) + unit * again[...]
        hid32[s] = h
        gat[0][s].block(e.p, e.t)[...] = h.astype(BF)

    def ffn_tile(s, i):
        sl = cut(i, 256)
        gate = dot(hid[s], g_v[:, sl], NN)
        up = dot(hid[s], u_v[:, sl], NN)
        sig = jax.nn.sigmoid(gate)
        act = gate * sig
        mixed[s, :, sl] = (act * up).astype(BF)
        aa[s, :, sl] = (up * sig * (1.0 + gate * (1.0 - sig))).astype(BF)
        bb[s, :, sl] = act.astype(BF)

    ffn_tiles = half // 256

    def down_tiles(s):
        def step(i):
            sl = cut(i, tile)
            part[s, :, sl] = dot(mixed[s], d_v[sl, :], NT).astype(BF)

        loop(dm // tile, step)

    def norm2(s):
        y = scratch_y
        red[1][s].result(y)
        v = y[...]
        scale = lax.rsqrt(jnp.mean(v * v, axis=-1, keepdims=True) + epsilon)
        unit = v * scale
        block_out[s] = (hid32[s] + unit * fgain[...]).astype(BF)
        upstream = cot[s].astype(F32)
        gains[3:4, :] += jnp.sum(upstream * unit, axis=0, keepdims=True)
        g = upstream * fgain[...]
        m = scale * (g - unit * jnp.mean(g * unit, axis=-1, keepdims=True))
        gat[1][s].block(e.p, e.t)[...] = m.astype(BF)

    def inner_tiles(s):
        def step(i):
            sl = cut(i, 256)
            inner = dot(mgr[s], d_v[:, sl], NN)
            aa[s, :, sl] = (inner * aa[s, :, sl].astype(F32)).astype(BF)
            bb[s, :, sl] = (inner * bb[s, :, sl].astype(F32)).astype(BF)

        loop(ffn_tiles, step)

    def back_tiles(s):
        def step(i):
            sl = cut(i, tile)
            part[s, :, sl] = (dot(aa[s], g_v[sl, :], NT) + dot(bb[s], u_v[sl, :], NT)).astype(BF)

        loop(dm // tile, step)

    def norm3(s):
        y = scratch_y
        red[2][s].result(y)
        hg = cot[s].astype(F32) + y[...]
        hidden_grad[s] = hg
        unit = unit1[s]
        gains[2:3, :] += jnp.sum(hg * unit, axis=0, keepdims=True)
        g = hg * again[...]
        scale = scale1[s][:, 0:1]
        a = scale * (g - unit * jnp.mean(g * unit, axis=-1, keepdims=True))
        gat[2][s].block(e.p, e.t)[...] = a.astype(BF)

    def weight_tile(left_rows, right_rows, out, i, width):
        per = out.shape[1] // width
        sl, cl = cut(lax.div(i, per), tile), cut(lax.rem(i, per), width)
        lhs = left_rows[:, :, sl].reshape(-1, tile)
        rhs = right_rows[:, :, cl].reshape(-1, width)
        out[sl, cl] = dot(lhs, rhs, TN).astype(BF)

    n = e.nt
    span = agh.shape[2]

    def heads_copy(s, jj, q):
        src = agx.at[s, jj, pl.ds(q * span, span), :]
        dst = agh.at[s, e.c]
        return src, dst

    def heads_grad(s):
        r = dot(agr[s], wo_v[...], NN).astype(BF)
        for jj in range(heads):
            agx[s, jj] = r[:, jj * HD : (jj + 1) * HD]
        for jj in range(heads):
            head = heads * e.p + jj
            for q in range(2):
                src, dst = heads_copy(s, jj, q)
                self_here = both(head == e.c, q == e.p)

                def local(src=src, dst=dst):
                    pltpu.make_async_copy(src, dst, xrecv.at[s]).start()

                def away(src=src, dst=dst, q=q, head=head, jj=jj):
                    remote(
                        src, dst, xsend.at[s, jj, q], xrecv.at[s], e.at(f=e.group + q, c=head)
                    ).start()

                when(self_here, local)
                when(jnp.logical_not(self_here), away)

    def heads_wait(s):
        wait_bytes(agh.at[s], xrecv.at[s])
        block = agx.at[s, 0, pl.ds(0, span), :]
        for jj in range(heads):
            head = heads * e.p + jj
            for q in range(2):
                when(
                    jnp.logical_not(both(head == e.c, q == e.p)),
                    lambda jj=jj, q=q: wait_bytes(block, xsend.at[s, jj, q]),
                )

    w_o.wait()
    out_tiles(0)
    red[0][0].pair_send()
    out_tiles(1)
    red[0][0].pair_add()
    red[0][1].pair_send()

    def step(i):
        red[0][0].slot(i - 1)

    loop(n, step)
    red[0][1].pair_add()
    norm1(0)
    gat[0][0].init()

    def step(i):
        red[0][1].slot(i - 1)
        gat[0][0].slot(i - 1)

    loop(n, step)
    gat[0][0].done()
    norm1(1)
    gat[0][1].init()
    w_g.wait()
    w_u.wait()

    def step(i):
        ffn_tile(0, i)
        gat[0][1].slot(i)

    loop(ffn_tiles, step)
    w_d.wait()
    red[0][0].drain()
    down_tiles(0)
    red[1][0].pair_send()
    gat[0][1].done()
    ffn_tile(1, 0)
    red[1][0].pair_add()

    def step(i):
        red[1][0].slot(i - 1)
        ffn_tile(1, i + 1)

    loop(ffn_tiles - 1, step)
    for j in range(ffn_tiles - 2, n - 1):
        red[1][0].slot(j)
    norm2(0)
    gat[1][0].init()
    red[0][1].drain()
    down_tiles(1)
    red[1][1].pair_send()
    gat[1][0].slot(0)
    red[1][1].pair_add()

    def step(i):
        red[1][1].slot(i - 1)
        gat[1][0].slot(i + 1)

    loop(n, step)
    norm2(1)
    gat[1][1].init()
    gat[1][0].done()
    inner_tiles(0)
    red[1][0].drain()
    back_tiles(0)
    red[2][0].pair_send()
    gat[1][1].slot(0)
    red[2][0].pair_add()

    def step(i):
        red[2][0].slot(i - 1)
        gat[1][1].slot(i + 1)

    loop(n - 2, step)
    gat[1][1].done()
    inner_tiles(1)
    red[2][0].slot(n - 3)
    red[1][1].drain()
    back_tiles(1)
    red[2][1].pair_send()
    red[2][0].slot(n - 2)
    norm3(0)
    gat[2][0].init()
    red[2][1].pair_add()

    def step(i):
        red[2][1].slot(i - 1)
        gat[2][0].slot(i - 1)

        def fill(k):
            weight_tile(mgr, mixed, d_v, 2 * i + k, tile)
            weight_tile(hid, aa, g_v, 2 * i + k, tile)

        loop(2, fill)

    loop(n, step)
    out_d = pltpu.make_async_copy(d_v, down_part, osem.at[0])
    out_g = pltpu.make_async_copy(g_v, gate_part, osem.at[1])
    out_d.start()
    out_g.start()
    norm3(1)
    gat[2][1].init()
    gat[2][0].done()
    heads_grad(0)

    def step(i):
        gat[2][1].slot(i - 1)
        loop(2, lambda k: weight_tile(hid, bb, u_v, 2 * i + k, tile))

    loop(n, step)
    out_u = pltpu.make_async_copy(u_v, up_part, osem.at[2])
    out_u.start()
    gat[2][1].done()
    heads_grad(1)
    loop(dm // tile, lambda i: weight_tile(agr, att, wo_v, i, wide))
    out_o = pltpu.make_async_copy(wo_v, wo_part, osem.at[3])
    out_o.start()
    heads_wait(0)
    heads_wait(1)
    red[2][0].drain()
    red[2][1].drain()
    for k in range(3):
        for s in range(seqs):
            gat[k][s].drain()
    for w in weights:
        w.drain()
    for o in (out_d, out_g, out_u, out_o):
        o.wait()


def ffn_stage(sizes, att, wo_sh, gate_sh, up_sh, down_sh, tokens, cot, again, fgain):
    nf, nc, nt = sizes
    seqs, rows, dm = tokens.shape
    half = gate_sh.shape[1] // 2
    wide = wo_sh.shape[1] // 2
    full = 2 * nt * rows
    sds = jax.ShapeDtypeStruct
    v, dma = pltpu.VMEM, pltpu.SemaphoreType.DMA
    return pl.pallas_call(
        functools.partial(ffn_kernel, sizes, seqs, rows),
        name="ffn_stage",
        out_shape=(
            sds((seqs, rows, dm), BF),
            sds((seqs, rows, dm), F32),
            sds((seqs, nc, nt * rows, HD), BF),
            sds((dm, wide), BF),
            sds((dm, half), BF),
            sds((dm, half), BF),
            sds((dm, half), BF),
            sds((8, dm), F32),
        ),
        in_specs=[VMEM_SPEC] + [HBM_SPEC] * 4 + [VMEM_SPEC] * 4,
        out_specs=(VMEM_SPEC, VMEM_SPEC) + (HBM_SPEC,) * 5 + (VMEM_SPEC,),
        scratch_shapes=[
            v((dm, wide), BF),
            v((dm, half), BF),
            v((dm, half), BF),
            v((dm, half), BF),
            v((seqs, full, dm), BF),
            v((seqs, nt * rows, dm), BF),
            v((seqs, nt - 1, rows, dm), BF),
            v((seqs, nt - 1, rows, dm), BF),
            v((seqs, full, dm), BF),
            v((seqs, full, dm), BF),
            v((seqs, full, dm), BF),
            v((seqs, full, half), BF),
            v((seqs, full, half), BF),
            v((seqs, full, half), BF),
            v((seqs, rows, dm), F32),
            v((seqs, rows, dm), F32),
            v((seqs, rows, 128), F32),
            v((rows, dm), F32),
            v((seqs, wide // HD, full, HD), BF),
            dma((4, 2)),
            dma((3, seqs, 4, nt)),
            dma((3, seqs, 6, 2 * nt - 1)),
            dma((seqs, wide // HD, 2)),
            dma((seqs,)),
            dma((4,)),
        ],
        compiler_params=pltpu.CompilerParams(
            collective_id=1, has_side_effects=True, vmem_limit_bytes=63 << 20
        ),
    )(att, wo_sh, gate_sh, up_sh, down_sh, tokens, cot, again, fgain)


class Exchange:
    def __init__(self, e, mine, inbox, send, recv, members, own):
        self.e, self.mine, self.inbox, self.send, self.recv = e, mine, inbox, send, recv
        self.members, self.own = members, own

    @staticmethod
    def plane(e):
        out = []
        for f in range(e.nf):
            for c in range(e.nc):
                out.append((f * e.nc + c, e.at(f=f, c=c), both(e.f == f, e.c == c)))
        return out, e.f * e.nc + e.c

    @staticmethod
    def heads(e):
        out = []
        for q in range(2):
            for t in range(e.nt):
                out.append((q * e.nt + t, e.at(f=e.group + q, t=t), both(e.p == q, e.t == t)))
        return out, e.p * e.nt + e.t

    @staticmethod
    def line(e):
        return [(t, e.at(t=t), e.t == t) for t in range(e.nt)], e.t

    def start(self):
        self.inbox[self.own] = self.mine[...]
        for k, device, me in self.members:

            def go(k=k, device=device):
                remote(
                    self.mine, self.inbox.at[self.own], self.send.at[k], self.recv.at[self.own], device
                ).start()

            when(jnp.logical_not(me), go)

    def finish(self):
        for k, device, me in self.members:

            def go(k=k, device=device):
                d = remote(self.mine, self.inbox.at[k], self.send.at[k], self.recv.at[k], device)
                d.wait_recv()
                d.wait_send()

            when(jnp.logical_not(me), go)
        return jnp.sum(self.inbox[...], axis=0)


def to_heads(e, src, dst, send, recv, heads, span):
    for jj in range(heads):
        head = heads * e.p + jj
        for q in range(2):
            piece = src.at[jj, pl.ds(q * span, span), :]
            here = both(head == e.c, q == e.p)
            when(here, lambda piece=piece: pltpu.make_async_copy(piece, dst.at[e.c], recv).start())

            def away(piece=piece, jj=jj, q=q, head=head):
                remote(
                    piece, dst.at[e.c], send.at[jj, q], recv, e.at(f=e.group + q, c=head)
                ).start()

            when(jnp.logical_not(here), away)


def to_heads_drain(e, src, send, heads, span):
    piece = src.at[0, pl.ds(0, span), :]
    for jj in range(heads):
        head = heads * e.p + jj
        for q in range(2):
            here = both(head == e.c, q == e.p)
            when(jnp.logical_not(here), lambda jj=jj, q=q: wait_bytes(piece, send.at[jj, q]))


def from_heads(e, src, dst, send, recv, heads):
    core = lax.div(e.c, heads)
    for c in range(e.nc):
        here = both(e.c == c, core == e.p)
        when(here, lambda c=c: pltpu.make_async_copy(src.at[c], dst, recv).start())

        def away(c=c):
            remote(src.at[c], dst, send.at[c], recv, e.at(f=e.group + core, c=c)).start()

        when(jnp.logical_not(here), away)


def from_heads_drain(e, src, send, heads):
    core = lax.div(e.c, heads)
    for c in range(e.nc):
        here = both(e.c == c, core == e.p)
        when(jnp.logical_not(here), lambda c=c: wait_bytes(src.at[c], send.at[c]))


def columns(first, second):
    lane = lax.broadcasted_iota(jnp.int32, (first.shape[0], 128), 1)
    both_cols = jnp.where(lane == 0, first, jnp.where(lane == 1, second, 0.0))
    return both_cols.T[0:8]


def turn(values, angle_cos, angle_sin):
    return values * angle_cos + pltpu.roll(values, HD // 2, 1) * angle_sin


def turn_back(values, angle_cos, angle_sin):
    return values * angle_cos - pltpu.roll(values, HD // 2, 1) * angle_sin


def masked(scores, seg_col, seg_row, s, i, span):
    keys = scores.shape[1]
    row = lax.broadcasted_iota(jnp.int32, scores.shape, 0) + i * span
    col = lax.broadcasted_iota(jnp.int32, scores.shape, 1)
    same = seg_col[s, pl.ds(i * span, span), :] == seg_row[s, :, pl.ds(0, keys)]
    return jnp.where(jnp.logical_and(same, row >= col), scores, masked_score)


def front_kernel(
    sizes, seqs, rows,
    tokens, cos_own, sin_own, qgain, kgain, seg_col, seg_row, wq_sh, wk_sh, wv_sh,
    att, xs_out, wq_out, wk_out, wv_out, units, scales, angles, qkv_heads, att_heads, lse,
    x, wq, wk, wv, lin, qkvx, qkvh, atth, mine, inbox, wide_t, ang,
    wsem, gsem, asem, esem, hsend, hrecv, bsend, brecv, osem,
):
    e = Place(*sizes)
    n = e.nt
    span = n * rows
    wide = wq.shape[1]
    heads = wide // HD
    ws = [
        Weight(e, sh, full, wsem.at[i, 0], wsem.at[i, 1])
        for i, (sh, full) in enumerate(((wq_sh, wq), (wk_sh, wk), (wv_sh, wv)))
    ]
    gat = [Gather(e, x.at[s], gsem.at[s], rows) for s in range(seqs)]
    own = pl.ds(pl.multiple_of(e.p * span, span), span)

    def angle_copy():
        ref = ang.at[:, :, own, :]
        return remote(ref, ref, asem.at[0], asem.at[1], e.at(f=e.mate))

    e.barrier()
    for s in range(seqs):
        gat[s].block(e.p, e.t)[...] = tokens[s]
        gat[s].init()
    for w in (ws[2], ws[0], ws[1]):
        w.start()
    ang[0, :, own, :] = cos_own[...]
    ang[1, :, own, :] = sin_own[...]
    angle_copy().start()
    wide_t[...] = jnp.zeros_like(wide_t)

    def step(j):
        for s in range(seqs):
            gat[s].slot(j)

    loop(n - 1, step)
    for s in range(seqs):
        gat[s].done()
    outs = [pltpu.make_async_copy(x, xs_out, osem.at[0])]
    outs[0].start()
    ws[2].wait()
    for s in range(seqs):
        r = dot(x[s], wv[...], NN).astype(BF)
        for jj in range(heads):
            qkvx[2, s, jj] = r[:, jj * HD : (jj + 1) * HD]
        to_heads(e, qkvx.at[2, s], qkvh.at[2, s], hsend.at[2, s], hrecv.at[2, s], heads, span)
    ws[0].wait()
    ws[1].wait()
    for k, (w, out) in enumerate(((wq, wq_out), (wk, wk_out), (wv, wv_out))):
        outs.append(pltpu.make_async_copy(w, out, osem.at[1 + k]))
        outs[-1].start()
    sums = [[], []]
    for k, w in enumerate((wq, wk)):
        for s in range(seqs):
            r = dot(x[s], w[...], NN)
            lin[k, s] = r
            sums[k].append(jnp.sum(r * r, axis=-1, keepdims=True))
    mine[...] = columns(*[jnp.concatenate(v, axis=0) for v in sums])
    ex = Exchange(e, mine, inbox, esem.at[0], esem.at[1], *Exchange.heads(e))
    ex.start()
    angle_copy().wait_recv()
    angles[...] = ang[...]
    wide_t[0:8] = lax.rsqrt(ex.finish() / D + epsilon)
    sc = wide_t[...].T
    for s in range(seqs):
        scales[s] = sc[s * 2 * span : (s + 1) * 2 * span]
    place = cut(e.t * 2 + e.p, wide)
    for s in range(seqs):
        for k, gain in enumerate((qgain, kgain)):
            unit = lin[k, s] * scales[s][:, k : k + 1]
            units[k, s] = unit
            scaled = unit * gain[:, place]
            for jj in range(heads):
                turned = turn(scaled[:, jj * HD : (jj + 1) * HD], ang[0, s], ang[1, s])
                qkvx[k, s, jj] = turned.astype(BF)
            to_heads(e, qkvx.at[k, s], qkvh.at[k, s], hsend.at[k, s], hrecv.at[k, s], heads, span)

    for s in range(seqs):
        for k in (2, 0, 1):
            wait_bytes(qkvh.at[k, s], hrecv.at[k, s])
        for i in range(e.nc):
            keys = (i + 1) * span
            kb = qkvh[1, s, 0 : i + 1].reshape(keys, HD)
            vb = qkvh[2, s, 0 : i + 1].reshape(keys, HD)
            scores = masked(dot(qkvh[0, s, i], kb, NT) * HD**-0.5, seg_col, seg_row, s, i, span)
            top = jnp.max(scores, axis=-1, keepdims=True)
            ex_s = jnp.exp(scores - top)
            total = jnp.sum(ex_s, axis=-1, keepdims=True)
            log_total = top + jnp.log(total)
            lse[s, i * span : (i + 1) * span, :] = jnp.broadcast_to(log_total, (span, HD))
            probs = (ex_s * (1.0 / total)).astype(BF)
            atth[s, i] = dot(probs, vb, NN).astype(BF)
        dst = att.at[s, own, cut(lax.rem(e.c, heads), HD)]
        from_heads(e, atth.at[s], dst, bsend.at[s], brecv.at[s], heads)
    for k, (a, b) in enumerate(((qkvh, qkv_heads), (atth, att_heads))):
        outs.append(pltpu.make_async_copy(a, b, osem.at[4 + k]))
        outs[-1].start()
    for s in range(seqs):
        wait_bytes(att.at[s], brecv.at[s])
        from_heads_drain(e, atth.at[s], bsend.at[s], heads)
        for k in range(3):
            to_heads_drain(e, qkvx.at[k, s], hsend.at[k, s], heads, span)
        gat[s].drain()
    angle_copy().wait_send()
    for w in ws:
        w.drain()
    for o in outs:
        o.wait()


def front_stage(sizes, tokens, cos_own, sin_own, qgain, kgain, seg_col, seg_row, wq, wk, wv):
    nf, nc, nt = sizes
    seqs, rows, dm = tokens.shape
    wide = wq.shape[1] // 2
    heads = wide // HD
    full = 2 * nt * rows
    span = nt * rows
    sds = jax.ShapeDtypeStruct
    v, dma = pltpu.VMEM, pltpu.SemaphoreType.DMA
    return pl.pallas_call(
        functools.partial(front_kernel, sizes, seqs, rows),
        name="front_stage",
        out_shape=(
            sds((seqs, full, wide), BF),
            sds((seqs, full, dm), BF),
            sds((dm, wide), BF),
            sds((dm, wide), BF),
            sds((dm, wide), BF),
            sds((2, seqs, full, wide), F32),
            sds((seqs, full, 128), F32),
            sds((2, seqs, full, HD), F32),
            sds((3, seqs, nc, span, HD), BF),
            sds((seqs, nc, span, HD), BF),
            sds((seqs, nc * span, HD), F32),
        ),
        in_specs=[VMEM_SPEC] * 7 + [HBM_SPEC] * 3,
        out_specs=(HBM_SPEC,) * 5 + (VMEM_SPEC,) * 3 + (HBM_SPEC,) * 2 + (VMEM_SPEC,),
        scratch_shapes=[
            v((seqs, full, dm), BF),
            v((dm, wide), BF),
            v((dm, wide), BF),
            v((dm, wide), BF),
            v((2, seqs, full, wide), F32),
            v((3, seqs, heads, full, HD), BF),
            v((3, seqs, nc, span, HD), BF),
            v((seqs, nc, span, HD), BF),
            v((8, seqs * full), F32),
            v((2 * nt, 8, seqs * full), F32),
            v((128, seqs * full), F32),
            v((2, seqs, full, HD), F32),
            dma((3, 2)),
            dma((seqs, 6, 2 * nt - 1)),
            dma((2,)),
            dma((2, 2 * nt)),
            dma((3, seqs, heads, 2)),
            dma((3, seqs)),
            dma((seqs, nc)),
            dma((seqs,)),
            dma((6,)),
        ],
        compiler_params=pltpu.CompilerParams(
            collective_id=2, has_side_effects=True, vmem_limit_bytes=60 << 20
        ),
    )(tokens, cos_own, sin_own, qgain, kgain, seg_col, seg_row, wq, wk, wv)


class Scatter:
    def __init__(self, e, part, inbox, send, recv):
        self.e, self.part, self.inbox, self.send, self.recv = e, part, inbox, send, recv
        self.rows, self.half = inbox.shape[1], part.shape[1]

    def piece(self, f, c):
        return self.part.at[cut(f * self.e.nc + c, self.rows), :]

    def start(self):
        e = self.e
        slot = lax.div(e.group, 2) * e.nc + e.c
        dst = self.inbox.at[slot, :, cut(e.p, self.half)]
        for off in e.plane():
            f, _, c = e.peer(off)
            remote(self.piece(f, c), dst, self.send, self.recv, e.at(f=f, c=c)).start()
        pltpu.make_async_copy(self.piece(e.f, e.c), dst, self.recv).start()

    def wait(self):
        wait_bytes(self.inbox, self.recv)

    def drain(self):
        count = len(self.e.plane()) * self.rows
        wait_bytes(self.part.at[pl.ds(0, count), :], self.send)


def tail_kernel(
    sizes, seqs, rows,
    hidden_grad, gains_in, units, scales, angles, qgain, kgain, seg_col, seg_row, lse,
    agh_in, qkv_heads, att_heads, xs_in, wq_in, wk_in, wv_in,
    wo_part, gate_part, up_part, down_part,
    input_grad, gains_out, o_q, o_k, o_v, o_o, o_g, o_u, o_d,
    agh, qkvh, atth, x, wq, wk, wv, dh, dx, acck, accv, uu, pre, part, pair, right, left, y,
    mine, inbox, wide_t, gmine, gin, gin2, in_q, in_k, in_v, in_o, in_g, in_u, in_d, fin,
    lsem, dsend, drecv, esem, rsem, ssem, g1sem, g2sem, fsem,
):
    e = Place(*sizes)
    n = e.nt
    span = n * rows
    dm = x.shape[2]
    wide = wq.shape[1]
    heads = wide // HD
    scat = [
        Scatter(e, p, b, ssem.at[k, 0], ssem.at[k, 1])
        for k, (p, b) in enumerate(
            (
                (wq, in_q), (wk, in_k), (wv, in_v), (wo_part, in_o),
                (gate_part, in_g), (up_part, in_u), (down_part, in_d),
            )
        )
    ]
    outs = (o_q, o_k, o_v, o_o, o_g, o_u, o_d)
    loads = [
        pltpu.make_async_copy(a, b, lsem.at[k])
        for k, (a, b) in enumerate(
            (
                (qkv_heads, qkvh), (agh_in, agh), (att_heads, atth), (wq_in, wq),
                (wk_in, wk), (wv_in, wv), (xs_in, x),
            )
        )
    ]
    for ld in loads:
        ld.start()
    e.barrier()
    scat[6].start()
    scat[4].start()
    wide_t[...] = jnp.zeros_like(wide_t)
    for ld in loads[:3]:
        ld.wait()

    for s in range(seqs):
        acck[...] = jnp.zeros_like(acck)
        accv[...] = jnp.zeros_like(accv)
        for i in range(e.nc):
            keys = (i + 1) * span
            kb = qkvh[1, s, 0 : i + 1].reshape(keys, HD)
            vb = qkvh[2, s, 0 : i + 1].reshape(keys, HD)
            qb = qkvh[0, s, i]
            rowsl = pl.ds(i * span, span)
            scores = masked(dot(qb, kb, NT) * HD**-0.5, seg_col, seg_row, s, i, span)
            probs = jnp.exp(scores - lse[s, rowsl, 0:1])
            da = agh[s, i]
            accv[0:keys] += dot(probs.astype(BF), da, TN)
            delta = jnp.sum(da.astype(F32) * atth[s, i].astype(F32), axis=-1, keepdims=True)
            ds = (probs * (dot(da, vb, NT) - delta)).astype(BF)
            dh[0, s, i] = (dot(ds, kb, NN) * HD**-0.5).astype(BF)
            acck[0:keys] += dot(ds, qb, TN)
        dh[1, s] = (acck[...] * HD**-0.5).astype(BF).reshape(e.nc, span, HD)
        dh[2, s] = accv[...].astype(BF).reshape(e.nc, span, HD)
        own = pl.ds(pl.multiple_of(e.p * span, span), span)
        for k in range(3):
            dst = dx.at[k, s, lax.rem(e.c, heads), own, :]
            from_heads(e, dh.at[k, s], dst, dsend.at[k, s], drecv.at[k, s], heads)
    scat[5].start()
    scat[3].start()

    place = cut(e.t * 2 + e.p, wide)
    gmine[...] = gains_in[...]
    gmine[0:2, :] = jnp.zeros((2, dm), F32)
    inner = [[], []]
    for s in range(seqs):
        for k in range(3):
            wait_bytes(dx.at[k, s], drecv.at[k, s])
        for k, gain in enumerate((qgain, kgain)):
            for jj in range(heads):
                lanes = slice(jj * HD, (jj + 1) * HD)
                g = turn_back(dx[k, s, jj].astype(F32), angles[0, s], angles[1, s])
                uu[k, s, :, lanes] = g
            g = uu[k, s]
            unit = units[k, s]
            gmine[k : k + 1, place] += jnp.sum(g * unit, axis=0, keepdims=True)
            u = g * gain[:, place]
            uu[k, s] = u
            inner[k].append(jnp.sum(u * unit, axis=-1, keepdims=True))
        for jj in range(heads):
            pre[2, s, :, jj * HD : (jj + 1) * HD] = dx[2, s, jj]
    mine[...] = columns(*[jnp.concatenate(v, axis=0) for v in inner])
    ex = Exchange(e, mine, inbox, esem.at[0], esem.at[1], *Exchange.heads(e))
    ex.start()
    gx = Exchange(e, gmine, gin, g1sem.at[0], g1sem.at[1], *Exchange.plane(e))
    gx.start()
    for ld in loads[3:]:
        ld.wait()
    wide_t[0:8] = ex.finish() / D
    cols = wide_t[...].T
    for s in range(seqs):
        for k in range(2):
            mean = cols[s * 2 * span : (s + 1) * 2 * span, k : k + 1]
            v = scales[s][:, k : k + 1] * (uu[k, s] - units[k, s] * mean)
            pre[k, s] = v.astype(BF)

    tile = 512
    red = [
        Reduce(e, part.at[s], pair.at[s], right.at[s], left.at[s], rsem.at[s], rows)
        for s in range(seqs)
    ]
    for s in range(seqs):

        def step(i, s=s):
            sl = cut(i, tile)
            total = dot(pre[0, s], wq[sl, :], NT) + dot(pre[1, s], wk[sl, :], NT)
            part[s, :, sl] = (total + dot(pre[2, s], wv[sl, :], NT)).astype(BF)

        loop(dm // tile, step)
        red[s].pair_send()
    for s in range(seqs):
        red[s].pair_add()
        red[s].slot(-1)
    for k, w in enumerate((wq, wk, wv)):

        def step(i, k=k, w=w):
            sl = cut(i, tile)
            lhs = x[:, :, sl].reshape(-1, tile)
            w[sl, :] = dot(lhs, pre[k].reshape(-1, wide), TN).astype(BF)

        loop(dm // tile, step)
        scat[k].start()
        for s in range(seqs):
            red[s].slot(k)
    for j in range(3, n - 1):
        for s in range(seqs):
            red[s].slot(j)
    gmine[...] = gx.finish()
    gx2 = Exchange(e, gmine, gin2, g2sem.at[0], g2sem.at[1], *Exchange.line(e))
    gx2.start()
    for s in range(seqs):
        red[s].result(y)
        input_grad[s] = hidden_grad[s] + y[...]
    gains_out[...] = gx2.finish()

    stores = {}
    for turn_no, k in enumerate((6, 4, 5, 3, 0, 1, 2)):
        buf = turn_no % 2
        sc = scat[k]
        sc.wait()
        if buf in stores:
            stores[buf].wait()
        width = 2 * sc.half
        rb = sc.rows
        total = sc.inbox[0].astype(F32)
        for i in range(1, sc.inbox.shape[0]):
            total = total + sc.inbox[i].astype(F32)
        fin[buf, :, 0:width] = total
        stores[buf] = pltpu.make_async_copy(
            fin.at[buf, :, pl.ds(0, width)], outs[k], fsem.at[buf]
        )
        stores[buf].start()
    for st in stores.values():
        st.wait()
    for sc in scat:
        sc.drain()
    for s in range(seqs):
        red[s].drain()
        for k in range(3):
            from_heads_drain(e, dh.at[k, s], dsend.at[k, s], heads)


def tail_stage(sizes, *args):
    nf, nc, nt = sizes
    hidden_grad, xs, gate_part, wo_part = args[0], args[13], args[18], args[17]
    seqs, rows, dm = hidden_grad.shape
    half, wide = gate_part.shape[1], wo_part.shape[1]
    heads = wide // HD
    full = 2 * nt * rows
    span = nt * rows
    rb = dm // (nf * nc)
    slots = nf // 2 * nc
    sds = jax.ShapeDtypeStruct
    v, dma = pltpu.VMEM, pltpu.SemaphoreType.DMA
    small, large = v((slots, rb, 2 * wide), BF), v((slots, rb, 2 * half), BF)
    return pl.pallas_call(
        functools.partial(tail_kernel, sizes, seqs, rows),
        name="tail_stage",
        out_shape=(sds((seqs, rows, dm), F32), sds((8, dm), F32))
        + (sds((rb, 2 * wide), F32),) * 4
        + (sds((rb, 2 * half), F32),) * 3,
        in_specs=[VMEM_SPEC] * 10 + [HBM_SPEC] * 11,
        out_specs=(VMEM_SPEC,) * 2 + (HBM_SPEC,) * 7,
        scratch_shapes=[
            v((seqs, nc, span, HD), BF),
            v((3, seqs, nc, span, HD), BF),
            v((seqs, nc, span, HD), BF),
            v((seqs, full, dm), BF),
            v((dm, wide), BF),
            v((dm, wide), BF),
            v((dm, wide), BF),
            v((3, seqs, nc, span, HD), BF),
            v((3, seqs, heads, full, HD), BF),
            v((nc * span, HD), F32),
            v((nc * span, HD), F32),
            v((2, seqs, full, wide), F32),
            v((3, seqs, full, wide), BF),
            v((seqs, full, dm), BF),
            v((seqs, nt * rows, dm), BF),
            v((seqs, nt - 1, rows, dm), BF),
            v((seqs, nt - 1, rows, dm), BF),
            v((rows, dm), F32),
            v((8, seqs * full), F32),
            v((2 * nt, 8, seqs * full), F32),
            v((128, seqs * full), F32),
            v((8, dm), F32),
            v((nf * nc, 8, dm), F32),
            v((nt, 8, dm), F32),
            small, small, small, small, large, large, large,
            v((2, rb, 2 * half), F32),
            dma((7,)),
            dma((3, seqs, nc)),
            dma((3, seqs)),
            dma((2, 2 * nt)),
            dma((seqs, 4, nt)),
            dma((7, 2)),
            dma((2, nf * nc)),
            dma((2, nt)),
            dma((2,)),
        ],
        compiler_params=pltpu.CompilerParams(
            collective_id=3, has_side_effects=True, vmem_limit_bytes=63 << 20
        ),
    )(*args)


def body(
    tokens, segments, positions, query_weight, key_weight, value_weight, output_weight,
    gate_weight, up_projection_weight, down_weight, query_gain, key_gain, attention_gain,
    feedforward_gain, cotangent,
):
    sizes = (lax.axis_size("fsdp"), lax.axis_size("ctx"), lax.axis_size("tensor"))
    seqs, rows, _ = tokens.shape
    span = sizes[2] * rows
    block_pos = lax.dynamic_slice_in_dim(positions, lax.axis_index("ctx") * span, span, 1)
    cosine, sine = rope_tables(block_pos)
    cos_own = jnp.concatenate([cosine, cosine], axis=-1)
    sin_own = jnp.concatenate([-sine, sine], axis=-1)
    seg_col = segments[:, :, None]
    seg_row = segments[:, None, :]
    qgain, kgain = query_gain[None], key_gain[None]
    (
        att, xs, wq, wk, wv, units, scales, angles, qkv_heads, att_heads, lse,
    ) = front_stage(
        sizes, tokens, cos_own, sin_own, qgain, kgain, seg_col, seg_row,
        query_weight, key_weight, value_weight,
    )
    block_out, hidden_grad, agh, wo_part, gate_part, up_part, down_part, gains = ffn_stage(
        sizes, att, output_weight, gate_weight, up_projection_weight, down_weight,
        tokens, cotangent, attention_gain[None], feedforward_gain[None],
    )
    input_grad, gain_sums, *weight_grads = tail_stage(
        sizes, hidden_grad, gains, units, scales, angles, qgain, kgain, seg_col, seg_row, lse,
        agh, qkv_heads, att_heads, xs, wq, wk, wv, wo_part, gate_part, up_part, down_part,
    )
    return (block_out, input_grad, *weight_grads, *(gain_sums[k] for k in range(4)))


def solution(mesh):
    in_specs = (
        P("fsdp", ("ctx", "tensor"), None),
        P("fsdp", None),
        P("fsdp", None),
        P(("fsdp", "ctx"), "tensor"),
        P(("fsdp", "ctx"), "tensor"),
        P(("fsdp", "ctx"), "tensor"),
        P(("fsdp", "ctx"), "tensor"),
        P(("fsdp", "ctx"), "tensor"),
        P(("fsdp", "ctx"), "tensor"),
        P(("fsdp", "ctx"), "tensor"),
        P(),
        P(),
        P(),
        P(),
        P("fsdp", ("ctx", "tensor"), None),
    )
    out_specs = (
        P("fsdp", ("ctx", "tensor"), None),
        P("fsdp", ("ctx", "tensor"), None),
        P(("fsdp", "ctx"), "tensor"),
        P(("fsdp", "ctx"), "tensor"),
        P(("fsdp", "ctx"), "tensor"),
        P(("fsdp", "ctx"), "tensor"),
        P(("fsdp", "ctx"), "tensor"),
        P(("fsdp", "ctx"), "tensor"),
        P(("fsdp", "ctx"), "tensor"),
        P(),
        P(),
        P(),
        P(),
    )
    return jax.shard_map(body, mesh=mesh, in_specs=in_specs, out_specs=out_specs, check_vma=False)
```

```python
import functools

import jax
import jax.numpy as jnp
from jax import lax
from jax.experimental import pallas as pl
from jax.experimental.pallas import tpu as pltpu
from jax.sharding import PartitionSpec as P

D = 2048
HD = 128


epsilon = 1e-06
rope_theta = 500000.0
masked_score = -1e30


def rope_tables(position_ids):
    freq_index = jnp.arange(HD // 2, dtype=jnp.float32)
    inverse = rope_theta ** (-2.0 * freq_index / HD)
    angles = position_ids.astype(jnp.float32)[..., None] * inverse
    return (jnp.cos(angles), jnp.sin(angles))


MESH = pl.DeviceIdType.MESH
BF = jnp.bfloat16
F32 = jnp.float32
VMEM_SPEC = pl.BlockSpec(memory_space=pltpu.VMEM)
HBM_SPEC = pl.BlockSpec(memory_space=pltpu.HBM)
NN = (((1,), (0,)), ((), ()))
NT = (((1,), (1,)), ((), ()))
TN = (((0,), (0,)), ((), ()))


def dot(a, b, dims):
    return lax.dot_general(a, b, dims, preferred_element_type=F32)


def loop(count, step):
    def run(i, carry):
        step(i)
        return carry

    lax.fori_loop(0, count, run, 0)


def cut(i, size):
    return pl.ds(pl.multiple_of(i * size, size), size)


def both(*conds):
    out = True
    for cond in conds:
        if isinstance(cond, bool):
            if not cond:
                return False
        elif isinstance(out, bool):
            out = cond
        else:
            out = jnp.logical_and(out, cond)
    return out


def when(cond, step):
    if isinstance(cond, bool):
        if cond:
            step()
    else:
        pl.when(cond)(step)


class Place:
    def __init__(self, fsdp_size, ctx_size, tensor_size):
        self.nf, self.nc, self.nt = fsdp_size, ctx_size, tensor_size
        self.f = lax.axis_index("fsdp")
        self.c = lax.axis_index("ctx")
        self.t = lax.axis_index("tensor")
        self.p = lax.rem(self.f, 2)
        self.group = self.f - self.p
        self.mate = self.group + 1 - self.p

    def at(self, f=None, c=None, t=None):
        return {
            "fsdp": self.f if f is None else f,
            "ctx": self.c if c is None else c,
            "tensor": self.t if t is None else t,
        }

    def plane(self):
        out = []
        for dg in range(self.nf // 2):
            for dc in (3, 1, 2, 0) if self.nc == 4 else range(self.nc):
                for dp in (0, 1):
                    if dg or dc or dp:
                        out.append((dg, dc, dp))
        return out

    def peer(self, off):
        dg, dc, dp = off
        group = lax.rem(self.group + 2 * dg, self.nf)
        core = self.p + dp - 2 * self.p * dp
        return group + core, core, jnp.bitwise_xor(self.c, dc)

    def barrier(self):
        sem = pltpu.get_barrier_semaphore()

        def signal(**place):
            pl.semaphore_signal(sem, inc=1, device_id=self.at(**place), device_id_type=MESH)

        offs = self.plane()
        for off in offs:
            f, _, c = self.peer(off)
            signal(f=f, c=c)
        for dt in range(1, self.nt):
            for core in range(2):
                signal(f=self.group + core, t=lax.rem(self.t + dt, self.nt))
        pl.semaphore_wait(sem, len(offs) + 2 * (self.nt - 1))


def remote(src, dst, send, recv, device):
    return pltpu.make_async_remote_copy(
        src_ref=src, dst_ref=dst, send_sem=send, recv_sem=recv, device_id=device, device_id_type=MESH
    )


def wait_bytes(ref, sem):
    pltpu.make_async_copy(ref, ref, sem).wait()


class Reduce:
    def __init__(self, e, part, pair, right, left, sems, rows):
        self.e, self.part, self.pair, self.right, self.left, self.rows = e, part, pair, right, left, rows
        self.sems = sems

    def half(self, p):
        n = self.e.nt * self.rows
        return self.part.at[pl.ds(pl.multiple_of(p * n, n), n), :]

    def block(self, b):
        return self.part.at[cut(self.e.p * self.e.nt + b, self.rows), :]

    def _pair(self):
        return remote(
            self.half(1 - self.e.p), self.pair, self.sems.at[0, 0], self.sems.at[1, 0],
            self.e.at(f=self.e.mate),
        )

    def _side(self, b, k, up):
        e = self.e
        buf, row = (self.right, 0) if up else (self.left, 2)
        return remote(
            self.block(b), buf.at[k], self.sems.at[row, 1 + k], self.sems.at[row + 1, 1 + k],
            e.at(t=e.t + 1 if up else e.t - 1),
        )

    def pair_send(self):
        self._pair().start()

    def pair_add(self):
        self._pair().wait_recv()
        mine = self.half(self.e.p)

        def step(i):
            sl = cut(i, self.rows)
            mine[sl, :] = (mine[sl, :].astype(F32) + self.pair[sl, :].astype(F32)).astype(BF)

        loop(self.e.nt, step)

    def slot(self, j):
        e, n = self.e, self.e.nt
        for up in (True, False):
            b = e.t + (n - 2) - j if up else e.t - (n - 2) + j
            near = e.t > 0 if up else e.t < n - 1
            far = e.t < n - 1 if up else e.t > 0
            inside = b <= n - 1 if up else b >= 0
            buf = self.right if up else self.left

            def take(b=b, buf=buf, up=up):
                self._side(b, j, up).wait_recv()

                def add():
                    blk = self.block(b)
                    blk[...] = (blk[...].astype(F32) + buf[j].astype(F32)).astype(BF)

                when(j < n - 2, add)

            when(both(j >= 0, j <= n - 2, near, inside), take)
            when(both(j < n - 2, far, inside), lambda b=b, up=up: self._side(b, j + 1, up).start())

    def result(self, out):
        e, n = self.e, self.e.nt
        out[...] = self.block(e.t)[...].astype(F32)

        def add_right():
            out[...] += self.right[n - 2].astype(F32)

        def add_left():
            out[...] += self.left[n - 2].astype(F32)

        when(e.t > 0, add_right)
        when(e.t < n - 1, add_left)

    def drain(self):
        e, n = self.e, self.e.nt
        self._pair().wait_send()

        def step(i):
            j = i - 1
            for up in (True, False):
                b = e.t + (n - 2) - j if up else e.t - (n - 2) + j
                far = e.t < n - 1 if up else e.t > 0
                inside = b <= n - 1 if up else b >= 0
                when(both(far, inside), lambda b=b, up=up: self._side(b, j + 1, up).wait_send())

        for i in range(n - 1):
            step(i)


class Gather:
    def __init__(self, e, full, sems, rows):
        self.e, self.full, self.sems, self.rows = e, full, sems, rows

    def block(self, p, b):
        return self.full.at[cut(p * self.e.nt + b, self.rows), :]

    def _side(self, b, k, up):
        e = self.e
        row = 0 if up else 2
        ref = self.block(e.p, b)
        return remote(
            ref, ref, self.sems.at[row, k], self.sems.at[row + 1, k],
            e.at(t=e.t + 1 if up else e.t - 1),
        )

    def _pair(self, b, k, incoming):
        e = self.e
        ref = self.block(1 - e.p if incoming else e.p, b)
        return remote(ref, ref, self.sems.at[4, k], self.sems.at[5, k], e.at(f=e.mate))

    def init(self):
        e, n = self.e, self.e.nt
        when(e.t < n - 1, lambda: self._side(e.t, 0, True).start())
        when(e.t > 0, lambda: self._side(e.t, 0, False).start())
        self._pair(e.t, 0, False).start()

    def slot(self, j):
        e, n = self.e, self.e.nt
        for up in (True, False):
            b = e.t - 1 - j if up else e.t + 1 + j
            inside = b >= 0 if up else b <= n - 1
            far = e.t < n - 1 if up else e.t > 0
            k = 1 + j if up else n + j

            def take(b=b, up=up, far=far, k=k):
                self._side(b, j, up).wait_recv()
                when(both(far, j < n - 2), lambda: self._side(b, j + 1, up).start())
                self._pair(b, k, False).start()

            when(both(j >= 0, j <= n - 2, inside), take)

    def _rest(self, step_pair):
        e, n = self.e, self.e.nt
        step_pair(e.t, 0)
        for j in range(n - 1):
            when(e.t - 1 - j >= 0, lambda j=j: step_pair(e.t - 1 - j, 1 + j))
            when(e.t + 1 + j <= n - 1, lambda j=j: step_pair(e.t + 1 + j, n + j))

    def done(self):
        self._rest(lambda b, k: self._pair(b, k, True).wait_recv())

    def drain(self):
        e, n = self.e, self.e.nt
        self._rest(lambda b, k: self._pair(b, k, False).wait_send())
        when(e.t < n - 1, lambda: self._side(e.t, 0, True).wait_send())
        when(e.t > 0, lambda: self._side(e.t, 0, False).wait_send())
        for j in range(n - 2):
            when(
                both(e.t - 1 - j >= 0, e.t < n - 1),
                lambda j=j: self._side(e.t - 1 - j, j + 1, True).wait_send(),
            )
            when(
                both(e.t + 1 + j <= n - 1, e.t > 0),
                lambda j=j: self._side(e.t + 1 + j, j + 1, False).wait_send(),
            )


class Weight:
    def __init__(self, e, shard, full, sems, off=0):
        self.e, self.shard, self.full, self.sems, self.off = e, shard, full, sems, off
        self.rows, self.width = shard.shape[0], full.shape[1]
        self.stride = shard.shape[1] // 2

    def columns(self, core):
        start = pl.multiple_of(core * self.stride + self.off, 128)
        return self.shard.at[:, pl.ds(start, self.width)]

    def some(self, count):
        return self.full.at[pl.ds(0, count * self.rows), :]

    def targets(self):
        e = self.e
        if e.nf == 2:
            return [(0, 1, 0), (0, 2, 0), (0, 1, 1), (0, 2, 1), (0, 0, 1)]
        return e.plane()

    def start(self):
        e = self.e
        dst = self.full.at[cut(e.f * e.nc + e.c, self.rows), :]
        for off in self.targets():
            f, core, c = e.peer(off)
            remote(self.columns(core), dst, self.sems.at[0], self.sems.at[1], e.at(f=f, c=c)).start()
        pltpu.make_async_copy(self.columns(e.p), dst, self.sems.at[1]).start()

    def relay(self):
        e = self.e
        wait_bytes(self.some(len(self.targets()) + 1), self.sems.at[1])
        if e.nf != 2:
            return
        part = self.rows // 2
        for f in range(2):
            for k, (source, target) in enumerate(((1, 2), (2, 1))):
                row = (f * e.nc + jnp.bitwise_xor(e.c, source)) * self.rows + k * part
                ref = self.full.at[pl.ds(pl.multiple_of(row, part), part), :]
                device = e.at(c=jnp.bitwise_xor(e.c, target))
                remote(ref, ref, self.sems.at[2], self.sems.at[3], device).start()

    def wait(self):
        if self.e.nf == 2:
            wait_bytes(self.some(2), self.sems.at[3])

    def drain(self):
        wait_bytes(self.some(len(self.targets())), self.sems.at[0])
        if self.e.nf == 2:
            wait_bytes(self.some(2), self.sems.at[2])


class Scatter:
    def __init__(self, e, part, first, inbox, sems):
        self.e, self.part, self.first, self.inbox, self.sems = e, part, first, inbox, sems
        self.rows, self.half = inbox.shape[1], part.shape[1]
        self.upper = self.rows // 2

    def piece(self, f, c, side=None):
        row = (f * self.e.nc + c) * self.rows
        if side is None:
            return self.part.at[pl.ds(pl.multiple_of(row, self.rows), self.rows), :]
        row = pl.multiple_of(row + side * self.upper, self.upper)
        return self.part.at[pl.ds(row, self.upper), :]

    def start(self):
        e = self.e
        if e.nf == 2:
            for side in range(2):
                near = jnp.bitwise_xor(e.c, 1 + side)
                for k, owner in enumerate((near, jnp.bitwise_xor(e.c, 3))):
                    for f in range(2):
                        remote(
                            self.piece(f, owner, side), self.first.at[side, k, f],
                            self.sems.at[0], self.sems.at[1], e.at(c=near),
                        ).start()
            return
        slot = lax.div(e.group, 2) * e.nc + e.c
        dst = self.inbox.at[slot, :, cut(e.p, self.half)]
        for off in e.plane():
            f, _, c = e.peer(off)
            remote(
                self.piece(f, c), dst, self.sems.at[2], self.sems.at[3], e.at(f=f, c=c)
            ).start()
        pltpu.make_async_copy(self.piece(e.f, e.c), dst, self.sems.at[3]).start()

    def relay(self):
        e = self.e
        if e.nf != 2:
            return
        wait_bytes(self.first, self.sems.at[1])
        lanes = cut(e.p, self.half)
        for side in range(2):
            far = jnp.bitwise_xor(e.c, 2 - side)
            for k, owner in enumerate((e.c, far)):
                for f in range(2):
                    mine = self.piece(f, owner, side)
                    got = self.first[side, k, f].astype(F32)
                    mine[...] = (mine[...].astype(F32) + got).astype(BF)
            for f in range(2):
                dst = self.inbox.at[1, pl.ds(side * self.upper, self.upper), lanes]
                remote(
                    self.piece(f, far, side), dst, self.sems.at[2], self.sems.at[3],
                    e.at(f=f, c=far),
                ).start()
        dst = self.inbox.at[0, :, lanes]
        remote(
            self.piece(1 - e.p, e.c), dst, self.sems.at[2], self.sems.at[3], e.at(f=e.mate)
        ).start()
        pltpu.make_async_copy(self.piece(e.p, e.c), dst, self.sems.at[3]).start()

    def wait(self):
        wait_bytes(self.inbox, self.sems.at[3])

    def drain(self):
        e = self.e
        count = 3 if e.nf == 2 else len(e.plane())
        wait_bytes(self.part.at[pl.ds(0, count * self.rows), :], self.sems.at[2])
        if e.nf == 2:
            wait_bytes(self.part.at[pl.ds(0, 4 * self.rows), :], self.sems.at[0])


def scatter_shapes(sizes, dm, half):
    nf, nc, _ = sizes
    rb = dm // (nf * nc)
    if nf == 2:
        return (2, 2, 2, rb // 2, half), (2, rb, 2 * half)
    return (1, 1, 1, 16, 128), (nf // 2 * nc, rb, 2 * half)


def ffn_kernel(
    sizes, seqs, rows,
    att, wo_in, gate_in, gate_sh, up_sh, down_sh, tokens, cot, again, fgain,
    block_out, hidden_grad, agh, wo_part, gate_part, up_part, down_terms, gains,
    wo_v, g_v, u_v, d_v, part, pair, right, left, hid, mgr, agr, aa, bb, mixed,
    unit1, hid32, scale1, scratch_y, agx, first,
    wsem, lsem, dsem, rsem, gsem, xsend, xrecv, osem,
):
    e = Place(*sizes)
    dm = tokens.shape[2]
    half = g_v.shape[1]
    wide = att.shape[2]
    heads = wide // HD
    early = gate_in.shape[1]
    late = g_v.at[:, pl.ds(early, half - early)]
    w_g = Weight(e, gate_sh, late, wsem.at[0], off=early)
    w_u = Weight(e, up_sh, u_v, wsem.at[1])
    w_d = Weight(e, down_sh, d_v, wsem.at[2])
    load_o = pltpu.make_async_copy(wo_in, wo_v, lsem.at[0])
    load_g = pltpu.make_async_copy(gate_in, g_v.at[:, pl.ds(0, early)], lsem.at[1])
    load_o.start()
    load_g.start()
    scat_d = Scatter(e, d_v, first, down_terms, dsem)

    def reduce(k, s):
        return Reduce(e, part.at[s], pair.at[s], right.at[s], left.at[s], rsem.at[k, s], rows)

    def gather(k, s):
        return Gather(e, (hid, mgr, agr)[k].at[s], gsem.at[k, s], rows)

    red = [[reduce(k, s) for s in range(seqs)] for k in range(3)]
    gat = [[gather(k, s) for s in range(seqs)] for k in range(3)]

    e.barrier()
    w_g.start()
    w_u.start()
    gains[...] = jnp.zeros_like(gains)

    tile = 512

    def out_tiles(s):
        def step(i):
            sl = cut(i, tile)
            part[s, :, sl] = dot(att[s], wo_v[sl, :], NT).astype(BF)

        loop(dm // tile, step)

    def norm1(s):
        y = scratch_y
        red[0][s].result(y)
        v = y[...]
        scale = lax.rsqrt(jnp.mean(v * v, axis=-1, keepdims=True) + epsilon)
        unit = v * scale
        unit1[s] = unit
        scale1[s] = jnp.broadcast_to(scale, scale1.shape[1:])
        h = tokens[s].astype(F32) + unit * again[...]
        hid32[s] = h
        gat[0][s].block(e.p, e.t)[...] = h.astype(BF)

    def ffn_tile(s, i):
        sl = cut(i, 256)
        gate = dot(hid[s], g_v[:, sl], NN)
        up = dot(hid[s], u_v[:, sl], NN)
        sig = jax.nn.sigmoid(gate)
        act = gate * sig
        mixed[s, :, sl] = (act * up).astype(BF)
        aa[s, :, sl] = (up * sig * (1.0 + gate * (1.0 - sig))).astype(BF)
        bb[s, :, sl] = act.astype(BF)

    ffn_tiles = half // 256

    def down_tiles(s):
        def step(i):
            sl = cut(i, tile)
            part[s, :, sl] = dot(mixed[s], d_v[sl, :], NT).astype(BF)

        loop(dm // tile, step)

    def norm2(s):
        y = scratch_y
        red[1][s].result(y)
        v = y[...]
        scale = lax.rsqrt(jnp.mean(v * v, axis=-1, keepdims=True) + epsilon)
        unit = v * scale
        block_out[s] = (hid32[s] + unit * fgain[...]).astype(BF)
        upstream = cot[s].astype(F32)
        gains[3:4, :] += jnp.sum(upstream * unit, axis=0, keepdims=True)
        g = upstream * fgain[...]
        m = scale * (g - unit * jnp.mean(g * unit, axis=-1, keepdims=True))
        gat[1][s].block(e.p, e.t)[...] = m.astype(BF)

    def inner_tiles(s):
        def step(i):
            sl = cut(i, 256)
            inner = dot(mgr[s], d_v[:, sl], NN)
            aa[s, :, sl] = (inner * aa[s, :, sl].astype(F32)).astype(BF)
            bb[s, :, sl] = (inner * bb[s, :, sl].astype(F32)).astype(BF)

        loop(ffn_tiles, step)

    def back_tiles(s):
        def step(i):
            sl = cut(i, tile)
            part[s, :, sl] = (dot(aa[s], g_v[sl, :], NT) + dot(bb[s], u_v[sl, :], NT)).astype(BF)

        loop(dm // tile, step)

    def norm3(s):
        y = scratch_y
        red[2][s].result(y)
        hg = cot[s].astype(F32) + y[...]
        hidden_grad[s] = hg
        unit = unit1[s]
        gains[2:3, :] += jnp.sum(hg * unit, axis=0, keepdims=True)
        g = hg * again[...]
        scale = scale1[s][:, 0:1]
        a = scale * (g - unit * jnp.mean(g * unit, axis=-1, keepdims=True))
        gat[2][s].block(e.p, e.t)[...] = a.astype(BF)

    def weight_tile(left_rows, right_rows, out, i, width):
        per = out.shape[1] // width
        sl, cl = cut(lax.div(i, per), tile), cut(lax.rem(i, per), width)
        lhs = left_rows[:, :, sl].reshape(-1, tile)
        rhs = right_rows[:, :, cl].reshape(-1, width)
        out[sl, cl] = dot(lhs, rhs, TN).astype(BF)

    n = e.nt
    span = agh.shape[2]

    def heads_copy(s, jj, q):
        src = agx.at[s, jj, pl.ds(q * span, span), :]
        dst = agh.at[s, e.c]
        return src, dst

    def heads_grad(s):
        r = dot(agr[s], wo_v[...], NN).astype(BF)
        for jj in range(heads):
            agx[s, jj] = r[:, jj * HD : (jj + 1) * HD]
        for jj in range(heads):
            head = heads * e.p + jj
            for q in range(2):
                src, dst = heads_copy(s, jj, q)
                self_here = both(head == e.c, q == e.p)

                def local(src=src, dst=dst):
                    pltpu.make_async_copy(src, dst, xrecv.at[s]).start()

                def away(src=src, dst=dst, q=q, head=head, jj=jj):
                    remote(
                        src, dst, xsend.at[s, jj, q], xrecv.at[s], e.at(f=e.group + q, c=head)
                    ).start()

                when(self_here, local)
                when(jnp.logical_not(self_here), away)

    def heads_wait(s):
        wait_bytes(agh.at[s], xrecv.at[s])
        block = agx.at[s, 0, pl.ds(0, span), :]
        for jj in range(heads):
            head = heads * e.p + jj
            for q in range(2):
                when(
                    jnp.logical_not(both(head == e.c, q == e.p)),
                    lambda jj=jj, q=q: wait_bytes(block, xsend.at[s, jj, q]),
                )

    load_o.wait()
    out_tiles(0)
    red[0][0].pair_send()
    out_tiles(1)
    red[0][0].pair_add()
    red[0][1].pair_send()

    def step(i):
        red[0][0].slot(i - 1)

    loop(n, step)
    red[0][1].pair_add()
    norm1(0)
    gat[0][0].init()

    def step(i):
        red[0][1].slot(i - 1)
        gat[0][0].slot(i - 1)

    loop(2, step)
    w_g.relay()
    w_u.relay()
    w_d.start()
    loop(n - 2, lambda i: step(i + 2))
    gat[0][0].done()
    norm1(1)
    gat[0][1].init()
    load_g.wait()
    w_g.wait()
    w_u.wait()

    def step(i):
        ffn_tile(0, i)
        gat[0][1].slot(i)

    loop(ffn_tiles, step)
    w_d.relay()
    w_d.wait()
    red[0][0].drain()
    down_tiles(0)
    red[1][0].pair_send()
    gat[0][1].done()
    ffn_tile(1, 0)
    red[1][0].pair_add()

    def step(i):
        red[1][0].slot(i - 1)
        ffn_tile(1, i + 1)

    loop(ffn_tiles - 1, step)
    for j in range(ffn_tiles - 2, n - 1):
        red[1][0].slot(j)
    norm2(0)
    gat[1][0].init()
    red[0][1].drain()
    down_tiles(1)
    red[1][1].pair_send()
    gat[1][0].slot(0)
    red[1][1].pair_add()

    def step(i):
        red[1][1].slot(i - 1)
        gat[1][0].slot(i + 1)

    loop(n, step)
    norm2(1)
    gat[1][1].init()
    gat[1][0].done()
    inner_tiles(0)
    red[1][0].drain()
    back_tiles(0)
    red[2][0].pair_send()
    gat[1][1].slot(0)
    red[2][0].pair_add()

    def step(i):
        red[2][0].slot(i - 1)
        gat[1][1].slot(i + 1)

    loop(n - 2, step)
    gat[1][1].done()
    inner_tiles(1)
    red[2][0].slot(n - 3)
    red[1][1].drain()
    back_tiles(1)
    red[2][1].pair_send()
    red[2][0].slot(n - 2)
    norm3(0)
    gat[2][0].init()
    red[2][1].pair_add()
    red[2][1].slot(-1)
    tiles = (dm // tile) * (half // tile)
    share = -(-tiles // (n - 1))

    def fill(left_rows, right_rows, out, i):
        def go(k):
            which = share * i + k
            when(which < tiles, lambda: weight_tile(left_rows, right_rows, out, which, tile))

        loop(share, go)

    for w in (w_g, w_u, w_d):
        w.drain()
    loop(tiles, lambda i: weight_tile(mgr, mixed, d_v, i, tile))
    scat_d.start()

    def step(i):
        red[2][1].slot(i)
        gat[2][0].slot(i)
        fill(hid, aa, g_v, i)

    loop(n - 1, step)
    out_g = pltpu.make_async_copy(g_v, gate_part, osem.at[1])
    out_g.start()
    norm3(1)
    gat[2][1].init()
    gat[2][0].done()
    heads_grad(0)
    scat_d.relay()

    def step(i):
        gat[2][1].slot(i)
        fill(hid, bb, u_v, i)

    loop(n - 1, step)
    out_u = pltpu.make_async_copy(u_v, up_part, osem.at[2])
    out_u.start()
    gat[2][1].done()
    heads_grad(1)
    loop(dm // tile, lambda i: weight_tile(agr, att, wo_v, i, wide))
    out_o = pltpu.make_async_copy(wo_v, wo_part, osem.at[3])
    out_o.start()
    heads_wait(0)
    heads_wait(1)
    red[2][0].drain()
    red[2][1].drain()
    for k in range(3):
        for s in range(seqs):
            gat[k][s].drain()
    scat_d.wait()
    scat_d.drain()
    for o in (out_g, out_u, out_o):
        o.wait()


def ffn_stage(
    sizes, att, wo_in, gate_in, gate_sh, up_sh, down_sh, tokens, cot, again, fgain
):
    nf, nc, nt = sizes
    seqs, rows, dm = tokens.shape
    half = gate_sh.shape[1] // 2
    wide = wo_in.shape[1]
    first, terms = scatter_shapes(sizes, dm, half)
    full = 2 * nt * rows
    sds = jax.ShapeDtypeStruct
    v, dma = pltpu.VMEM, pltpu.SemaphoreType.DMA
    return pl.pallas_call(
        functools.partial(ffn_kernel, sizes, seqs, rows),
        name="ffn_stage",
        out_shape=(
            sds((seqs, rows, dm), BF),
            sds((seqs, rows, dm), F32),
            sds((seqs, nc, nt * rows, HD), BF),
            sds((dm, wide), BF),
            sds((dm, half), BF),
            sds((dm, half), BF),
            sds(terms, BF),
            sds((8, dm), F32),
        ),
        in_specs=[VMEM_SPEC] + [HBM_SPEC] * 5 + [VMEM_SPEC] * 4,
        out_specs=(VMEM_SPEC, VMEM_SPEC) + (HBM_SPEC,) * 5 + (VMEM_SPEC,),
        scratch_shapes=[
            v((dm, wide), BF),
            v((dm, half), BF),
            v((dm, half), BF),
            v((dm, half), BF),
            v((seqs, full, dm), BF),
            v((seqs, nt * rows, dm), BF),
            v((seqs, nt - 1, rows, dm), BF),
            v((seqs, nt - 1, rows, dm), BF),
            v((seqs, full, dm), BF),
            v((seqs, full, dm), BF),
            v((seqs, full, dm), BF),
            v((seqs, full, half), BF),
            v((seqs, full, half), BF),
            v((seqs, full, half), BF),
            v((seqs, rows, dm), F32),
            v((seqs, rows, dm), F32),
            v((seqs, rows, 128), F32),
            v((rows, dm), F32),
            v((seqs, wide // HD, full, HD), BF),
            v(first, BF),
            dma((3, 4)),
            dma((2,)),
            dma((4,)),
            dma((3, seqs, 4, nt)),
            dma((3, seqs, 6, 2 * nt - 1)),
            dma((seqs, wide // HD, 2)),
            dma((seqs,)),
            dma((4,)),
        ],
        compiler_params=pltpu.CompilerParams(
            collective_id=1, has_side_effects=True, vmem_limit_bytes=63 << 20
        ),
    )(att, wo_in, gate_in, gate_sh, up_sh, down_sh, tokens, cot, again, fgain)


class Exchange:
    def __init__(self, e, mine, inbox, send, recv, members, own):
        self.e, self.mine, self.inbox, self.send, self.recv = e, mine, inbox, send, recv
        self.members, self.own = members, own

    @staticmethod
    def plane(e):
        out = []
        for f in range(e.nf):
            for c in range(e.nc):
                out.append((f * e.nc + c, e.at(f=f, c=c), both(e.f == f, e.c == c)))
        return out, e.f * e.nc + e.c

    @staticmethod
    def heads(e):
        out = []
        for q in range(2):
            for t in range(e.nt):
                out.append((q * e.nt + t, e.at(f=e.group + q, t=t), both(e.p == q, e.t == t)))
        return out, e.p * e.nt + e.t

    @staticmethod
    def line(e):
        return [(t, e.at(t=t), e.t == t) for t in range(e.nt)], e.t

    def start(self):
        self.inbox[self.own] = self.mine[...]
        for k, device, me in self.members:

            def go(k=k, device=device):
                remote(
                    self.mine, self.inbox.at[self.own], self.send.at[k], self.recv.at[self.own], device
                ).start()

            when(jnp.logical_not(me), go)

    def finish(self):
        for k, device, me in self.members:

            def go(k=k, device=device):
                d = remote(self.mine, self.inbox.at[k], self.send.at[k], self.recv.at[k], device)
                d.wait_recv()
                d.wait_send()

            when(jnp.logical_not(me), go)
        return jnp.sum(self.inbox[...], axis=0)


def to_heads(e, src, dst, send, recv, heads, span):
    for jj in range(heads):
        head = heads * e.p + jj
        for q in range(2):
            piece = src.at[jj, pl.ds(q * span, span), :]
            here = both(head == e.c, q == e.p)
            when(here, lambda piece=piece: pltpu.make_async_copy(piece, dst.at[e.c], recv).start())

            def away(piece=piece, jj=jj, q=q, head=head):
                remote(
                    piece, dst.at[e.c], send.at[jj, q], recv, e.at(f=e.group + q, c=head)
                ).start()

            when(jnp.logical_not(here), away)


def to_heads_drain(e, src, send, heads, span):
    piece = src.at[0, pl.ds(0, span), :]
    for jj in range(heads):
        head = heads * e.p + jj
        for q in range(2):
            here = both(head == e.c, q == e.p)
            when(jnp.logical_not(here), lambda jj=jj, q=q: wait_bytes(piece, send.at[jj, q]))


def from_heads(e, src, dst, send, recv, heads):
    core = lax.div(e.c, heads)
    for c in range(e.nc):
        here = both(e.c == c, core == e.p)
        when(here, lambda c=c: pltpu.make_async_copy(src.at[c], dst, recv).start())

        def away(c=c):
            remote(src.at[c], dst, send.at[c], recv, e.at(f=e.group + core, c=c)).start()

        when(jnp.logical_not(here), away)


def from_heads_drain(e, src, send, heads):
    core = lax.div(e.c, heads)
    for c in range(e.nc):
        here = both(e.c == c, core == e.p)
        when(jnp.logical_not(here), lambda c=c: wait_bytes(src.at[c], send.at[c]))


def columns(first, second):
    lane = lax.broadcasted_iota(jnp.int32, (first.shape[0], 128), 1)
    both_cols = jnp.where(lane == 0, first, jnp.where(lane == 1, second, 0.0))
    return both_cols.T[0:8]


def turn(values, angle_cos, angle_sin):
    return values * angle_cos + pltpu.roll(values, HD // 2, 1) * angle_sin


def turn_back(values, angle_cos, angle_sin):
    return values * angle_cos - pltpu.roll(values, HD // 2, 1) * angle_sin


def masked(scores, seg_col, seg_row, s, i, span):
    keys = scores.shape[1]
    row = lax.broadcasted_iota(jnp.int32, scores.shape, 0) + i * span
    col = lax.broadcasted_iota(jnp.int32, scores.shape, 1)
    same = seg_col[s, pl.ds(i * span, span), :] == seg_row[s, :, pl.ds(0, keys)]
    return jnp.where(jnp.logical_and(same, row >= col), scores, masked_score)


def front_kernel(
    sizes, seqs, rows,
    tokens, cos_own, sin_own, qgain, kgain, seg_col, seg_row, wq_sh, wk_sh, wv_sh, wo_sh, gate_sh,
    att, xs_out, wq_out, wk_out, wv_out, wo_out, gate_out, units, scales, angles, qkv_heads, att_heads, lse,
    x, wq, wk, wv, lin, qkvx, qkvh, atth, mine, inbox, wide_t, ang,
    wsem, gsem, asem, esem, hsend, hrecv, bsend, brecv, osem,
):
    e = Place(*sizes)
    n = e.nt
    span = n * rows
    wide = wq.shape[1]
    heads = wide // HD
    pairs = ((wq_sh, wq), (wk_sh, wk), (wv_sh, wv), (wo_sh, wo_out), (gate_sh, gate_out))
    ws = [Weight(e, sh, full, wsem.at[i]) for i, (sh, full) in enumerate(pairs)]
    gat = [Gather(e, x.at[s], gsem.at[s], rows) for s in range(seqs)]
    own = pl.ds(pl.multiple_of(e.p * span, span), span)

    def angle_copy():
        ref = ang.at[:, :, own, :]
        return remote(ref, ref, asem.at[0], asem.at[1], e.at(f=e.mate))

    e.barrier()
    for s in range(seqs):
        gat[s].block(e.p, e.t)[...] = tokens[s]
        gat[s].init()
    for w in (ws[2], ws[0], ws[1]):
        w.start()
    ang[0, :, own, :] = cos_own[...]
    ang[1, :, own, :] = sin_own[...]
    angle_copy().start()
    wide_t[...] = jnp.zeros_like(wide_t)

    def step(j):
        for s in range(seqs):
            gat[s].slot(j)

    loop(n - 2, step)
    for w in (ws[2], ws[0], ws[1]):
        w.relay()
    ws[3].start()
    ws[4].start()
    step(n - 2)
    for s in range(seqs):
        gat[s].done()
    outs = [pltpu.make_async_copy(x, xs_out, osem.at[0])]
    outs[0].start()
    ws[2].wait()
    for s in range(seqs):
        r = dot(x[s], wv[...], NN).astype(BF)
        for jj in range(heads):
            qkvx[2, s, jj] = r[:, jj * HD : (jj + 1) * HD]
        to_heads(e, qkvx.at[2, s], qkvh.at[2, s], hsend.at[2, s], hrecv.at[2, s], heads, span)
    ws[0].wait()
    ws[1].wait()
    for k, (w, out) in enumerate(((wq, wq_out), (wk, wk_out), (wv, wv_out))):
        outs.append(pltpu.make_async_copy(w, out, osem.at[1 + k]))
        outs[-1].start()
    sums = [[], []]
    for k, w in enumerate((wq, wk)):
        for s in range(seqs):
            r = dot(x[s], w[...], NN)
            lin[k, s] = r
            sums[k].append(jnp.sum(r * r, axis=-1, keepdims=True))
    mine[...] = columns(*[jnp.concatenate(v, axis=0) for v in sums])
    ex = Exchange(e, mine, inbox, esem.at[0], esem.at[1], *Exchange.heads(e))
    ex.start()
    angle_copy().wait_recv()
    angles[...] = ang[...]
    wide_t[0:8] = lax.rsqrt(ex.finish() / D + epsilon)
    sc = wide_t[...].T
    for s in range(seqs):
        scales[s] = sc[s * 2 * span : (s + 1) * 2 * span]
    place = cut(e.t * 2 + e.p, wide)
    for s in range(seqs):
        for k, gain in enumerate((qgain, kgain)):
            unit = lin[k, s] * scales[s][:, k : k + 1]
            units[k, s] = unit
            scaled = unit * gain[:, place]
            for jj in range(heads):
                turned = turn(scaled[:, jj * HD : (jj + 1) * HD], ang[0, s], ang[1, s])
                qkvx[k, s, jj] = turned.astype(BF)
            to_heads(e, qkvx.at[k, s], qkvh.at[k, s], hsend.at[k, s], hrecv.at[k, s], heads, span)

    ws[3].relay()
    ws[4].relay()

    for s in range(seqs):
        for k in (2, 0, 1):
            wait_bytes(qkvh.at[k, s], hrecv.at[k, s])
        for i in range(e.nc):
            keys = (i + 1) * span
            kb = qkvh[1, s, 0 : i + 1].reshape(keys, HD)
            vb = qkvh[2, s, 0 : i + 1].reshape(keys, HD)
            scores = masked(dot(qkvh[0, s, i], kb, NT) * HD**-0.5, seg_col, seg_row, s, i, span)
            top = jnp.max(scores, axis=-1, keepdims=True)
            ex_s = jnp.exp(scores - top)
            total = jnp.sum(ex_s, axis=-1, keepdims=True)
            log_total = top + jnp.log(total)
            lse[s, i * span : (i + 1) * span, :] = jnp.broadcast_to(log_total, (span, HD))
            probs = (ex_s * (1.0 / total)).astype(BF)
            atth[s, i] = dot(probs, vb, NN).astype(BF)
        dst = att.at[s, own, cut(lax.rem(e.c, heads), HD)]
        from_heads(e, atth.at[s], dst, bsend.at[s], brecv.at[s], heads)
    for k, (a, b) in enumerate(((qkvh, qkv_heads), (atth, att_heads))):
        outs.append(pltpu.make_async_copy(a, b, osem.at[4 + k]))
        outs[-1].start()
    for s in range(seqs):
        wait_bytes(att.at[s], brecv.at[s])
        from_heads_drain(e, atth.at[s], bsend.at[s], heads)
        for k in range(3):
            to_heads_drain(e, qkvx.at[k, s], hsend.at[k, s], heads, span)
        gat[s].drain()
    angle_copy().wait_send()
    ws[3].wait()
    ws[4].wait()
    for w in ws:
        w.drain()
    for o in outs:
        o.wait()


def front_stage(
    sizes, tokens, cos_own, sin_own, qgain, kgain, seg_col, seg_row, wq, wk, wv, wo, gate
):
    nf, nc, nt = sizes
    seqs, rows, dm = tokens.shape
    wide = wq.shape[1] // 2
    heads = wide // HD
    full = 2 * nt * rows
    span = nt * rows
    sds = jax.ShapeDtypeStruct
    v, dma = pltpu.VMEM, pltpu.SemaphoreType.DMA
    return pl.pallas_call(
        functools.partial(front_kernel, sizes, seqs, rows),
        name="front_stage",
        out_shape=(
            sds((seqs, full, wide), BF),
            sds((seqs, full, dm), BF),
            sds((dm, wide), BF),
            sds((dm, wide), BF),
            sds((dm, wide), BF),
            sds((dm, wide), BF),
            sds((dm, gate.shape[1] // 4), BF),
            sds((2, seqs, full, wide), F32),
            sds((seqs, full, 128), F32),
            sds((2, seqs, full, HD), F32),
            sds((3, seqs, nc, span, HD), BF),
            sds((seqs, nc, span, HD), BF),
            sds((seqs, nc * span, HD), F32),
        ),
        in_specs=[VMEM_SPEC] * 7 + [HBM_SPEC] * 5,
        out_specs=(HBM_SPEC,) * 7 + (VMEM_SPEC,) * 3 + (HBM_SPEC,) * 2 + (VMEM_SPEC,),
        scratch_shapes=[
            v((seqs, full, dm), BF),
            v((dm, wide), BF),
            v((dm, wide), BF),
            v((dm, wide), BF),
            v((2, seqs, full, wide), F32),
            v((3, seqs, heads, full, HD), BF),
            v((3, seqs, nc, span, HD), BF),
            v((seqs, nc, span, HD), BF),
            v((8, seqs * full), F32),
            v((2 * nt, 8, seqs * full), F32),
            v((128, seqs * full), F32),
            v((2, seqs, full, HD), F32),
            dma((5, 4)),
            dma((seqs, 6, 2 * nt - 1)),
            dma((2,)),
            dma((2, 2 * nt)),
            dma((3, seqs, heads, 2)),
            dma((3, seqs)),
            dma((seqs, nc)),
            dma((seqs,)),
            dma((6,)),
        ],
        compiler_params=pltpu.CompilerParams(
            collective_id=2, has_side_effects=True, vmem_limit_bytes=60 << 20
        ),
    )(tokens, cos_own, sin_own, qgain, kgain, seg_col, seg_row, wq, wk, wv, wo, gate)


def tail_kernel(
    sizes, seqs, rows,
    hidden_grad, gains_in, units, scales, angles, qgain, kgain, seg_col, seg_row, lse,
    agh_in, qkv_heads, att_heads, xs_in, wq_in, wk_in, wv_in,
    wo_part, gate_part, up_part,
    input_grad, gains_out, in_q, in_k, in_v, in_o, in_g, in_u,
    agh, qkvh, atth, x, wq, wk, wv, dh, dx, acck, accv, uu, pre, part, pair, right, left, y,
    mine, inbox, wide_t, gmine, gin, gin2, p_o, p_g, p_u, f_q, f_k, f_v, f_o, f_g, f_u,
    lsem, dsend, drecv, esem, rsem, ssem, g1sem, g2sem,
):
    e = Place(*sizes)
    n = e.nt
    span = n * rows
    dm = x.shape[2]
    wide = wq.shape[1]
    heads = wide // HD
    scat = [
        Scatter(e, p, fi, b, ssem.at[k])
        for k, (p, fi, b) in enumerate(
            (
                (wq, f_q, in_q), (wk, f_k, in_k), (wv, f_v, in_v),
                (p_o, f_o, in_o), (p_g, f_g, in_g), (p_u, f_u, in_u),
            )
        )
    ]
    loads = [
        pltpu.make_async_copy(a, b, lsem.at[k])
        for k, (a, b) in enumerate(
            (
                (qkv_heads, qkvh), (agh_in, agh), (att_heads, atth), (wq_in, wq),
                (wk_in, wk), (wv_in, wv), (xs_in, x),
                (gate_part, p_g), (wo_part, p_o), (up_part, p_u),
            )
        )
    ]
    for ld in loads:
        ld.start()
    e.barrier()
    loads[7].wait()
    scat[4].start()
    loads[8].wait()
    scat[3].start()
    wide_t[...] = jnp.zeros_like(wide_t)
    for ld in loads[:3]:
        ld.wait()

    for s in range(seqs):
        acck[...] = jnp.zeros_like(acck)
        accv[...] = jnp.zeros_like(accv)
        for i in range(e.nc):
            keys = (i + 1) * span
            kb = qkvh[1, s, 0 : i + 1].reshape(keys, HD)
            vb = qkvh[2, s, 0 : i + 1].reshape(keys, HD)
            qb = qkvh[0, s, i]
            rowsl = pl.ds(i * span, span)
            scores = masked(dot(qb, kb, NT) * HD**-0.5, seg_col, seg_row, s, i, span)
            probs = jnp.exp(scores - lse[s, rowsl, 0:1])
            da = agh[s, i]
            accv[0:keys] += dot(probs.astype(BF), da, TN)
            delta = jnp.sum(da.astype(F32) * atth[s, i].astype(F32), axis=-1, keepdims=True)
            ds = (probs * (dot(da, vb, NT) - delta)).astype(BF)
            dh[0, s, i] = (dot(ds, kb, NN) * HD**-0.5).astype(BF)
            acck[0:keys] += dot(ds, qb, TN)
        dh[1, s] = (acck[...] * HD**-0.5).astype(BF).reshape(e.nc, span, HD)
        dh[2, s] = accv[...].astype(BF).reshape(e.nc, span, HD)
        own = pl.ds(pl.multiple_of(e.p * span, span), span)
        for k in range(3):
            dst = dx.at[k, s, lax.rem(e.c, heads), own, :]
            from_heads(e, dh.at[k, s], dst, dsend.at[k, s], drecv.at[k, s], heads)
    scat[4].relay()
    scat[3].relay()
    loads[9].wait()
    scat[5].start()

    place = cut(e.t * 2 + e.p, wide)
    gmine[...] = gains_in[...]
    gmine[0:2, :] = jnp.zeros((2, dm), F32)
    inner = [[], []]
    for s in range(seqs):
        for k in range(3):
            wait_bytes(dx.at[k, s], drecv.at[k, s])
        for k, gain in enumerate((qgain, kgain)):
            for jj in range(heads):
                lanes = slice(jj * HD, (jj + 1) * HD)
                g = turn_back(dx[k, s, jj].astype(F32), angles[0, s], angles[1, s])
                uu[k, s, :, lanes] = g
            g = uu[k, s]
            unit = units[k, s]
            gmine[k : k + 1, place] += jnp.sum(g * unit, axis=0, keepdims=True)
            u = g * gain[:, place]
            uu[k, s] = u
            inner[k].append(jnp.sum(u * unit, axis=-1, keepdims=True))
        for jj in range(heads):
            pre[2, s, :, jj * HD : (jj + 1) * HD] = dx[2, s, jj]
    mine[...] = columns(*[jnp.concatenate(v, axis=0) for v in inner])
    ex = Exchange(e, mine, inbox, esem.at[0], esem.at[1], *Exchange.heads(e))
    ex.start()
    gx = Exchange(e, gmine, gin, g1sem.at[0], g1sem.at[1], *Exchange.plane(e))
    gx.start()
    for ld in loads[3:7]:
        ld.wait()
    wide_t[0:8] = ex.finish() / D
    cols = wide_t[...].T
    for s in range(seqs):
        for k in range(2):
            mean = cols[s * 2 * span : (s + 1) * 2 * span, k : k + 1]
            v = scales[s][:, k : k + 1] * (uu[k, s] - units[k, s] * mean)
            pre[k, s] = v.astype(BF)

    tile = 512
    red = [
        Reduce(e, part.at[s], pair.at[s], right.at[s], left.at[s], rsem.at[s], rows)
        for s in range(seqs)
    ]
    for s in range(seqs):

        def step(i, s=s):
            sl = cut(i, tile)
            total = dot(pre[0, s], wq[sl, :], NT) + dot(pre[1, s], wk[sl, :], NT)
            part[s, :, sl] = (total + dot(pre[2, s], wv[sl, :], NT)).astype(BF)

        loop(dm // tile, step)
        red[s].pair_send()
    for s in range(seqs):
        red[s].pair_add()
        red[s].slot(-1)
    for k, w in enumerate((wq, wk, wv)):

        def step(i, k=k, w=w):
            sl = cut(i, tile)
            lhs = x[:, :, sl].reshape(-1, tile)
            w[sl, :] = dot(lhs, pre[k].reshape(-1, wide), TN).astype(BF)

        loop(dm // tile, step)
        scat[k].start()
        for s in range(seqs):
            red[s].slot(k)
        if k == 0:
            scat[5].relay()
    for j in range(3, n - 1):
        for s in range(seqs):
            red[s].slot(j)
    gmine[...] = gx.finish()
    gx2 = Exchange(e, gmine, gin2, g2sem.at[0], g2sem.at[1], *Exchange.line(e))
    gx2.start()
    for k in range(3):
        scat[k].relay()
    for s in range(seqs):
        red[s].result(y)
        input_grad[s] = hidden_grad[s] + y[...]
    gains_out[...] = gx2.finish()
    for sc in scat:
        sc.wait()
        sc.drain()
    for s in range(seqs):
        red[s].drain()
        for k in range(3):
            from_heads_drain(e, dh.at[k, s], dsend.at[k, s], heads)


def tail_stage(sizes, *args):
    nf, nc, nt = sizes
    hidden_grad, xs, gate_part, wo_part = args[0], args[13], args[18], args[17]
    seqs, rows, dm = hidden_grad.shape
    half, wide = gate_part.shape[1], wo_part.shape[1]
    heads = wide // HD
    full = 2 * nt * rows
    span = nt * rows
    sds = jax.ShapeDtypeStruct
    v, dma = pltpu.VMEM, pltpu.SemaphoreType.DMA
    small, small_terms = scatter_shapes(sizes, dm, wide)
    large, large_terms = scatter_shapes(sizes, dm, half)
    return pl.pallas_call(
        functools.partial(tail_kernel, sizes, seqs, rows),
        name="tail_stage",
        out_shape=(sds((seqs, rows, dm), F32), sds((8, dm), F32))
        + (sds(small_terms, BF),) * 4
        + (sds(large_terms, BF),) * 2,
        in_specs=[VMEM_SPEC] * 10 + [HBM_SPEC] * 10,
        out_specs=(VMEM_SPEC,) * 2 + (HBM_SPEC,) * 6,
        scratch_shapes=[
            v((seqs, nc, span, HD), BF),
            v((3, seqs, nc, span, HD), BF),
            v((seqs, nc, span, HD), BF),
            v((seqs, full, dm), BF),
            v((dm, wide), BF),
            v((dm, wide), BF),
            v((dm, wide), BF),
            v((3, seqs, nc, span, HD), BF),
            v((3, seqs, heads, full, HD), BF),
            v((nc * span, HD), F32),
            v((nc * span, HD), F32),
            v((2, seqs, full, wide), F32),
            v((3, seqs, full, wide), BF),
            v((seqs, full, dm), BF),
            v((seqs, nt * rows, dm), BF),
            v((seqs, nt - 1, rows, dm), BF),
            v((seqs, nt - 1, rows, dm), BF),
            v((rows, dm), F32),
            v((8, seqs * full), F32),
            v((2 * nt, 8, seqs * full), F32),
            v((128, seqs * full), F32),
            v((8, dm), F32),
            v((nf * nc, 8, dm), F32),
            v((nt, 8, dm), F32),
            v((dm, wide), BF),
            v((dm, half), BF),
            v((dm, half), BF),
            v(small, BF),
            v(small, BF),
            v(small, BF),
            v(small, BF),
            v(large, BF),
            v(large, BF),
            dma((10,)),
            dma((3, seqs, nc)),
            dma((3, seqs)),
            dma((2, 2 * nt)),
            dma((seqs, 4, nt)),
            dma((6, 4)),
            dma((2, nf * nc)),
            dma((2, nt)),
        ],
        compiler_params=pltpu.CompilerParams(
            collective_id=3, has_side_effects=True, vmem_limit_bytes=63 << 20
        ),
    )(*args)


def body(
    tokens, segments, positions, query_weight, key_weight, value_weight, output_weight,
    gate_weight, up_projection_weight, down_weight, query_gain, key_gain, attention_gain,
    feedforward_gain, cotangent,
):
    sizes = (lax.axis_size("fsdp"), lax.axis_size("ctx"), lax.axis_size("tensor"))
    seqs, rows, _ = tokens.shape
    span = sizes[2] * rows
    block_pos = lax.dynamic_slice_in_dim(positions, lax.axis_index("ctx") * span, span, 1)
    cosine, sine = rope_tables(block_pos)
    cos_own = jnp.concatenate([cosine, cosine], axis=-1)
    sin_own = jnp.concatenate([-sine, sine], axis=-1)
    seg_col = segments[:, :, None]
    seg_row = segments[:, None, :]
    qgain, kgain = query_gain[None], key_gain[None]
    (
        att, xs, wq, wk, wv, wo, gate, units, scales, angles, qkv_heads, att_heads, lse,
    ) = front_stage(
        sizes, tokens, cos_own, sin_own, qgain, kgain, seg_col, seg_row,
        query_weight, key_weight, value_weight, output_weight, gate_weight,
    )
    block_out, hidden_grad, agh, wo_part, gate_part, up_part, down_terms, gains = ffn_stage(
        sizes, att, wo, gate, gate_weight, up_projection_weight, down_weight,
        tokens, cotangent, attention_gain[None], feedforward_gain[None],
    )
    input_grad, gain_sums, *terms = tail_stage(
        sizes, hidden_grad, gains, units, scales, angles, qgain, kgain, seg_col, seg_row, lse,
        agh, qkv_heads, att_heads, xs, wq, wk, wv, wo_part, gate_part, up_part,
    )
    weight_grads = [jnp.sum(x.astype(F32), axis=0) for x in (*terms, down_terms)]
    return (block_out, input_grad, *weight_grads, *(gain_sums[k] for k in range(4)))


def solution(mesh):
    in_specs = (
        P("fsdp", ("ctx", "tensor"), None),
        P("fsdp", None),
        P("fsdp", None),
        P(("fsdp", "ctx"), "tensor"),
        P(("fsdp", "ctx"), "tensor"),
        P(("fsdp", "ctx"), "tensor"),
        P(("fsdp", "ctx"), "tensor"),
        P(("fsdp", "ctx"), "tensor"),
        P(("fsdp", "ctx"), "tensor"),
        P(("fsdp", "ctx"), "tensor"),
        P(),
        P(),
        P(),
        P(),
        P("fsdp", ("ctx", "tensor"), None),
    )
    out_specs = (
        P("fsdp", ("ctx", "tensor"), None),
        P("fsdp", ("ctx", "tensor"), None),
        P(("fsdp", "ctx"), "tensor"),
        P(("fsdp", "ctx"), "tensor"),
        P(("fsdp", "ctx"), "tensor"),
        P(("fsdp", "ctx"), "tensor"),
        P(("fsdp", "ctx"), "tensor"),
        P(("fsdp", "ctx"), "tensor"),
        P(("fsdp", "ctx"), "tensor"),
        P(),
        P(),
        P(),
        P(),
    )
    return jax.shard_map(body, mesh=mesh, in_specs=in_specs, out_specs=out_specs, check_vma=False)
```

```python
import functools

import jax
import jax.numpy as jnp
from jax import lax
from jax.experimental import pallas as pl
from jax.experimental.pallas import tpu as pltpu
from jax.sharding import PartitionSpec as P

D = 2048
HD = 128


epsilon = 1e-06
rope_theta = 500000.0
masked_score = -1e30


def rope_tables(position_ids):
    freq_index = jnp.arange(HD // 2, dtype=jnp.float32)
    inverse = rope_theta ** (-2.0 * freq_index / HD)
    angles = position_ids.astype(jnp.float32)[..., None] * inverse
    return (jnp.cos(angles), jnp.sin(angles))


MESH = pl.DeviceIdType.MESH
BF = jnp.bfloat16
F32 = jnp.float32
VMEM_SPEC = pl.BlockSpec(memory_space=pltpu.VMEM)
HBM_SPEC = pl.BlockSpec(memory_space=pltpu.HBM)
NN = (((1,), (0,)), ((), ()))
NT = (((1,), (1,)), ((), ()))
TN = (((0,), (0,)), ((), ()))


def dot(a, b, dims):
    return lax.dot_general(a, b, dims, preferred_element_type=F32)


def loop(count, step):
    def run(i, carry):
        step(i)
        return carry

    lax.fori_loop(0, count, run, 0)


def cut(i, size):
    return pl.ds(pl.multiple_of(i * size, size), size)


def both(*conds):
    out = True
    for cond in conds:
        if isinstance(cond, bool):
            if not cond:
                return False
        elif isinstance(out, bool):
            out = cond
        else:
            out = jnp.logical_and(out, cond)
    return out


def when(cond, step):
    if isinstance(cond, bool):
        if cond:
            step()
    else:
        pl.when(cond)(step)


class Place:
    def __init__(self, fsdp_size, ctx_size, tensor_size):
        self.nf, self.nc, self.nt = fsdp_size, ctx_size, tensor_size
        self.f = lax.axis_index("fsdp")
        self.c = lax.axis_index("ctx")
        self.t = lax.axis_index("tensor")
        self.p = lax.rem(self.f, 2)
        self.group = self.f - self.p
        self.mate = self.group + 1 - self.p

    def at(self, f=None, c=None, t=None):
        return {
            "fsdp": self.f if f is None else f,
            "ctx": self.c if c is None else c,
            "tensor": self.t if t is None else t,
        }

    def plane(self):
        out = []
        for dg in range(self.nf // 2):
            for dc in (3, 1, 2, 0) if self.nc == 4 else range(self.nc):
                for dp in (0, 1):
                    if dg or dc or dp:
                        out.append((dg, dc, dp))
        return out

    def peer(self, off):
        dg, dc, dp = off
        group = lax.rem(self.group + 2 * dg, self.nf)
        core = self.p + dp - 2 * self.p * dp
        return group + core, core, jnp.bitwise_xor(self.c, dc)

    def barrier(self):
        sem = pltpu.get_barrier_semaphore()

        def signal(**place):
            pl.semaphore_signal(sem, inc=1, device_id=self.at(**place), device_id_type=MESH)

        offs = self.plane()
        for off in offs:
            f, _, c = self.peer(off)
            signal(f=f, c=c)
        for dt in range(1, self.nt):
            for core in range(2):
                signal(f=self.group + core, t=lax.rem(self.t + dt, self.nt))
        pl.semaphore_wait(sem, len(offs) + 2 * (self.nt - 1))


def remote(src, dst, send, recv, device):
    return pltpu.make_async_remote_copy(
        src_ref=src, dst_ref=dst, send_sem=send, recv_sem=recv, device_id=device, device_id_type=MESH
    )


def wait_bytes(ref, sem):
    pltpu.make_async_copy(ref, ref, sem).wait()


class Reduce:
    def __init__(self, e, part, pair, right, left, sems, rows):
        self.e, self.part, self.pair, self.right, self.left, self.rows = e, part, pair, right, left, rows
        self.sems = sems

    def half(self, p):
        n = self.e.nt * self.rows
        return self.part.at[pl.ds(pl.multiple_of(p * n, n), n), :]

    def block(self, b):
        return self.part.at[cut(self.e.p * self.e.nt + b, self.rows), :]

    def _pair(self):
        return remote(
            self.half(1 - self.e.p), self.pair, self.sems.at[0, 0], self.sems.at[1, 0],
            self.e.at(f=self.e.mate),
        )

    def _side(self, b, k, up):
        e = self.e
        buf, row = (self.right, 0) if up else (self.left, 2)
        return remote(
            self.block(b), buf.at[k], self.sems.at[row, 1 + k], self.sems.at[row + 1, 1 + k],
            e.at(t=e.t + 1 if up else e.t - 1),
        )

    def pair_send(self):
        self._pair().start()

    def pair_add(self):
        self._pair().wait_recv()
        mine = self.half(self.e.p)

        def step(i):
            sl = cut(i, self.rows)
            mine[sl, :] = (mine[sl, :].astype(F32) + self.pair[sl, :].astype(F32)).astype(BF)

        loop(self.e.nt, step)

    def slot(self, j):
        e, n = self.e, self.e.nt
        for up in (True, False):
            b = e.t + (n - 2) - j if up else e.t - (n - 2) + j
            near = e.t > 0 if up else e.t < n - 1
            far = e.t < n - 1 if up else e.t > 0
            inside = b <= n - 1 if up else b >= 0
            buf = self.right if up else self.left

            def take(b=b, buf=buf, up=up):
                self._side(b, j, up).wait_recv()

                def add():
                    blk = self.block(b)
                    blk[...] = (blk[...].astype(F32) + buf[j].astype(F32)).astype(BF)

                when(j < n - 2, add)

            when(both(j >= 0, j <= n - 2, near, inside), take)
            when(both(j < n - 2, far, inside), lambda b=b, up=up: self._side(b, j + 1, up).start())

    def result(self, out):
        e, n = self.e, self.e.nt
        out[...] = self.block(e.t)[...].astype(F32)

        def add_right():
            out[...] += self.right[n - 2].astype(F32)

        def add_left():
            out[...] += self.left[n - 2].astype(F32)

        when(e.t > 0, add_right)
        when(e.t < n - 1, add_left)

    def drain(self):
        e, n = self.e, self.e.nt
        self._pair().wait_send()

        def step(i):
            j = i - 1
            for up in (True, False):
                b = e.t + (n - 2) - j if up else e.t - (n - 2) + j
                far = e.t < n - 1 if up else e.t > 0
                inside = b <= n - 1 if up else b >= 0
                when(both(far, inside), lambda b=b, up=up: self._side(b, j + 1, up).wait_send())

        for i in range(n - 1):
            step(i)


class Gather:
    def __init__(self, e, full, sems, rows):
        self.e, self.full, self.sems, self.rows = e, full, sems, rows

    def block(self, p, b):
        return self.full.at[cut(p * self.e.nt + b, self.rows), :]

    def _side(self, b, k, up):
        e = self.e
        row = 0 if up else 2
        ref = self.block(e.p, b)
        return remote(
            ref, ref, self.sems.at[row, k], self.sems.at[row + 1, k],
            e.at(t=e.t + 1 if up else e.t - 1),
        )

    def _pair(self, b, k, incoming):
        e = self.e
        ref = self.block(1 - e.p if incoming else e.p, b)
        return remote(ref, ref, self.sems.at[4, k], self.sems.at[5, k], e.at(f=e.mate))

    def init(self):
        e, n = self.e, self.e.nt
        when(e.t < n - 1, lambda: self._side(e.t, 0, True).start())
        when(e.t > 0, lambda: self._side(e.t, 0, False).start())
        self._pair(e.t, 0, False).start()

    def slot(self, j):
        e, n = self.e, self.e.nt
        for up in (True, False):
            b = e.t - 1 - j if up else e.t + 1 + j
            inside = b >= 0 if up else b <= n - 1
            far = e.t < n - 1 if up else e.t > 0
            k = 1 + j if up else n + j

            def take(b=b, up=up, far=far, k=k):
                self._side(b, j, up).wait_recv()
                when(both(far, j < n - 2), lambda: self._side(b, j + 1, up).start())
                self._pair(b, k, False).start()

            when(both(j >= 0, j <= n - 2, inside), take)

    def _rest(self, step_pair):
        e, n = self.e, self.e.nt
        step_pair(e.t, 0)
        for j in range(n - 1):
            when(e.t - 1 - j >= 0, lambda j=j: step_pair(e.t - 1 - j, 1 + j))
            when(e.t + 1 + j <= n - 1, lambda j=j: step_pair(e.t + 1 + j, n + j))

    def done(self):
        self._rest(lambda b, k: self._pair(b, k, True).wait_recv())

    def drain(self):
        e, n = self.e, self.e.nt
        self._rest(lambda b, k: self._pair(b, k, False).wait_send())
        when(e.t < n - 1, lambda: self._side(e.t, 0, True).wait_send())
        when(e.t > 0, lambda: self._side(e.t, 0, False).wait_send())
        for j in range(n - 2):
            when(
                both(e.t - 1 - j >= 0, e.t < n - 1),
                lambda j=j: self._side(e.t - 1 - j, j + 1, True).wait_send(),
            )
            when(
                both(e.t + 1 + j <= n - 1, e.t > 0),
                lambda j=j: self._side(e.t + 1 + j, j + 1, False).wait_send(),
            )


SPLIT = 2


def parts_of(width):
    size = width // SPLIT
    return [pl.ds(u * size, size) for u in range(SPLIT)]


class Both:
    def __init__(self, each):
        self.each = list(each)

    def __getattr__(self, name):
        def call(*args):
            for x in self.each:
                getattr(x, name)(*args)

        return call


class Weight:
    def __init__(self, e, shard, full, sems, off=0):
        self.e, self.shard, self.full, self.sems, self.off = e, shard, full, sems, off
        self.rows, self.width = shard.shape[0], full.shape[1]
        self.stride = shard.shape[1] // 2

    def columns(self, core):
        start = pl.multiple_of(core * self.stride + self.off, 128)
        return self.shard.at[:, pl.ds(start, self.width)]

    def some(self, count):
        return self.full.at[pl.ds(0, count * self.rows), :]

    def targets(self):
        e = self.e
        if e.nf == 2:
            return [(0, 1, 0), (0, 2, 0), (0, 1, 1), (0, 2, 1), (0, 0, 1)]
        return e.plane()

    def start(self):
        e = self.e
        dst = self.full.at[cut(e.f * e.nc + e.c, self.rows), :]
        for off in self.targets():
            f, core, c = e.peer(off)
            remote(self.columns(core), dst, self.sems.at[0], self.sems.at[1], e.at(f=f, c=c)).start()
        pltpu.make_async_copy(self.columns(e.p), dst, self.sems.at[1]).start()

    def relay(self):
        e = self.e
        wait_bytes(self.some(len(self.targets()) + 1), self.sems.at[1])
        if e.nf != 2:
            return
        part = self.rows // 2
        for f in range(2):
            for k, (source, target) in enumerate(((1, 2), (2, 1))):
                row = (f * e.nc + jnp.bitwise_xor(e.c, source)) * self.rows + k * part
                ref = self.full.at[pl.ds(pl.multiple_of(row, part), part), :]
                device = e.at(c=jnp.bitwise_xor(e.c, target))
                remote(ref, ref, self.sems.at[2], self.sems.at[3], device).start()

    def wait(self):
        if self.e.nf == 2:
            wait_bytes(self.some(2), self.sems.at[3])

    def drain(self):
        wait_bytes(self.some(len(self.targets())), self.sems.at[0])
        if self.e.nf == 2:
            wait_bytes(self.some(2), self.sems.at[2])


class Scatter:
    def __init__(self, e, part, first, inbox, sems):
        self.e, self.part, self.first, self.inbox, self.sems = e, part, first, inbox, sems
        self.rows, self.half = inbox.shape[1], part.shape[1]
        self.upper = self.rows // 2

    def piece(self, f, c, side=None):
        row = (f * self.e.nc + c) * self.rows
        if side is None:
            return self.part.at[pl.ds(pl.multiple_of(row, self.rows), self.rows), :]
        row = pl.multiple_of(row + side * self.upper, self.upper)
        return self.part.at[pl.ds(row, self.upper), :]

    def start(self):
        e = self.e
        if e.nf == 2:
            for side in range(2):
                near = jnp.bitwise_xor(e.c, 1 + side)
                for k, owner in enumerate((near, jnp.bitwise_xor(e.c, 3))):
                    for f in range(2):
                        remote(
                            self.piece(f, owner, side), self.first.at[side, k, f],
                            self.sems.at[0], self.sems.at[1], e.at(c=near),
                        ).start()
            return
        slot = lax.div(e.group, 2) * e.nc + e.c
        dst = self.inbox.at[slot, :, cut(e.p, self.half)]
        for off in e.plane():
            f, _, c = e.peer(off)
            remote(
                self.piece(f, c), dst, self.sems.at[2], self.sems.at[3], e.at(f=f, c=c)
            ).start()
        pltpu.make_async_copy(self.piece(e.f, e.c), dst, self.sems.at[3]).start()

    def relay(self):
        e = self.e
        if e.nf != 2:
            return
        wait_bytes(self.first, self.sems.at[1])
        lanes = cut(e.p, self.half)
        for side in range(2):
            far = jnp.bitwise_xor(e.c, 2 - side)
            for k, owner in enumerate((e.c, far)):
                for f in range(2):
                    mine = self.piece(f, owner, side)
                    got = self.first[side, k, f].astype(F32)
                    mine[...] = (mine[...].astype(F32) + got).astype(BF)
            for f in range(2):
                dst = self.inbox.at[1, pl.ds(side * self.upper, self.upper), lanes]
                remote(
                    self.piece(f, far, side), dst, self.sems.at[2], self.sems.at[3],
                    e.at(f=f, c=far),
                ).start()
        dst = self.inbox.at[0, :, lanes]
        remote(
            self.piece(1 - e.p, e.c), dst, self.sems.at[2], self.sems.at[3], e.at(f=e.mate)
        ).start()
        pltpu.make_async_copy(self.piece(e.p, e.c), dst, self.sems.at[3]).start()

    def wait(self):
        wait_bytes(self.inbox, self.sems.at[3])

    def drain(self):
        e = self.e
        count = 3 if e.nf == 2 else len(e.plane())
        wait_bytes(self.part.at[pl.ds(0, count * self.rows), :], self.sems.at[2])
        if e.nf == 2:
            wait_bytes(self.part.at[pl.ds(0, 4 * self.rows), :], self.sems.at[0])


def scatter_shapes(sizes, dm, half):
    nf, nc, _ = sizes
    rb = dm // (nf * nc)
    if nf == 2:
        return (2, 2, 2, rb // 2, half), (2, rb, 2 * half)
    return (1, 1, 1, 16, 128), (nf // 2 * nc, rb, 2 * half)


def ffn_kernel(
    sizes, seqs, rows,
    att, wo_in, gate_in, gate_sh, up_sh, down_sh, tokens, cot, again, fgain,
    block_out, hidden_grad, agh, wo_part, gate_terms, up_part, down_terms, gains,
    wo_v, g_v, u_v, d_v, part, pair, right, left, hid, mgr, agr, aa, bb, mixed,
    unit1, hid32, scale1, scratch_y, agx, first, first_g,
    wsem, lsem, dsem, rsem, gsem, xsend, xrecv, osem,
):
    e = Place(*sizes)
    dm = tokens.shape[2]
    half = g_v.shape[1]
    wide = att.shape[2]
    heads = wide // HD
    early = gate_in.shape[1]
    late = g_v.at[:, pl.ds(early, half - early)]
    w_g = Weight(e, gate_sh, late, wsem.at[0], off=early)
    w_u = Weight(e, up_sh, u_v, wsem.at[1])
    w_d = Weight(e, down_sh, d_v, wsem.at[2])
    load_o = pltpu.make_async_copy(wo_in, wo_v, lsem.at[0])
    load_g = pltpu.make_async_copy(gate_in, g_v.at[:, pl.ds(0, early)], lsem.at[1])
    load_o.start()
    load_g.start()
    scat_d = Scatter(e, d_v, first, down_terms, dsem.at[0])
    scat_g = Scatter(e, g_v, first_g, gate_terms, dsem.at[1])

    def reduce(k, s):
        return Both(
            Reduce(
                e, part.at[s, :, cl], pair.at[s, :, cl], right.at[s, :, :, cl],
                left.at[s, :, :, cl], rsem.at[k, s, u], rows,
            )
            for u, cl in enumerate(parts_of(dm))
        )

    def gather(k, s):
        full = (hid, mgr, agr)[k]
        return Both(
            Gather(e, full.at[s, :, cl], gsem.at[k, s, u], rows)
            for u, cl in enumerate(parts_of(dm))
        )

    def own_rows(k, s):
        return (hid, mgr, agr)[k].at[s, cut(e.p * e.nt + e.t, rows), :]

    def result(k, s, out):
        for r, cl in zip(red[k][s].each, parts_of(dm)):
            r.result(out.at[:, cl])

    red = [[reduce(k, s) for s in range(seqs)] for k in range(3)]
    gat = [[gather(k, s) for s in range(seqs)] for k in range(3)]

    e.barrier()
    w_g.start()
    w_u.start()
    gains[...] = jnp.zeros_like(gains)

    tile = 512

    def out_tiles(s):
        def step(i):
            sl = cut(i, tile)
            part[s, :, sl] = dot(att[s], wo_v[sl, :], NT).astype(BF)

        loop(dm // tile, step)

    def norm1(s):
        y = scratch_y
        result(0, s, y)
        v = y[...]
        scale = lax.rsqrt(jnp.mean(v * v, axis=-1, keepdims=True) + epsilon)
        unit = v * scale
        unit1[s] = unit
        scale1[s] = jnp.broadcast_to(scale, scale1.shape[1:])
        h = tokens[s].astype(F32) + unit * again[...]
        hid32[s] = h
        own_rows(0, s)[...] = h.astype(BF)

    def ffn_tile(s, i):
        sl = cut(i, 256)
        gate = dot(hid[s], g_v[:, sl], NN)
        up = dot(hid[s], u_v[:, sl], NN)
        sig = jax.nn.sigmoid(gate)
        act = gate * sig
        mixed[s, :, sl] = (act * up).astype(BF)
        aa[s, :, sl] = (up * sig * (1.0 + gate * (1.0 - sig))).astype(BF)
        bb[s, :, sl] = act.astype(BF)

    ffn_tiles = half // 256

    def down_tiles(s):
        def step(i):
            sl = cut(i, tile)
            part[s, :, sl] = dot(mixed[s], d_v[sl, :], NT).astype(BF)

        loop(dm // tile, step)

    def norm2(s):
        y = scratch_y
        result(1, s, y)
        v = y[...]
        scale = lax.rsqrt(jnp.mean(v * v, axis=-1, keepdims=True) + epsilon)
        unit = v * scale
        block_out[s] = (hid32[s] + unit * fgain[...]).astype(BF)
        upstream = cot[s].astype(F32)
        gains[3:4, :] += jnp.sum(upstream * unit, axis=0, keepdims=True)
        g = upstream * fgain[...]
        m = scale * (g - unit * jnp.mean(g * unit, axis=-1, keepdims=True))
        own_rows(1, s)[...] = m.astype(BF)

    def inner_tiles(s):
        def step(i):
            sl = cut(i, 256)
            inner = dot(mgr[s], d_v[:, sl], NN)
            aa[s, :, sl] = (inner * aa[s, :, sl].astype(F32)).astype(BF)
            bb[s, :, sl] = (inner * bb[s, :, sl].astype(F32)).astype(BF)

        loop(ffn_tiles, step)

    def back_tiles(s):
        def step(i):
            sl = cut(i, tile)
            part[s, :, sl] = (dot(aa[s], g_v[sl, :], NT) + dot(bb[s], u_v[sl, :], NT)).astype(BF)

        loop(dm // tile, step)

    def norm3(s):
        y = scratch_y
        result(2, s, y)
        hg = cot[s].astype(F32) + y[...]
        hidden_grad[s] = hg
        unit = unit1[s]
        gains[2:3, :] += jnp.sum(hg * unit, axis=0, keepdims=True)
        g = hg * again[...]
        scale = scale1[s][:, 0:1]
        a = scale * (g - unit * jnp.mean(g * unit, axis=-1, keepdims=True))
        own_rows(2, s)[...] = a.astype(BF)

    def weight_tile(left_rows, right_rows, out, i, width):
        per = out.shape[1] // width
        sl, cl = cut(lax.div(i, per), tile), cut(lax.rem(i, per), width)
        lhs = left_rows[:, :, sl].reshape(-1, tile)
        rhs = right_rows[:, :, cl].reshape(-1, width)
        out[sl, cl] = dot(lhs, rhs, TN).astype(BF)

    n = e.nt
    span = agh.shape[2]

    def heads_copy(s, jj, q):
        src = agx.at[s, jj, pl.ds(q * span, span), :]
        dst = agh.at[s, e.c]
        return src, dst

    def heads_grad(s):
        r = dot(agr[s], wo_v[...], NN).astype(BF)
        for jj in range(heads):
            agx[s, jj] = r[:, jj * HD : (jj + 1) * HD]
        for jj in range(heads):
            head = heads * e.p + jj
            for q in range(2):
                src, dst = heads_copy(s, jj, q)
                self_here = both(head == e.c, q == e.p)

                def local(src=src, dst=dst):
                    pltpu.make_async_copy(src, dst, xrecv.at[s]).start()

                def away(src=src, dst=dst, q=q, head=head, jj=jj):
                    remote(
                        src, dst, xsend.at[s, jj, q], xrecv.at[s], e.at(f=e.group + q, c=head)
                    ).start()

                when(self_here, local)
                when(jnp.logical_not(self_here), away)

    def heads_wait(s):
        wait_bytes(agh.at[s], xrecv.at[s])
        block = agx.at[s, 0, pl.ds(0, span), :]
        for jj in range(heads):
            head = heads * e.p + jj
            for q in range(2):
                when(
                    jnp.logical_not(both(head == e.c, q == e.p)),
                    lambda jj=jj, q=q: wait_bytes(block, xsend.at[s, jj, q]),
                )

    load_o.wait()
    out_tiles(0)
    red[0][0].pair_send()
    out_tiles(1)
    red[0][0].pair_add()
    red[0][1].pair_send()

    def step(i):
        red[0][0].slot(i - 1)

    loop(n, step)
    red[0][1].pair_add()
    norm1(0)
    gat[0][0].init()

    def step(i):
        red[0][1].slot(i - 1)
        gat[0][0].slot(i - 1)

    loop(2, step)
    w_g.relay()
    w_u.relay()
    w_d.start()
    loop(n - 2, lambda i: step(i + 2))
    gat[0][0].done()
    norm1(1)
    gat[0][1].init()
    load_g.wait()
    w_g.wait()
    w_u.wait()

    def step(i):
        ffn_tile(0, i)
        gat[0][1].slot(i)

    loop(ffn_tiles, step)
    w_d.relay()
    w_d.wait()
    red[0][0].drain()
    down_tiles(0)
    red[1][0].pair_send()
    gat[0][1].done()
    ffn_tile(1, 0)
    red[1][0].pair_add()

    def step(i):
        red[1][0].slot(i - 1)
        ffn_tile(1, i + 1)

    loop(ffn_tiles - 1, step)
    for j in range(ffn_tiles - 2, n - 1):
        red[1][0].slot(j)
    norm2(0)
    gat[1][0].init()
    red[0][1].drain()
    down_tiles(1)
    red[1][1].pair_send()
    gat[1][0].slot(0)
    red[1][1].pair_add()

    def step(i):
        red[1][1].slot(i - 1)
        gat[1][0].slot(i + 1)

    loop(n, step)
    norm2(1)
    gat[1][1].init()
    gat[1][0].done()
    inner_tiles(0)
    red[1][0].drain()
    back_tiles(0)
    red[2][0].pair_send()
    gat[1][1].slot(0)
    red[2][0].pair_add()

    def step(i):
        red[2][0].slot(i - 1)
        gat[1][1].slot(i + 1)

    loop(n - 2, step)
    gat[1][1].done()
    inner_tiles(1)
    red[2][0].slot(n - 3)
    red[1][1].drain()
    back_tiles(1)
    red[2][1].pair_send()
    red[2][0].slot(n - 2)
    norm3(0)
    gat[2][0].init()
    red[2][1].pair_add()
    red[2][1].slot(-1)
    tiles = (dm // tile) * (half // tile)
    share = -(-tiles // (n - 1))

    def fill(left_rows, right_rows, out, i):
        def go(k):
            which = share * i + k
            when(which < tiles, lambda: weight_tile(left_rows, right_rows, out, which, tile))

        loop(share, go)

    for w in (w_g, w_u, w_d):
        w.drain()
    loop(tiles, lambda i: weight_tile(mgr, mixed, d_v, i, tile))
    scat_d.start()

    def step(i):
        red[2][1].slot(i)
        gat[2][0].slot(i)
        fill(hid, aa, g_v, i)

    loop(n - 1, step)
    scat_g.start()
    norm3(1)
    gat[2][1].init()
    gat[2][0].done()
    heads_grad(0)
    scat_d.relay()

    def step(i):
        gat[2][1].slot(i)
        fill(hid, bb, u_v, i)

    loop(n - 1, step)
    out_u = pltpu.make_async_copy(u_v, up_part, osem.at[2])
    out_u.start()
    gat[2][1].done()
    heads_grad(1)
    scat_g.relay()
    loop(dm // tile, lambda i: weight_tile(agr, att, wo_v, i, wide))
    out_o = pltpu.make_async_copy(wo_v, wo_part, osem.at[3])
    out_o.start()
    heads_wait(0)
    heads_wait(1)
    red[2][0].drain()
    red[2][1].drain()
    for k in range(3):
        for s in range(seqs):
            gat[k][s].drain()
    for sc in (scat_d, scat_g):
        sc.wait()
        sc.drain()
    for o in (out_u, out_o):
        o.wait()


def ffn_stage(
    sizes, att, wo_in, gate_in, gate_sh, up_sh, down_sh, tokens, cot, again, fgain
):
    nf, nc, nt = sizes
    seqs, rows, dm = tokens.shape
    half = gate_sh.shape[1] // 2
    wide = wo_in.shape[1]
    first, terms = scatter_shapes(sizes, dm, half)
    full = 2 * nt * rows
    sds = jax.ShapeDtypeStruct
    v, dma = pltpu.VMEM, pltpu.SemaphoreType.DMA
    return pl.pallas_call(
        functools.partial(ffn_kernel, sizes, seqs, rows),
        name="ffn_stage",
        out_shape=(
            sds((seqs, rows, dm), BF),
            sds((seqs, rows, dm), F32),
            sds((seqs, nc, nt * rows, HD), BF),
            sds((dm, wide), BF),
            sds(terms, BF),
            sds((dm, half), BF),
            sds(terms, BF),
            sds((8, dm), F32),
        ),
        in_specs=[VMEM_SPEC] + [HBM_SPEC] * 5 + [VMEM_SPEC] * 4,
        out_specs=(VMEM_SPEC, VMEM_SPEC) + (HBM_SPEC,) * 5 + (VMEM_SPEC,),
        scratch_shapes=[
            v((dm, wide), BF),
            v((dm, half), BF),
            v((dm, half), BF),
            v((dm, half), BF),
            v((seqs, full, dm), BF),
            v((seqs, nt * rows, dm), BF),
            v((seqs, nt - 1, rows, dm), BF),
            v((seqs, nt - 1, rows, dm), BF),
            v((seqs, full, dm), BF),
            v((seqs, full, dm), BF),
            v((seqs, full, dm), BF),
            v((seqs, full, half), BF),
            v((seqs, full, half), BF),
            v((seqs, full, half), BF),
            v((seqs, rows, dm), F32),
            v((seqs, rows, dm), F32),
            v((seqs, rows, 128), F32),
            v((rows, dm), F32),
            v((seqs, wide // HD, full, HD), BF),
            v(first, BF),
            v(first, BF),
            dma((3, 4)),
            dma((2,)),
            dma((2, 4)),
            dma((3, seqs, SPLIT, 4, nt)),
            dma((3, seqs, SPLIT, 6, 2 * nt - 1)),
            dma((seqs, wide // HD, 2)),
            dma((seqs,)),
            dma((4,)),
        ],
        compiler_params=pltpu.CompilerParams(
            collective_id=1, has_side_effects=True, vmem_limit_bytes=63 << 20
        ),
    )(att, wo_in, gate_in, gate_sh, up_sh, down_sh, tokens, cot, again, fgain)


class Exchange:
    def __init__(self, e, mine, inbox, send, recv, members, own):
        self.e, self.mine, self.inbox, self.send, self.recv = e, mine, inbox, send, recv
        self.members, self.own = members, own

    @staticmethod
    def plane(e):
        out = []
        for f in range(e.nf):
            for c in range(e.nc):
                out.append((f * e.nc + c, e.at(f=f, c=c), both(e.f == f, e.c == c)))
        return out, e.f * e.nc + e.c

    @staticmethod
    def heads(e):
        out = []
        for q in range(2):
            for t in range(e.nt):
                out.append((q * e.nt + t, e.at(f=e.group + q, t=t), both(e.p == q, e.t == t)))
        return out, e.p * e.nt + e.t

    @staticmethod
    def line(e):
        return [(t, e.at(t=t), e.t == t) for t in range(e.nt)], e.t

    def start(self):
        self.inbox[self.own] = self.mine[...]
        for k, device, me in self.members:

            def go(k=k, device=device):
                remote(
                    self.mine, self.inbox.at[self.own], self.send.at[k], self.recv.at[self.own], device
                ).start()

            when(jnp.logical_not(me), go)

    def finish(self):
        for k, device, me in self.members:

            def go(k=k, device=device):
                d = remote(self.mine, self.inbox.at[k], self.send.at[k], self.recv.at[k], device)
                d.wait_recv()
                d.wait_send()

            when(jnp.logical_not(me), go)
        return jnp.sum(self.inbox[...], axis=0)


def to_heads(e, src, dst, send, recv, heads, span):
    for jj in range(heads):
        head = heads * e.p + jj
        for q in range(2):
            piece = src.at[jj, pl.ds(q * span, span), :]
            here = both(head == e.c, q == e.p)
            when(here, lambda piece=piece: pltpu.make_async_copy(piece, dst.at[e.c], recv).start())

            def away(piece=piece, jj=jj, q=q, head=head):
                remote(
                    piece, dst.at[e.c], send.at[jj, q], recv, e.at(f=e.group + q, c=head)
                ).start()

            when(jnp.logical_not(here), away)


def to_heads_drain(e, src, send, heads, span):
    piece = src.at[0, pl.ds(0, span), :]
    for jj in range(heads):
        head = heads * e.p + jj
        for q in range(2):
            here = both(head == e.c, q == e.p)
            when(jnp.logical_not(here), lambda jj=jj, q=q: wait_bytes(piece, send.at[jj, q]))


def from_heads(e, src, dst, send, recv, heads):
    core = lax.div(e.c, heads)
    for c in range(e.nc):
        here = both(e.c == c, core == e.p)
        when(here, lambda c=c: pltpu.make_async_copy(src.at[c], dst, recv).start())

        def away(c=c):
            remote(src.at[c], dst, send.at[c], recv, e.at(f=e.group + core, c=c)).start()

        when(jnp.logical_not(here), away)


def from_heads_drain(e, src, send, heads):
    core = lax.div(e.c, heads)
    for c in range(e.nc):
        here = both(e.c == c, core == e.p)
        when(jnp.logical_not(here), lambda c=c: wait_bytes(src.at[c], send.at[c]))


def columns(first, second):
    lane = lax.broadcasted_iota(jnp.int32, (first.shape[0], 128), 1)
    both_cols = jnp.where(lane == 0, first, jnp.where(lane == 1, second, 0.0))
    return both_cols.T[0:8]


def turn(values, angle_cos, angle_sin):
    return values * angle_cos + pltpu.roll(values, HD // 2, 1) * angle_sin


def turn_back(values, angle_cos, angle_sin):
    return values * angle_cos - pltpu.roll(values, HD // 2, 1) * angle_sin


def masked(scores, seg_col, seg_row, s, i, span):
    keys = scores.shape[1]
    row = lax.broadcasted_iota(jnp.int32, scores.shape, 0) + i * span
    col = lax.broadcasted_iota(jnp.int32, scores.shape, 1)
    same = seg_col[s, pl.ds(i * span, span), :] == seg_row[s, :, pl.ds(0, keys)]
    return jnp.where(jnp.logical_and(same, row >= col), scores, masked_score)


def front_kernel(
    sizes, seqs, rows,
    tokens, cos_own, sin_own, qgain, kgain, seg_col, seg_row, wq_sh, wk_sh, wv_sh, wo_sh, gate_sh,
    att, xs_out, wq_out, wk_out, wv_out, wo_out, gate_out, units, scales, angles, qkv_heads, att_heads, lse,
    x, wq, wk, wv, lin, qkvx, qkvh, atth, mine, inbox, wide_t, ang,
    wsem, gsem, asem, esem, hsend, hrecv, bsend, brecv, osem,
):
    e = Place(*sizes)
    n = e.nt
    span = n * rows
    wide = wq.shape[1]
    heads = wide // HD
    pairs = ((wq_sh, wq), (wk_sh, wk), (wv_sh, wv), (wo_sh, wo_out), (gate_sh, gate_out))
    ws = [Weight(e, sh, full, wsem.at[i]) for i, (sh, full) in enumerate(pairs)]
    gat = [Gather(e, x.at[s], gsem.at[s], rows) for s in range(seqs)]
    own = pl.ds(pl.multiple_of(e.p * span, span), span)

    def angle_copy():
        ref = ang.at[:, :, own, :]
        return remote(ref, ref, asem.at[0], asem.at[1], e.at(f=e.mate))

    e.barrier()
    for s in range(seqs):
        gat[s].block(e.p, e.t)[...] = tokens[s]
        gat[s].init()
    for w in (ws[2], ws[0], ws[1]):
        w.start()
    ang[0, :, own, :] = cos_own[...]
    ang[1, :, own, :] = sin_own[...]
    angle_copy().start()
    wide_t[...] = jnp.zeros_like(wide_t)

    def step(j):
        for s in range(seqs):
            gat[s].slot(j)

    loop(n - 2, step)
    for w in (ws[2], ws[0], ws[1]):
        w.relay()
    ws[3].start()
    ws[4].start()
    step(n - 2)
    for s in range(seqs):
        gat[s].done()
    outs = [pltpu.make_async_copy(x, xs_out, osem.at[0])]
    outs[0].start()
    ws[2].wait()
    for s in range(seqs):
        r = dot(x[s], wv[...], NN).astype(BF)
        for jj in range(heads):
            qkvx[2, s, jj] = r[:, jj * HD : (jj + 1) * HD]
        to_heads(e, qkvx.at[2, s], qkvh.at[2, s], hsend.at[2, s], hrecv.at[2, s], heads, span)
    ws[0].wait()
    ws[1].wait()
    for k, (w, out) in enumerate(((wq, wq_out), (wk, wk_out), (wv, wv_out))):
        outs.append(pltpu.make_async_copy(w, out, osem.at[1 + k]))
        outs[-1].start()
    sums = [[], []]
    for k, w in enumerate((wq, wk)):
        for s in range(seqs):
            r = dot(x[s], w[...], NN)
            lin[k, s] = r
            sums[k].append(jnp.sum(r * r, axis=-1, keepdims=True))
    mine[...] = columns(*[jnp.concatenate(v, axis=0) for v in sums])
    ex = Exchange(e, mine, inbox, esem.at[0], esem.at[1], *Exchange.heads(e))
    ex.start()
    angle_copy().wait_recv()
    angles[...] = ang[...]
    wide_t[0:8] = lax.rsqrt(ex.finish() / D + epsilon)
    sc = wide_t[...].T
    for s in range(seqs):
        scales[s] = sc[s * 2 * span : (s + 1) * 2 * span]
    place = cut(e.t * 2 + e.p, wide)
    for s in range(seqs):
        for k, gain in enumerate((qgain, kgain)):
            unit = lin[k, s] * scales[s][:, k : k + 1]
            units[k, s] = unit
            scaled = unit * gain[:, place]
            for jj in range(heads):
                turned = turn(scaled[:, jj * HD : (jj + 1) * HD], ang[0, s], ang[1, s])
                qkvx[k, s, jj] = turned.astype(BF)
            to_heads(e, qkvx.at[k, s], qkvh.at[k, s], hsend.at[k, s], hrecv.at[k, s], heads, span)

    ws[3].relay()
    ws[4].relay()

    def attend(s):
        for k in (2, 0, 1):
            wait_bytes(qkvh.at[k, s], hrecv.at[k, s])
        for i in range(e.nc):
            keys = (i + 1) * span
            kb = qkvh[1, s, 0 : i + 1].reshape(keys, HD)
            vb = qkvh[2, s, 0 : i + 1].reshape(keys, HD)
            scores = masked(dot(qkvh[0, s, i], kb, NT) * HD**-0.5, seg_col, seg_row, s, i, span)
            top = jnp.max(scores, axis=-1, keepdims=True)
            ex_s = jnp.exp(scores - top)
            total = jnp.sum(ex_s, axis=-1, keepdims=True)
            log_total = top + jnp.log(total)
            lse[s, i * span : (i + 1) * span, :] = jnp.broadcast_to(log_total, (span, HD))
            probs = (ex_s * (1.0 / total)).astype(BF)
            atth[s, i] = dot(probs, vb, NN).astype(BF)
        dst = att.at[s, own, cut(lax.rem(e.c, heads), HD)]
        from_heads(e, atth.at[s], dst, bsend.at[s], brecv.at[s], heads)

    loop(seqs, attend)
    for k, (a, b) in enumerate(((qkvh, qkv_heads), (atth, att_heads))):
        outs.append(pltpu.make_async_copy(a, b, osem.at[4 + k]))
        outs[-1].start()
    for s in range(seqs):
        wait_bytes(att.at[s], brecv.at[s])
        from_heads_drain(e, atth.at[s], bsend.at[s], heads)
        for k in range(3):
            to_heads_drain(e, qkvx.at[k, s], hsend.at[k, s], heads, span)
        gat[s].drain()
    angle_copy().wait_send()
    ws[3].wait()
    ws[4].wait()
    for w in ws:
        w.drain()
    for o in outs:
        o.wait()


def front_stage(
    sizes, tokens, cos_own, sin_own, qgain, kgain, seg_col, seg_row, wq, wk, wv, wo, gate
):
    nf, nc, nt = sizes
    seqs, rows, dm = tokens.shape
    wide = wq.shape[1] // 2
    heads = wide // HD
    full = 2 * nt * rows
    span = nt * rows
    sds = jax.ShapeDtypeStruct
    v, dma = pltpu.VMEM, pltpu.SemaphoreType.DMA
    return pl.pallas_call(
        functools.partial(front_kernel, sizes, seqs, rows),
        name="front_stage",
        out_shape=(
            sds((seqs, full, wide), BF),
            sds((seqs, full, dm), BF),
            sds((dm, wide), BF),
            sds((dm, wide), BF),
            sds((dm, wide), BF),
            sds((dm, wide), BF),
            sds((dm, gate.shape[1] // 8), BF),
            sds((2, seqs, full, wide), F32),
            sds((seqs, full, 128), F32),
            sds((2, seqs, full, HD), F32),
            sds((3, seqs, nc, span, HD), BF),
            sds((seqs, nc, span, HD), BF),
            sds((seqs, nc * span, HD), F32),
        ),
        in_specs=[VMEM_SPEC] * 7 + [HBM_SPEC] * 5,
        out_specs=(HBM_SPEC,) * 7 + (VMEM_SPEC,) * 3 + (HBM_SPEC,) * 2 + (VMEM_SPEC,),
        scratch_shapes=[
            v((seqs, full, dm), BF),
            v((dm, wide), BF),
            v((dm, wide), BF),
            v((dm, wide), BF),
            v((2, seqs, full, wide), F32),
            v((3, seqs, heads, full, HD), BF),
            v((3, seqs, nc, span, HD), BF),
            v((seqs, nc, span, HD), BF),
            v((8, seqs * full), F32),
            v((2 * nt, 8, seqs * full), F32),
            v((128, seqs * full), F32),
            v((2, seqs, full, HD), F32),
            dma((5, 4)),
            dma((seqs, 6, 2 * nt - 1)),
            dma((2,)),
            dma((2, 2 * nt)),
            dma((3, seqs, heads, 2)),
            dma((3, seqs)),
            dma((seqs, nc)),
            dma((seqs,)),
            dma((6,)),
        ],
        compiler_params=pltpu.CompilerParams(
            collective_id=2, has_side_effects=True, vmem_limit_bytes=60 << 20
        ),
    )(tokens, cos_own, sin_own, qgain, kgain, seg_col, seg_row, wq, wk, wv, wo, gate)


def tail_kernel(
    sizes, seqs, rows,
    hidden_grad, gains_in, units, scales, angles, qgain, kgain, seg_col, seg_row, lse,
    agh_in, qkv_heads, att_heads, xs_in, wq_in, wk_in, wv_in,
    wo_part, up_part,
    input_grad, gains_out, in_q, in_k, in_v, in_o, in_u,
    agh, qkvh, atth, x, wq, wk, wv, dh, dx, acck, accv, uu, pre, part, pair, right, left, y,
    mine, inbox, wide_t, gmine, gin, gin2, p_o, p_u, f_q, f_k, f_v, f_o, f_u,
    lsem, dsend, drecv, esem, rsem, ssem, g1sem, g2sem,
):
    e = Place(*sizes)
    n = e.nt
    span = n * rows
    dm = x.shape[2]
    wide = wq.shape[1]
    heads = wide // HD
    scat = [
        Scatter(e, p, fi, b, ssem.at[k])
        for k, (p, fi, b) in enumerate(
            (
                (wq, f_q, in_q), (wk, f_k, in_k), (wv, f_v, in_v),
                (p_o, f_o, in_o), (p_u, f_u, in_u),
            )
        )
    ]
    loads = [
        pltpu.make_async_copy(a, b, lsem.at[k])
        for k, (a, b) in enumerate(
            (
                (qkv_heads, qkvh), (agh_in, agh), (att_heads, atth), (wq_in, wq),
                (wk_in, wk), (wv_in, wv), (xs_in, x),
                (up_part, p_u), (wo_part, p_o),
            )
        )
    ]
    for ld in loads:
        ld.start()
    e.barrier()
    loads[7].wait()
    scat[4].start()
    loads[8].wait()
    scat[3].start()
    wide_t[...] = jnp.zeros_like(wide_t)
    for ld in loads[:3]:
        ld.wait()

    def attend_back(s):
        acck[...] = jnp.zeros_like(acck)
        accv[...] = jnp.zeros_like(accv)
        for i in range(e.nc):
            keys = (i + 1) * span
            kb = qkvh[1, s, 0 : i + 1].reshape(keys, HD)
            vb = qkvh[2, s, 0 : i + 1].reshape(keys, HD)
            qb = qkvh[0, s, i]
            rowsl = pl.ds(i * span, span)
            scores = masked(dot(qb, kb, NT) * HD**-0.5, seg_col, seg_row, s, i, span)
            probs = jnp.exp(scores - lse[s, rowsl, 0:1])
            da = agh[s, i]
            accv[0:keys] += dot(probs.astype(BF), da, TN)
            delta = jnp.sum(da.astype(F32) * atth[s, i].astype(F32), axis=-1, keepdims=True)
            ds = (probs * (dot(da, vb, NT) - delta)).astype(BF)
            dh[0, s, i] = (dot(ds, kb, NN) * HD**-0.5).astype(BF)
            acck[0:keys] += dot(ds, qb, TN)
        dh[1, s] = (acck[...] * HD**-0.5).astype(BF).reshape(e.nc, span, HD)
        dh[2, s] = accv[...].astype(BF).reshape(e.nc, span, HD)
        own = pl.ds(pl.multiple_of(e.p * span, span), span)
        for k in range(3):
            dst = dx.at[k, s, lax.rem(e.c, heads), own, :]
            from_heads(e, dh.at[k, s], dst, dsend.at[k, s], drecv.at[k, s], heads)

    loop(seqs, attend_back)
    scat[4].relay()
    scat[3].relay()

    place = cut(e.t * 2 + e.p, wide)
    gmine[...] = gains_in[...]
    gmine[0:2, :] = jnp.zeros((2, dm), F32)
    inner = [[], []]
    for s in range(seqs):
        for k in range(3):
            wait_bytes(dx.at[k, s], drecv.at[k, s])
        for k, gain in enumerate((qgain, kgain)):
            for jj in range(heads):
                lanes = slice(jj * HD, (jj + 1) * HD)
                g = turn_back(dx[k, s, jj].astype(F32), angles[0, s], angles[1, s])
                uu[k, s, :, lanes] = g
            g = uu[k, s]
            unit = units[k, s]
            gmine[k : k + 1, place] += jnp.sum(g * unit, axis=0, keepdims=True)
            u = g * gain[:, place]
            uu[k, s] = u
            inner[k].append(jnp.sum(u * unit, axis=-1, keepdims=True))
        for jj in range(heads):
            pre[2, s, :, jj * HD : (jj + 1) * HD] = dx[2, s, jj]
    mine[...] = columns(*[jnp.concatenate(v, axis=0) for v in inner])
    ex = Exchange(e, mine, inbox, esem.at[0], esem.at[1], *Exchange.heads(e))
    ex.start()
    gx = Exchange(e, gmine, gin, g1sem.at[0], g1sem.at[1], *Exchange.plane(e))
    gx.start()
    for ld in loads[3:7]:
        ld.wait()
    wide_t[0:8] = ex.finish() / D
    cols = wide_t[...].T
    for s in range(seqs):
        for k in range(2):
            mean = cols[s * 2 * span : (s + 1) * 2 * span, k : k + 1]
            v = scales[s][:, k : k + 1] * (uu[k, s] - units[k, s] * mean)
            pre[k, s] = v.astype(BF)

    tile = 512
    red = [
        Reduce(e, part.at[s], pair.at[s], right.at[s], left.at[s], rsem.at[s], rows)
        for s in range(seqs)
    ]
    for s in range(seqs):

        def step(i, s=s):
            sl = cut(i, tile)
            total = dot(pre[0, s], wq[sl, :], NT) + dot(pre[1, s], wk[sl, :], NT)
            part[s, :, sl] = (total + dot(pre[2, s], wv[sl, :], NT)).astype(BF)

        loop(dm // tile, step)
        red[s].pair_send()
    for s in range(seqs):
        red[s].pair_add()
        red[s].slot(-1)
    for k, w in enumerate((wq, wk, wv)):

        def step(i, k=k, w=w):
            sl = cut(i, tile)
            lhs = x[:, :, sl].reshape(-1, tile)
            w[sl, :] = dot(lhs, pre[k].reshape(-1, wide), TN).astype(BF)

        loop(dm // tile, step)
        scat[k].start()
    for j in range(n - 1):
        if j == n - 2:
            scat[0].relay()
            scat[1].relay()
        for s in range(seqs):
            red[s].slot(j)
    scat[2].relay()
    gmine[...] = gx.finish()
    gx2 = Exchange(e, gmine, gin2, g2sem.at[0], g2sem.at[1], *Exchange.line(e))
    gx2.start()
    for s in range(seqs):
        red[s].result(y)
        input_grad[s] = hidden_grad[s] + y[...]
    gains_out[...] = gx2.finish()
    for sc in scat:
        sc.wait()
        sc.drain()
    for s in range(seqs):
        red[s].drain()
        for k in range(3):
            from_heads_drain(e, dh.at[k, s], dsend.at[k, s], heads)


def tail_stage(sizes, *args):
    nf, nc, nt = sizes
    hidden_grad, up_part, wo_part = args[0], args[18], args[17]
    seqs, rows, dm = hidden_grad.shape
    half, wide = up_part.shape[1], wo_part.shape[1]
    heads = wide // HD
    full = 2 * nt * rows
    span = nt * rows
    sds = jax.ShapeDtypeStruct
    v, dma = pltpu.VMEM, pltpu.SemaphoreType.DMA
    small, small_terms = scatter_shapes(sizes, dm, wide)
    large, large_terms = scatter_shapes(sizes, dm, half)
    return pl.pallas_call(
        functools.partial(tail_kernel, sizes, seqs, rows),
        name="tail_stage",
        out_shape=(sds((seqs, rows, dm), F32), sds((8, dm), F32))
        + (sds(small_terms, BF),) * 4
        + (sds(large_terms, BF),),
        in_specs=[VMEM_SPEC] * 10 + [HBM_SPEC] * 9,
        out_specs=(VMEM_SPEC,) * 2 + (HBM_SPEC,) * 5,
        scratch_shapes=[
            v((seqs, nc, span, HD), BF),
            v((3, seqs, nc, span, HD), BF),
            v((seqs, nc, span, HD), BF),
            v((seqs, full, dm), BF),
            v((dm, wide), BF),
            v((dm, wide), BF),
            v((dm, wide), BF),
            v((3, seqs, nc, span, HD), BF),
            v((3, seqs, heads, full, HD), BF),
            v((nc * span, HD), F32),
            v((nc * span, HD), F32),
            v((2, seqs, full, wide), F32),
            v((3, seqs, full, wide), BF),
            v((seqs, full, dm), BF),
            v((seqs, nt * rows, dm), BF),
            v((seqs, nt - 1, rows, dm), BF),
            v((seqs, nt - 1, rows, dm), BF),
            v((rows, dm), F32),
            v((8, seqs * full), F32),
            v((2 * nt, 8, seqs * full), F32),
            v((128, seqs * full), F32),
            v((8, dm), F32),
            v((nf * nc, 8, dm), F32),
            v((nt, 8, dm), F32),
            v((dm, wide), BF),
            v((dm, half), BF),
            v(small, BF),
            v(small, BF),
            v(small, BF),
            v(small, BF),
            v(large, BF),
            dma((9,)),
            dma((3, seqs, nc)),
            dma((3, seqs)),
            dma((2, 2 * nt)),
            dma((seqs, 4, nt)),
            dma((5, 4)),
            dma((2, nf * nc)),
            dma((2, nt)),
        ],
        compiler_params=pltpu.CompilerParams(
            collective_id=3, has_side_effects=True, vmem_limit_bytes=63 << 20
        ),
    )(*args)


def add_kernel(count, *refs):
    for src, dst in zip(refs[:count], refs[count:]):
        total = src[0].astype(F32)
        for i in range(1, src.shape[0]):
            total += src[i].astype(F32)
        dst[...] = total


def add_terms(terms):
    steps = 4

    def rows(x):
        return x.shape[1] // steps

    return pl.pallas_call(
        functools.partial(add_kernel, len(terms)),
        name="add_terms",
        grid=(steps,),
        out_shape=tuple(jax.ShapeDtypeStruct(x.shape[1:], F32) for x in terms),
        in_specs=[
            pl.BlockSpec((x.shape[0], rows(x), x.shape[2]), lambda i: (0, i, 0)) for x in terms
        ],
        out_specs=tuple(pl.BlockSpec((rows(x), x.shape[2]), lambda i: (i, 0)) for x in terms),
    )(*terms)


def body(
    tokens, segments, positions, query_weight, key_weight, value_weight, output_weight,
    gate_weight, up_projection_weight, down_weight, query_gain, key_gain, attention_gain,
    feedforward_gain, cotangent,
):
    sizes = (lax.axis_size("fsdp"), lax.axis_size("ctx"), lax.axis_size("tensor"))
    seqs, rows, _ = tokens.shape
    span = sizes[2] * rows
    block_pos = lax.dynamic_slice_in_dim(positions, lax.axis_index("ctx") * span, span, 1)
    cosine, sine = rope_tables(block_pos)
    cos_own = jnp.concatenate([cosine, cosine], axis=-1)
    sin_own = jnp.concatenate([-sine, sine], axis=-1)
    seg_col = segments[:, :, None]
    seg_row = segments[:, None, :]
    qgain, kgain = query_gain[None], key_gain[None]
    (
        att, xs, wq, wk, wv, wo, gate, units, scales, angles, qkv_heads, att_heads, lse,
    ) = front_stage(
        sizes, tokens, cos_own, sin_own, qgain, kgain, seg_col, seg_row,
        query_weight, key_weight, value_weight, output_weight, gate_weight,
    )
    block_out, hidden_grad, agh, wo_part, gate_terms, up_part, down_terms, gains = ffn_stage(
        sizes, att, wo, gate, gate_weight, up_projection_weight, down_weight,
        tokens, cotangent, attention_gain[None], feedforward_gain[None],
    )
    input_grad, gain_sums, *terms, up_terms = tail_stage(
        sizes, hidden_grad, gains, units, scales, angles, qgain, kgain, seg_col, seg_row, lse,
        agh, qkv_heads, att_heads, xs, wq, wk, wv, wo_part, up_part,
    )
    weight_grads = add_terms((*terms, gate_terms, up_terms, down_terms))
    return (block_out, input_grad, *weight_grads, *(gain_sums[k] for k in range(4)))


def solution(mesh):
    in_specs = (
        P("fsdp", ("ctx", "tensor"), None),
        P("fsdp", None),
        P("fsdp", None),
        P(("fsdp", "ctx"), "tensor"),
        P(("fsdp", "ctx"), "tensor"),
        P(("fsdp", "ctx"), "tensor"),
        P(("fsdp", "ctx"), "tensor"),
        P(("fsdp", "ctx"), "tensor"),
        P(("fsdp", "ctx"), "tensor"),
        P(("fsdp", "ctx"), "tensor"),
        P(),
        P(),
        P(),
        P(),
        P("fsdp", ("ctx", "tensor"), None),
    )
    out_specs = (
        P("fsdp", ("ctx", "tensor"), None),
        P("fsdp", ("ctx", "tensor"), None),
        P(("fsdp", "ctx"), "tensor"),
        P(("fsdp", "ctx"), "tensor"),
        P(("fsdp", "ctx"), "tensor"),
        P(("fsdp", "ctx"), "tensor"),
        P(("fsdp", "ctx"), "tensor"),
        P(("fsdp", "ctx"), "tensor"),
        P(("fsdp", "ctx"), "tensor"),
        P(),
        P(),
        P(),
        P(),
    )
    return jax.shard_map(body, mesh=mesh, in_specs=in_specs, out_specs=out_specs, check_vma=False)
```

```python
import functools

import jax
import jax.numpy as jnp
from jax import lax
from jax.experimental import pallas as pl
from jax.experimental.pallas import tpu as pltpu
from jax.sharding import PartitionSpec as P

D = 2048
HD = 128


epsilon = 1e-06
rope_theta = 500000.0
masked_score = -1e30


def rope_tables(position_ids):
    freq_index = jnp.arange(HD // 2, dtype=jnp.float32)
    inverse = rope_theta ** (-2.0 * freq_index / HD)
    angles = position_ids.astype(jnp.float32)[..., None] * inverse
    return (jnp.cos(angles), jnp.sin(angles))


MESH = pl.DeviceIdType.MESH
BF = jnp.bfloat16
F32 = jnp.float32
VMEM_SPEC = pl.BlockSpec(memory_space=pltpu.VMEM)
HBM_SPEC = pl.BlockSpec(memory_space=pltpu.HBM)
NN = (((1,), (0,)), ((), ()))
NT = (((1,), (1,)), ((), ()))
TN = (((0,), (0,)), ((), ()))


def dot(a, b, dims):
    return lax.dot_general(a, b, dims, preferred_element_type=F32)


def loop(count, step):
    def run(i, carry):
        step(i)
        return carry

    lax.fori_loop(0, count, run, 0)


def cut(i, size):
    return pl.ds(pl.multiple_of(i * size, size), size)


def both(*conds):
    out = True
    for cond in conds:
        if isinstance(cond, bool):
            if not cond:
                return False
        elif isinstance(out, bool):
            out = cond
        else:
            out = jnp.logical_and(out, cond)
    return out


def when(cond, step):
    if isinstance(cond, bool):
        if cond:
            step()
    else:
        pl.when(cond)(step)


class Place:
    def __init__(self, fsdp_size, ctx_size, tensor_size):
        self.nf, self.nc, self.nt = fsdp_size, ctx_size, tensor_size
        self.f = lax.axis_index("fsdp")
        self.c = lax.axis_index("ctx")
        self.t = lax.axis_index("tensor")
        self.p = lax.rem(self.f, 2)
        self.group = self.f - self.p
        self.mate = self.group + 1 - self.p

    def at(self, f=None, c=None, t=None):
        return {
            "fsdp": self.f if f is None else f,
            "ctx": self.c if c is None else c,
            "tensor": self.t if t is None else t,
        }

    def plane(self):
        out = []
        for dg in range(self.nf // 2):
            for dc in (3, 1, 2, 0) if self.nc == 4 else range(self.nc):
                for dp in (0, 1):
                    if dg or dc or dp:
                        out.append((dg, dc, dp))
        return out

    def peer(self, off):
        dg, dc, dp = off
        group = lax.rem(self.group + 2 * dg, self.nf)
        core = self.p + dp - 2 * self.p * dp
        return group + core, core, jnp.bitwise_xor(self.c, dc)

    def barrier(self):
        sem = pltpu.get_barrier_semaphore()

        def signal(**place):
            pl.semaphore_signal(sem, inc=1, device_id=self.at(**place), device_id_type=MESH)

        offs = self.plane()
        for off in offs:
            f, _, c = self.peer(off)
            signal(f=f, c=c)
        for dt in range(1, self.nt):
            for core in range(2):
                signal(f=self.group + core, t=lax.rem(self.t + dt, self.nt))
        pl.semaphore_wait(sem, len(offs) + 2 * (self.nt - 1))


def remote(src, dst, send, recv, device):
    return pltpu.make_async_remote_copy(
        src_ref=src, dst_ref=dst, send_sem=send, recv_sem=recv, device_id=device, device_id_type=MESH
    )


def wait_bytes(ref, sem):
    pltpu.make_async_copy(ref, ref, sem).wait()


class Reduce:
    def __init__(self, e, part, pair, right, left, sems, rows):
        self.e, self.part, self.pair, self.right, self.left, self.rows = e, part, pair, right, left, rows
        self.sems = sems

    def half(self, p):
        n = self.e.nt * self.rows
        return self.part.at[pl.ds(pl.multiple_of(p * n, n), n), :]

    def block(self, b):
        return self.part.at[cut(self.e.p * self.e.nt + b, self.rows), :]

    def _pair(self):
        return remote(
            self.half(1 - self.e.p), self.pair, self.sems.at[0, 0], self.sems.at[1, 0],
            self.e.at(f=self.e.mate),
        )

    def _side(self, b, k, up):
        e = self.e
        buf, row = (self.right, 0) if up else (self.left, 2)
        return remote(
            self.block(b), buf.at[k], self.sems.at[row, 1 + k], self.sems.at[row + 1, 1 + k],
            e.at(t=e.t + 1 if up else e.t - 1),
        )

    def pair_send(self):
        self._pair().start()

    def pair_add(self):
        self._pair().wait_recv()
        mine = self.half(self.e.p)

        def step(i):
            sl = cut(i, self.rows)
            mine[sl, :] = (mine[sl, :].astype(F32) + self.pair[sl, :].astype(F32)).astype(BF)

        loop(self.e.nt, step)

    def slot(self, j):
        e, n = self.e, self.e.nt
        for up in (True, False):
            b = e.t + (n - 2) - j if up else e.t - (n - 2) + j
            near = e.t > 0 if up else e.t < n - 1
            far = e.t < n - 1 if up else e.t > 0
            inside = b <= n - 1 if up else b >= 0
            buf = self.right if up else self.left

            def take(b=b, buf=buf, up=up):
                self._side(b, j, up).wait_recv()

                def add():
                    blk = self.block(b)
                    blk[...] = (blk[...].astype(F32) + buf[j].astype(F32)).astype(BF)

                when(j < n - 2, add)

            when(both(j >= 0, j <= n - 2, near, inside), take)
            when(both(j < n - 2, far, inside), lambda b=b, up=up: self._side(b, j + 1, up).start())

    def result(self, out):
        e, n = self.e, self.e.nt
        out[...] = self.block(e.t)[...].astype(F32)

        def add_right():
            out[...] += self.right[n - 2].astype(F32)

        def add_left():
            out[...] += self.left[n - 2].astype(F32)

        when(e.t > 0, add_right)
        when(e.t < n - 1, add_left)

    def drain(self):
        e, n = self.e, self.e.nt
        self._pair().wait_send()

        def step(i):
            j = i - 1
            for up in (True, False):
                b = e.t + (n - 2) - j if up else e.t - (n - 2) + j
                far = e.t < n - 1 if up else e.t > 0
                inside = b <= n - 1 if up else b >= 0
                when(both(far, inside), lambda b=b, up=up: self._side(b, j + 1, up).wait_send())

        for i in range(n - 1):
            step(i)


class Gather:
    def __init__(self, e, full, sems, rows):
        self.e, self.full, self.sems, self.rows = e, full, sems, rows

    def block(self, p, b):
        return self.full.at[cut(p * self.e.nt + b, self.rows), :]

    def _side(self, b, k, up):
        e = self.e
        row = 0 if up else 2
        ref = self.block(e.p, b)
        return remote(
            ref, ref, self.sems.at[row, k], self.sems.at[row + 1, k],
            e.at(t=e.t + 1 if up else e.t - 1),
        )

    def _pair(self, b, k, incoming):
        e = self.e
        ref = self.block(1 - e.p if incoming else e.p, b)
        return remote(ref, ref, self.sems.at[4, k], self.sems.at[5, k], e.at(f=e.mate))

    def init(self):
        e, n = self.e, self.e.nt
        when(e.t < n - 1, lambda: self._side(e.t, 0, True).start())
        when(e.t > 0, lambda: self._side(e.t, 0, False).start())
        self._pair(e.t, 0, False).start()

    def slot(self, j):
        e, n = self.e, self.e.nt
        for up in (True, False):
            b = e.t - 1 - j if up else e.t + 1 + j
            inside = b >= 0 if up else b <= n - 1
            far = e.t < n - 1 if up else e.t > 0
            k = 1 + j if up else n + j

            def take(b=b, up=up, far=far, k=k):
                self._side(b, j, up).wait_recv()
                when(both(far, j < n - 2), lambda: self._side(b, j + 1, up).start())
                self._pair(b, k, False).start()

            when(both(j >= 0, j <= n - 2, inside), take)

    def _rest(self, step_pair):
        e, n = self.e, self.e.nt
        step_pair(e.t, 0)
        for j in range(n - 1):
            when(e.t - 1 - j >= 0, lambda j=j: step_pair(e.t - 1 - j, 1 + j))
            when(e.t + 1 + j <= n - 1, lambda j=j: step_pair(e.t + 1 + j, n + j))

    def done(self):
        self._rest(lambda b, k: self._pair(b, k, True).wait_recv())

    def drain(self):
        e, n = self.e, self.e.nt
        self._rest(lambda b, k: self._pair(b, k, False).wait_send())
        when(e.t < n - 1, lambda: self._side(e.t, 0, True).wait_send())
        when(e.t > 0, lambda: self._side(e.t, 0, False).wait_send())
        for j in range(n - 2):
            when(
                both(e.t - 1 - j >= 0, e.t < n - 1),
                lambda j=j: self._side(e.t - 1 - j, j + 1, True).wait_send(),
            )
            when(
                both(e.t + 1 + j <= n - 1, e.t > 0),
                lambda j=j: self._side(e.t + 1 + j, j + 1, False).wait_send(),
            )


SPLIT = 2


def parts_of(width):
    size = width // SPLIT
    return [pl.ds(u * size, size) for u in range(SPLIT)]


class Both:
    def __init__(self, each):
        self.each = list(each)

    def __getattr__(self, name):
        def call(*args):
            for x in self.each:
                getattr(x, name)(*args)

        return call


class Weight:
    def __init__(self, e, shard, full, sems, off=0):
        self.e, self.shard, self.full, self.sems, self.off = e, shard, full, sems, off
        self.rows, self.width = shard.shape[0], full.shape[1]
        self.stride = shard.shape[1] // 2

    def columns(self, core):
        start = pl.multiple_of(core * self.stride + self.off, 128)
        return self.shard.at[:, pl.ds(start, self.width)]

    def some(self, count):
        return self.full.at[pl.ds(0, count * self.rows), :]

    def targets(self):
        e = self.e
        if e.nf == 2:
            return [(0, 1, 0), (0, 2, 0), (0, 1, 1), (0, 2, 1), (0, 0, 1)]
        return e.plane()

    def start(self):
        e = self.e
        dst = self.full.at[cut(e.f * e.nc + e.c, self.rows), :]
        for off in self.targets():
            f, core, c = e.peer(off)
            remote(self.columns(core), dst, self.sems.at[0], self.sems.at[1], e.at(f=f, c=c)).start()
        pltpu.make_async_copy(self.columns(e.p), dst, self.sems.at[1]).start()

    def relay(self):
        e = self.e
        wait_bytes(self.some(len(self.targets()) + 1), self.sems.at[1])
        if e.nf != 2:
            return
        part = self.rows // 2
        for f in range(2):
            for k, (source, target) in enumerate(((1, 2), (2, 1))):
                row = (f * e.nc + jnp.bitwise_xor(e.c, source)) * self.rows + k * part
                ref = self.full.at[pl.ds(pl.multiple_of(row, part), part), :]
                device = e.at(c=jnp.bitwise_xor(e.c, target))
                remote(ref, ref, self.sems.at[2], self.sems.at[3], device).start()

    def wait(self):
        if self.e.nf == 2:
            wait_bytes(self.some(2), self.sems.at[3])

    def drain(self):
        wait_bytes(self.some(len(self.targets())), self.sems.at[0])
        if self.e.nf == 2:
            wait_bytes(self.some(2), self.sems.at[2])


class Scatter:
    def __init__(self, e, part, first, inbox, sems):
        self.e, self.part, self.first, self.inbox, self.sems = e, part, first, inbox, sems
        self.rows, self.half = inbox.shape[1], part.shape[1]
        self.upper = self.rows // 2

    def piece(self, f, c, side=None):
        row = (f * self.e.nc + c) * self.rows
        if side is None:
            return self.part.at[pl.ds(pl.multiple_of(row, self.rows), self.rows), :]
        row = pl.multiple_of(row + side * self.upper, self.upper)
        return self.part.at[pl.ds(row, self.upper), :]

    def start(self):
        e = self.e
        if e.nf == 2:
            for side in range(2):
                near = jnp.bitwise_xor(e.c, 1 + side)
                for k, owner in enumerate((near, jnp.bitwise_xor(e.c, 3))):
                    for f in range(2):
                        remote(
                            self.piece(f, owner, side), self.first.at[side, k, f],
                            self.sems.at[0], self.sems.at[1], e.at(c=near),
                        ).start()
            return
        slot = lax.div(e.group, 2) * e.nc + e.c
        dst = self.inbox.at[slot, :, cut(e.p, self.half)]
        for off in e.plane():
            f, _, c = e.peer(off)
            remote(
                self.piece(f, c), dst, self.sems.at[2], self.sems.at[3], e.at(f=f, c=c)
            ).start()
        pltpu.make_async_copy(self.piece(e.f, e.c), dst, self.sems.at[3]).start()

    def relay(self):
        e = self.e
        if e.nf != 2:
            return
        wait_bytes(self.first, self.sems.at[1])
        lanes = cut(e.p, self.half)
        for side in range(2):
            far = jnp.bitwise_xor(e.c, 2 - side)
            for k, owner in enumerate((e.c, far)):
                for f in range(2):
                    mine = self.piece(f, owner, side)
                    got = self.first[side, k, f].astype(F32)
                    mine[...] = (mine[...].astype(F32) + got).astype(BF)
            for f in range(2):
                dst = self.inbox.at[1, pl.ds(side * self.upper, self.upper), lanes]
                remote(
                    self.piece(f, far, side), dst, self.sems.at[2], self.sems.at[3],
                    e.at(f=f, c=far),
                ).start()
        dst = self.inbox.at[0, :, lanes]
        remote(
            self.piece(1 - e.p, e.c), dst, self.sems.at[2], self.sems.at[3], e.at(f=e.mate)
        ).start()
        pltpu.make_async_copy(self.piece(e.p, e.c), dst, self.sems.at[3]).start()

    def wait(self):
        wait_bytes(self.inbox, self.sems.at[3])

    def drain(self):
        e = self.e
        count = 3 if e.nf == 2 else len(e.plane())
        wait_bytes(self.part.at[pl.ds(0, count * self.rows), :], self.sems.at[2])
        if e.nf == 2:
            wait_bytes(self.part.at[pl.ds(0, 4 * self.rows), :], self.sems.at[0])


def scatter_shapes(sizes, dm, half):
    nf, nc, _ = sizes
    rb = dm // (nf * nc)
    if nf == 2:
        return (2, 2, 2, rb // 2, half), (2, rb, 2 * half)
    return (1, 1, 1, 16, 128), (nf // 2 * nc, rb, 2 * half)


def ffn_kernel(
    sizes, seqs, rows,
    att, wo_in, gate_in, gate_sh, up_sh, down_sh, tokens, cot, again, fgain,
    block_out, hidden_grad, agh, wo_part, gate_terms, up_part, down_terms, gains,
    wo_v, g_v, u_v, d_v, part, pair, right, left, hid, mgr, agr, aa, bb, mixed,
    unit1, hid32, scale1, scratch_y, agx, first, first_g,
    wsem, lsem, dsem, rsem, gsem, xsend, xrecv, osem,
):
    e = Place(*sizes)
    dm = tokens.shape[2]
    half = g_v.shape[1]
    wide = att.shape[2]
    heads = wide // HD
    early = gate_in.shape[1]
    late = g_v.at[:, pl.ds(early, half - early)]
    w_g = Weight(e, gate_sh, late, wsem.at[0], off=early)
    w_u = Weight(e, up_sh, u_v, wsem.at[1])
    w_d = Weight(e, down_sh, d_v, wsem.at[2])
    load_o = pltpu.make_async_copy(wo_in, wo_v, lsem.at[0])
    load_g = pltpu.make_async_copy(gate_in, g_v.at[:, pl.ds(0, early)], lsem.at[1])
    load_o.start()
    load_g.start()
    scat_d = Scatter(e, d_v, first, down_terms, dsem.at[0])
    scat_g = Scatter(e, g_v, first_g, gate_terms, dsem.at[1])

    def reduce(k, s):
        return Both(
            Reduce(
                e, part.at[s, :, cl], pair.at[s, :, cl], right.at[s, :, :, cl],
                left.at[s, :, :, cl], rsem.at[k, s, u], rows,
            )
            for u, cl in enumerate(parts_of(dm))
        )

    def gather(k, s):
        full = (hid, mgr, agr)[k]
        return Both(
            Gather(e, full.at[s, :, cl], gsem.at[k, s, u], rows)
            for u, cl in enumerate(parts_of(dm))
        )

    def own_rows(k, s):
        return (hid, mgr, agr)[k].at[s, cut(e.p * e.nt + e.t, rows), :]

    def result(k, s, out):
        for r, cl in zip(red[k][s].each, parts_of(dm)):
            r.result(out.at[:, cl])

    red = [[reduce(k, s) for s in range(seqs)] for k in range(3)]
    gat = [[gather(k, s) for s in range(seqs)] for k in range(3)]

    e.barrier()
    w_g.start()
    w_u.start()
    gains[...] = jnp.zeros_like(gains)

    tile = 512

    def out_tiles(s):
        def step(i):
            sl = cut(i, tile)
            part[s, :, sl] = dot(att[s], wo_v[sl, :], NT).astype(BF)

        loop(dm // tile, step)

    def norm1(s):
        y = scratch_y
        result(0, s, y)
        v = y[...]
        scale = lax.rsqrt(jnp.mean(v * v, axis=-1, keepdims=True) + epsilon)
        unit = v * scale
        unit1[s] = unit
        scale1[s] = jnp.broadcast_to(scale, scale1.shape[1:])
        h = tokens[s].astype(F32) + unit * again[...]
        hid32[s] = h
        own_rows(0, s)[...] = h.astype(BF)

    def ffn_tile(s, i):
        sl = cut(i, 256)
        gate = dot(hid[s], g_v[:, sl], NN)
        up = dot(hid[s], u_v[:, sl], NN)
        sig = jax.nn.sigmoid(gate)
        act = gate * sig
        mixed[s, :, sl] = (act * up).astype(BF)
        aa[s, :, sl] = (up * sig * (1.0 + gate * (1.0 - sig))).astype(BF)
        bb[s, :, sl] = act.astype(BF)

    ffn_tiles = half // 256

    def down_tiles(s):
        def step(i):
            sl = cut(i, tile)
            part[s, :, sl] = dot(mixed[s], d_v[sl, :], NT).astype(BF)

        loop(dm // tile, step)

    def norm2(s):
        y = scratch_y
        result(1, s, y)
        v = y[...]
        scale = lax.rsqrt(jnp.mean(v * v, axis=-1, keepdims=True) + epsilon)
        unit = v * scale
        block_out[s] = (hid32[s] + unit * fgain[...]).astype(BF)
        upstream = cot[s].astype(F32)
        gains[3:4, :] += jnp.sum(upstream * unit, axis=0, keepdims=True)
        g = upstream * fgain[...]
        m = scale * (g - unit * jnp.mean(g * unit, axis=-1, keepdims=True))
        own_rows(1, s)[...] = m.astype(BF)

    def inner_tiles(s):
        def step(i):
            sl = cut(i, 256)
            inner = dot(mgr[s], d_v[:, sl], NN)
            aa[s, :, sl] = (inner * aa[s, :, sl].astype(F32)).astype(BF)
            bb[s, :, sl] = (inner * bb[s, :, sl].astype(F32)).astype(BF)

        loop(ffn_tiles, step)

    def back_tiles(s):
        def step(i):
            sl = cut(i, tile)
            part[s, :, sl] = (dot(aa[s], g_v[sl, :], NT) + dot(bb[s], u_v[sl, :], NT)).astype(BF)

        loop(dm // tile, step)

    def norm3(s):
        y = scratch_y
        result(2, s, y)
        hg = cot[s].astype(F32) + y[...]
        hidden_grad[s] = hg
        unit = unit1[s]
        gains[2:3, :] += jnp.sum(hg * unit, axis=0, keepdims=True)
        g = hg * again[...]
        scale = scale1[s][:, 0:1]
        a = scale * (g - unit * jnp.mean(g * unit, axis=-1, keepdims=True))
        own_rows(2, s)[...] = a.astype(BF)

    def weight_tile(left_rows, right_rows, out, i, width):
        per = out.shape[1] // width
        sl, cl = cut(lax.div(i, per), tile), cut(lax.rem(i, per), width)
        lhs = left_rows[:, :, sl].reshape(-1, tile)
        rhs = right_rows[:, :, cl].reshape(-1, width)
        out[sl, cl] = dot(lhs, rhs, TN).astype(BF)

    n = e.nt
    span = agh.shape[2]

    def heads_copy(s, jj, q):
        src = agx.at[s, jj, pl.ds(q * span, span), :]
        dst = agh.at[s, e.c]
        return src, dst

    def heads_grad(s):
        r = dot(agr[s], wo_v[...], NN).astype(BF)
        for jj in range(heads):
            agx[s, jj] = r[:, jj * HD : (jj + 1) * HD]
        for jj in range(heads):
            head = heads * e.p + jj
            for q in range(2):
                src, dst = heads_copy(s, jj, q)
                self_here = both(head == e.c, q == e.p)

                def local(src=src, dst=dst):
                    pltpu.make_async_copy(src, dst, xrecv.at[s]).start()

                def away(src=src, dst=dst, q=q, head=head, jj=jj):
                    remote(
                        src, dst, xsend.at[s, jj, q], xrecv.at[s], e.at(f=e.group + q, c=head)
                    ).start()

                when(self_here, local)
                when(jnp.logical_not(self_here), away)

    def heads_wait(s):
        wait_bytes(agh.at[s], xrecv.at[s])
        block = agx.at[s, 0, pl.ds(0, span), :]
        for jj in range(heads):
            head = heads * e.p + jj
            for q in range(2):
                when(
                    jnp.logical_not(both(head == e.c, q == e.p)),
                    lambda jj=jj, q=q: wait_bytes(block, xsend.at[s, jj, q]),
                )

    load_o.wait()
    out_tiles(0)
    red[0][0].pair_send()
    out_tiles(1)
    red[0][0].pair_add()
    red[0][1].pair_send()

    def step(i):
        red[0][0].slot(i - 1)

    loop(n, step)
    red[0][1].pair_add()
    norm1(0)
    gat[0][0].init()

    def step(i):
        red[0][1].slot(i - 1)
        gat[0][0].slot(i - 1)

    loop(2, step)
    w_g.relay()
    w_u.relay()
    w_d.start()
    loop(n - 2, lambda i: step(i + 2))
    gat[0][0].done()
    norm1(1)
    gat[0][1].init()
    load_g.wait()
    w_g.wait()
    w_u.wait()

    def step(i):
        ffn_tile(0, i)
        gat[0][1].slot(i)

    loop(ffn_tiles, step)
    w_d.relay()
    w_d.wait()
    red[0][0].drain()
    down_tiles(0)
    red[1][0].pair_send()
    gat[0][1].done()
    ffn_tile(1, 0)
    red[1][0].pair_add()

    def step(i):
        red[1][0].slot(i - 1)
        ffn_tile(1, i + 1)

    loop(ffn_tiles - 1, step)
    for j in range(ffn_tiles - 2, n - 1):
        red[1][0].slot(j)
    norm2(0)
    gat[1][0].init()
    red[0][1].drain()
    down_tiles(1)
    red[1][1].pair_send()
    gat[1][0].slot(0)
    red[1][1].pair_add()

    def step(i):
        red[1][1].slot(i - 1)
        gat[1][0].slot(i + 1)

    loop(n, step)
    norm2(1)
    gat[1][1].init()
    gat[1][0].done()
    inner_tiles(0)
    red[1][0].drain()
    back_tiles(0)
    red[2][0].pair_send()
    gat[1][1].slot(0)
    red[2][0].pair_add()

    def step(i):
        red[2][0].slot(i - 1)
        gat[1][1].slot(i + 1)

    loop(n - 2, step)
    gat[1][1].done()
    inner_tiles(1)
    red[2][0].slot(n - 3)
    red[1][1].drain()
    back_tiles(1)
    red[2][1].pair_send()
    red[2][0].slot(n - 2)
    norm3(0)
    gat[2][0].init()
    red[2][1].pair_add()
    red[2][1].slot(-1)
    tiles = (dm // tile) * (half // tile)
    share = -(-tiles // (n - 1))

    def fill(left_rows, right_rows, out, i):
        def go(k):
            which = share * i + k
            when(which < tiles, lambda: weight_tile(left_rows, right_rows, out, which, tile))

        loop(share, go)

    for w in (w_g, w_u, w_d):
        w.drain()
    loop(tiles, lambda i: weight_tile(mgr, mixed, d_v, i, tile))
    scat_d.start()

    def step(i):
        red[2][1].slot(i)
        gat[2][0].slot(i)
        fill(hid, aa, g_v, i)

    loop(n - 1, step)
    scat_g.start()
    norm3(1)
    gat[2][1].init()
    gat[2][0].done()
    heads_grad(0)
    scat_d.relay()

    def step(i):
        gat[2][1].slot(i)
        fill(hid, bb, u_v, i)

    loop(n - 1, step)
    out_u = pltpu.make_async_copy(u_v, up_part, osem.at[2])
    out_u.start()
    gat[2][1].done()
    heads_grad(1)
    scat_g.relay()
    loop(dm // tile, lambda i: weight_tile(agr, att, wo_v, i, wide))
    out_o = pltpu.make_async_copy(wo_v, wo_part, osem.at[3])
    out_o.start()
    heads_wait(0)
    heads_wait(1)
    red[2][0].drain()
    red[2][1].drain()
    for k in range(3):
        for s in range(seqs):
            gat[k][s].drain()
    for sc in (scat_d, scat_g):
        sc.wait()
        sc.drain()
    for o in (out_u, out_o):
        o.wait()


def ffn_stage(
    sizes, att, wo_in, gate_in, gate_sh, up_sh, down_sh, tokens, cot, again, fgain
):
    nf, nc, nt = sizes
    seqs, rows, dm = tokens.shape
    half = gate_sh.shape[1] // 2
    wide = wo_in.shape[1]
    first, terms = scatter_shapes(sizes, dm, half)
    full = 2 * nt * rows
    sds = jax.ShapeDtypeStruct
    v, dma = pltpu.VMEM, pltpu.SemaphoreType.DMA
    return pl.pallas_call(
        functools.partial(ffn_kernel, sizes, seqs, rows),
        name="ffn_stage",
        out_shape=(
            sds((seqs, rows, dm), BF),
            sds((seqs, rows, dm), F32),
            sds((seqs, nc, nt * rows, HD), BF),
            sds((dm, wide), BF),
            sds(terms, BF),
            sds((dm, half), BF),
            sds(terms, BF),
            sds((8, dm), F32),
        ),
        in_specs=[VMEM_SPEC] + [HBM_SPEC] * 5 + [VMEM_SPEC] * 4,
        out_specs=(VMEM_SPEC, VMEM_SPEC) + (HBM_SPEC,) * 5 + (VMEM_SPEC,),
        scratch_shapes=[
            v((dm, wide), BF),
            v((dm, half), BF),
            v((dm, half), BF),
            v((dm, half), BF),
            v((seqs, full, dm), BF),
            v((seqs, nt * rows, dm), BF),
            v((seqs, nt - 1, rows, dm), BF),
            v((seqs, nt - 1, rows, dm), BF),
            v((seqs, full, dm), BF),
            v((seqs, full, dm), BF),
            v((seqs, full, dm), BF),
            v((seqs, full, half), BF),
            v((seqs, full, half), BF),
            v((seqs, full, half), BF),
            v((seqs, rows, dm), F32),
            v((seqs, rows, dm), F32),
            v((seqs, rows, 128), F32),
            v((rows, dm), F32),
            v((seqs, wide // HD, full, HD), BF),
            v(first, BF),
            v(first, BF),
            dma((3, 4)),
            dma((2,)),
            dma((2, 4)),
            dma((3, seqs, SPLIT, 4, nt)),
            dma((3, seqs, SPLIT, 6, 2 * nt - 1)),
            dma((seqs, wide // HD, 2)),
            dma((seqs,)),
            dma((4,)),
        ],
        compiler_params=pltpu.CompilerParams(
            collective_id=1, has_side_effects=True, vmem_limit_bytes=63 << 20
        ),
    )(att, wo_in, gate_in, gate_sh, up_sh, down_sh, tokens, cot, again, fgain)


class Exchange:
    def __init__(self, e, mine, inbox, send, recv, members, own):
        self.e, self.mine, self.inbox, self.send, self.recv = e, mine, inbox, send, recv
        self.members, self.own = members, own

    @staticmethod
    def plane(e):
        out = []
        for f in range(e.nf):
            for c in range(e.nc):
                out.append((f * e.nc + c, e.at(f=f, c=c), both(e.f == f, e.c == c)))
        return out, e.f * e.nc + e.c

    @staticmethod
    def heads(e):
        out = []
        for q in range(2):
            for t in range(e.nt):
                out.append((q * e.nt + t, e.at(f=e.group + q, t=t), both(e.p == q, e.t == t)))
        return out, e.p * e.nt + e.t

    @staticmethod
    def line(e):
        return [(t, e.at(t=t), e.t == t) for t in range(e.nt)], e.t

    def start(self):
        self.inbox[self.own] = self.mine[...]
        for k, device, me in self.members:

            def go(k=k, device=device):
                remote(
                    self.mine, self.inbox.at[self.own], self.send.at[k], self.recv.at[self.own], device
                ).start()

            when(jnp.logical_not(me), go)

    def finish(self):
        for k, device, me in self.members:

            def go(k=k, device=device):
                d = remote(self.mine, self.inbox.at[k], self.send.at[k], self.recv.at[k], device)
                d.wait_recv()
                d.wait_send()

            when(jnp.logical_not(me), go)
        return jnp.sum(self.inbox[...], axis=0)


def to_heads(e, src, dst, send, recv, heads, span):
    for jj in range(heads):
        head = heads * e.p + jj
        for q in range(2):
            piece = src.at[jj, pl.ds(q * span, span), :]
            here = both(head == e.c, q == e.p)
            when(here, lambda piece=piece: pltpu.make_async_copy(piece, dst.at[e.c], recv).start())

            def away(piece=piece, jj=jj, q=q, head=head):
                remote(
                    piece, dst.at[e.c], send.at[jj, q], recv, e.at(f=e.group + q, c=head)
                ).start()

            when(jnp.logical_not(here), away)


def to_heads_drain(e, src, send, heads, span):
    piece = src.at[0, pl.ds(0, span), :]
    for jj in range(heads):
        head = heads * e.p + jj
        for q in range(2):
            here = both(head == e.c, q == e.p)
            when(jnp.logical_not(here), lambda jj=jj, q=q: wait_bytes(piece, send.at[jj, q]))


def from_heads(e, src, dst, send, recv, heads):
    core = lax.div(e.c, heads)
    for c in range(e.nc):
        here = both(e.c == c, core == e.p)
        when(here, lambda c=c: pltpu.make_async_copy(src.at[c], dst, recv).start())

        def away(c=c):
            remote(src.at[c], dst, send.at[c], recv, e.at(f=e.group + core, c=c)).start()

        when(jnp.logical_not(here), away)


def from_heads_drain(e, src, send, heads):
    core = lax.div(e.c, heads)
    for c in range(e.nc):
        here = both(e.c == c, core == e.p)
        when(jnp.logical_not(here), lambda c=c: wait_bytes(src.at[c], send.at[c]))


def columns(first, second):
    lane = lax.broadcasted_iota(jnp.int32, (first.shape[0], 128), 1)
    both_cols = jnp.where(lane == 0, first, jnp.where(lane == 1, second, 0.0))
    return both_cols.T[0:8]


def turn(values, angle_cos, angle_sin):
    return values * angle_cos + pltpu.roll(values, HD // 2, 1) * angle_sin


def turn_back(values, angle_cos, angle_sin):
    return values * angle_cos - pltpu.roll(values, HD // 2, 1) * angle_sin


def masked(scores, seg_col, seg_row, s, i, span):
    keys = scores.shape[1]
    row = lax.broadcasted_iota(jnp.int32, scores.shape, 0) + i * span
    col = lax.broadcasted_iota(jnp.int32, scores.shape, 1)
    same = seg_col[s, pl.ds(i * span, span), :] == seg_row[s, :, pl.ds(0, keys)]
    return jnp.where(jnp.logical_and(same, row >= col), scores, masked_score)


def front_kernel(
    sizes, seqs, rows,
    tokens, cos_own, sin_own, qgain, kgain, seg_col, seg_row, wq_sh, wk_sh, wv_sh, wo_sh, gate_sh,
    att, xs_out, wq_out, wk_out, wv_out, wo_out, gate_out, units, scales, angles, qkv_heads, att_heads, lse,
    x, wq, wk, wv, lin, qkvx, qkvh, atth, mine, inbox, wide_t, ang,
    wsem, gsem, asem, esem, hsend, hrecv, bsend, brecv, osem,
):
    e = Place(*sizes)
    n = e.nt
    span = n * rows
    wide = wq.shape[1]
    heads = wide // HD
    pairs = ((wq_sh, wq), (wk_sh, wk), (wv_sh, wv), (wo_sh, wo_out), (gate_sh, gate_out))
    ws = [Weight(e, sh, full, wsem.at[i]) for i, (sh, full) in enumerate(pairs)]
    gat = [Gather(e, x.at[s], gsem.at[s], rows) for s in range(seqs)]
    own = pl.ds(pl.multiple_of(e.p * span, span), span)

    def angle_copy():
        ref = ang.at[:, :, own, :]
        return remote(ref, ref, asem.at[0], asem.at[1], e.at(f=e.mate))

    e.barrier()
    for s in range(seqs):
        gat[s].block(e.p, e.t)[...] = tokens[s]
        gat[s].init()
    for w in (ws[2], ws[0], ws[1]):
        w.start()
    ang[0, :, own, :] = cos_own[...]
    ang[1, :, own, :] = sin_own[...]
    angle_copy().start()
    wide_t[...] = jnp.zeros_like(wide_t)

    def step(j):
        for s in range(seqs):
            gat[s].slot(j)

    loop(n - 2, step)
    for w in (ws[2], ws[0], ws[1]):
        w.relay()
    ws[3].start()
    ws[4].start()
    step(n - 2)
    for s in range(seqs):
        gat[s].done()
    outs = [pltpu.make_async_copy(x, xs_out, osem.at[0])]
    outs[0].start()
    ws[2].wait()
    for s in range(seqs):
        r = dot(x[s], wv[...], NN).astype(BF)
        for jj in range(heads):
            qkvx[2, s, jj] = r[:, jj * HD : (jj + 1) * HD]
        to_heads(e, qkvx.at[2, s], qkvh.at[2, s], hsend.at[2, s], hrecv.at[2, s], heads, span)
    ws[0].wait()
    ws[1].wait()
    for k, (w, out) in enumerate(((wq, wq_out), (wk, wk_out), (wv, wv_out))):
        outs.append(pltpu.make_async_copy(w, out, osem.at[1 + k]))
        outs[-1].start()
    sums = [[], []]
    for k, w in enumerate((wq, wk)):
        for s in range(seqs):
            r = dot(x[s], w[...], NN)
            lin[k, s] = r
            sums[k].append(jnp.sum(r * r, axis=-1, keepdims=True))
    mine[...] = columns(*[jnp.concatenate(v, axis=0) for v in sums])
    ex = Exchange(e, mine, inbox, esem.at[0], esem.at[1], *Exchange.heads(e))
    ex.start()
    angle_copy().wait_recv()
    angles[...] = ang[...]
    wide_t[0:8] = lax.rsqrt(ex.finish() / D + epsilon)
    sc = wide_t[...].T
    for s in range(seqs):
        scales[s] = sc[s * 2 * span : (s + 1) * 2 * span]
    place = cut(e.t * 2 + e.p, wide)
    for s in range(seqs):
        for k, gain in enumerate((qgain, kgain)):
            unit = lin[k, s] * scales[s][:, k : k + 1]
            units[k, s] = unit
            scaled = unit * gain[:, place]
            for jj in range(heads):
                turned = turn(scaled[:, jj * HD : (jj + 1) * HD], ang[0, s], ang[1, s])
                qkvx[k, s, jj] = turned.astype(BF)
            to_heads(e, qkvx.at[k, s], qkvh.at[k, s], hsend.at[k, s], hrecv.at[k, s], heads, span)

    ws[3].relay()
    ws[4].relay()

    def attend(s):
        for k in (2, 0, 1):
            wait_bytes(qkvh.at[k, s], hrecv.at[k, s])
        for i in range(e.nc):
            keys = (i + 1) * span
            kb = qkvh[1, s, 0 : i + 1].reshape(keys, HD)
            vb = qkvh[2, s, 0 : i + 1].reshape(keys, HD)
            scores = masked(dot(qkvh[0, s, i], kb, NT) * HD**-0.5, seg_col, seg_row, s, i, span)
            top = jnp.max(scores, axis=-1, keepdims=True)
            ex_s = jnp.exp(scores - top)
            total = jnp.sum(ex_s, axis=-1, keepdims=True)
            log_total = top + jnp.log(total)
            lse[s, i * span : (i + 1) * span, :] = jnp.broadcast_to(log_total, (span, HD))
            probs = (ex_s * (1.0 / total)).astype(BF)
            atth[s, i] = dot(probs, vb, NN).astype(BF)
        dst = att.at[s, own, cut(lax.rem(e.c, heads), HD)]
        from_heads(e, atth.at[s], dst, bsend.at[s], brecv.at[s], heads)

    loop(seqs, attend)
    for k, (a, b) in enumerate(((qkvh, qkv_heads), (atth, att_heads))):
        outs.append(pltpu.make_async_copy(a, b, osem.at[4 + k]))
        outs[-1].start()
    for s in range(seqs):
        wait_bytes(att.at[s], brecv.at[s])
        from_heads_drain(e, atth.at[s], bsend.at[s], heads)
        for k in range(3):
            to_heads_drain(e, qkvx.at[k, s], hsend.at[k, s], heads, span)
        gat[s].drain()
    angle_copy().wait_send()
    ws[3].wait()
    ws[4].wait()
    for w in ws:
        w.drain()
    for o in outs:
        o.wait()


def front_stage(
    sizes, tokens, cos_own, sin_own, qgain, kgain, seg_col, seg_row, wq, wk, wv, wo, gate
):
    nf, nc, nt = sizes
    seqs, rows, dm = tokens.shape
    wide = wq.shape[1] // 2
    heads = wide // HD
    full = 2 * nt * rows
    span = nt * rows
    sds = jax.ShapeDtypeStruct
    v, dma = pltpu.VMEM, pltpu.SemaphoreType.DMA
    return pl.pallas_call(
        functools.partial(front_kernel, sizes, seqs, rows),
        name="front_stage",
        out_shape=(
            sds((seqs, full, wide), BF),
            sds((seqs, full, dm), BF),
            sds((dm, wide), BF),
            sds((dm, wide), BF),
            sds((dm, wide), BF),
            sds((dm, wide), BF),
            sds((dm, gate.shape[1] // 8), BF),
            sds((2, seqs, full, wide), F32),
            sds((seqs, full, 128), F32),
            sds((2, seqs, full, HD), F32),
            sds((3, seqs, nc, span, HD), BF),
            sds((seqs, nc, span, HD), BF),
            sds((seqs, nc * span, HD), F32),
        ),
        in_specs=[VMEM_SPEC] * 7 + [HBM_SPEC] * 5,
        out_specs=(HBM_SPEC,) * 7 + (VMEM_SPEC,) * 3 + (HBM_SPEC,) * 2 + (VMEM_SPEC,),
        scratch_shapes=[
            v((seqs, full, dm), BF),
            v((dm, wide), BF),
            v((dm, wide), BF),
            v((dm, wide), BF),
            v((2, seqs, full, wide), F32),
            v((3, seqs, heads, full, HD), BF),
            v((3, seqs, nc, span, HD), BF),
            v((seqs, nc, span, HD), BF),
            v((8, seqs * full), F32),
            v((2 * nt, 8, seqs * full), F32),
            v((128, seqs * full), F32),
            v((2, seqs, full, HD), F32),
            dma((5, 4)),
            dma((seqs, 6, 2 * nt - 1)),
            dma((2,)),
            dma((2, 2 * nt)),
            dma((3, seqs, heads, 2)),
            dma((3, seqs)),
            dma((seqs, nc)),
            dma((seqs,)),
            dma((6,)),
        ],
        compiler_params=pltpu.CompilerParams(
            collective_id=2, has_side_effects=True, vmem_limit_bytes=60 << 20
        ),
    )(tokens, cos_own, sin_own, qgain, kgain, seg_col, seg_row, wq, wk, wv, wo, gate)


def tail_kernel(
    sizes, seqs, rows,
    hidden_grad, gains_in, units, scales, angles, qgain, kgain, seg_col, seg_row, lse,
    agh_in, qkv_heads, att_heads, xs_in, wq_in, wk_in, wv_in,
    wo_part, up_part,
    input_grad, gains_out, in_q, in_k, in_v, in_o, in_u,
    agh, qkvh, atth, x, wq, wk, wv, dh, dx, acck, accv, uu, pre, part, pair, right, left, y,
    mine, inbox, wide_t, gmine, gin, gin2, p_o, p_u, f_q, f_k, f_v, f_o, f_u,
    lsem, dsend, drecv, esem, rsem, ssem, g1sem, g2sem,
):
    e = Place(*sizes)
    n = e.nt
    span = n * rows
    dm = x.shape[2]
    wide = wq.shape[1]
    heads = wide // HD
    scat = [
        Scatter(e, p, fi, b, ssem.at[k])
        for k, (p, fi, b) in enumerate(
            (
                (wq, f_q, in_q), (wk, f_k, in_k), (wv, f_v, in_v),
                (p_o, f_o, in_o), (p_u, f_u, in_u),
            )
        )
    ]
    loads = [
        pltpu.make_async_copy(a, b, lsem.at[k])
        for k, (a, b) in enumerate(
            (
                (qkv_heads, qkvh), (agh_in, agh), (att_heads, atth), (wq_in, wq),
                (wk_in, wk), (wv_in, wv), (xs_in, x),
                (up_part, p_u), (wo_part, p_o),
            )
        )
    ]
    for ld in loads:
        ld.start()
    e.barrier()
    loads[8].wait()
    scat[3].start()
    wide_t[...] = jnp.zeros_like(wide_t)
    for ld in loads[:3]:
        ld.wait()

    def attend_back(s):
        acck[...] = jnp.zeros_like(acck)
        accv[...] = jnp.zeros_like(accv)
        for i in range(e.nc):
            keys = (i + 1) * span
            kb = qkvh[1, s, 0 : i + 1].reshape(keys, HD)
            vb = qkvh[2, s, 0 : i + 1].reshape(keys, HD)
            qb = qkvh[0, s, i]
            rowsl = pl.ds(i * span, span)
            scores = masked(dot(qb, kb, NT) * HD**-0.5, seg_col, seg_row, s, i, span)
            probs = jnp.exp(scores - lse[s, rowsl, 0:1])
            da = agh[s, i]
            accv[0:keys] += dot(probs.astype(BF), da, TN)
            delta = jnp.sum(da.astype(F32) * atth[s, i].astype(F32), axis=-1, keepdims=True)
            ds = (probs * (dot(da, vb, NT) - delta)).astype(BF)
            dh[0, s, i] = (dot(ds, kb, NN) * HD**-0.5).astype(BF)
            acck[0:keys] += dot(ds, qb, TN)
        dh[1, s] = (acck[...] * HD**-0.5).astype(BF).reshape(e.nc, span, HD)
        dh[2, s] = accv[...].astype(BF).reshape(e.nc, span, HD)
        own = pl.ds(pl.multiple_of(e.p * span, span), span)
        for k in range(3):
            dst = dx.at[k, s, lax.rem(e.c, heads), own, :]
            from_heads(e, dh.at[k, s], dst, dsend.at[k, s], drecv.at[k, s], heads)

    loop(seqs, attend_back)
    loads[7].wait()
    scat[4].start()
    scat[3].relay()

    place = cut(e.t * 2 + e.p, wide)
    gmine[...] = gains_in[...]
    gmine[0:2, :] = jnp.zeros((2, dm), F32)
    inner = [[], []]
    for s in range(seqs):
        for k in range(3):
            wait_bytes(dx.at[k, s], drecv.at[k, s])
        for k, gain in enumerate((qgain, kgain)):
            for jj in range(heads):
                lanes = slice(jj * HD, (jj + 1) * HD)
                g = turn_back(dx[k, s, jj].astype(F32), angles[0, s], angles[1, s])
                uu[k, s, :, lanes] = g
            g = uu[k, s]
            unit = units[k, s]
            gmine[k : k + 1, place] += jnp.sum(g * unit, axis=0, keepdims=True)
            u = g * gain[:, place]
            uu[k, s] = u
            inner[k].append(jnp.sum(u * unit, axis=-1, keepdims=True))
        for jj in range(heads):
            pre[2, s, :, jj * HD : (jj + 1) * HD] = dx[2, s, jj]
    mine[...] = columns(*[jnp.concatenate(v, axis=0) for v in inner])
    ex = Exchange(e, mine, inbox, esem.at[0], esem.at[1], *Exchange.heads(e))
    ex.start()
    gx = Exchange(e, gmine, gin, g1sem.at[0], g1sem.at[1], *Exchange.plane(e))
    gx.start()
    for ld in loads[3:7]:
        ld.wait()
    wide_t[0:8] = ex.finish() / D
    cols = wide_t[...].T
    for s in range(seqs):
        for k in range(2):
            mean = cols[s * 2 * span : (s + 1) * 2 * span, k : k + 1]
            v = scales[s][:, k : k + 1] * (uu[k, s] - units[k, s] * mean)
            pre[k, s] = v.astype(BF)

    tile = 512
    red = [
        Both(
            Reduce(
                e, part.at[s, :, cl], pair.at[s, :, cl], right.at[s, :, :, cl],
                left.at[s, :, :, cl], rsem.at[s, u], rows,
            )
            for u, cl in enumerate(parts_of(dm))
        )
        for s in range(seqs)
    ]
    for s in range(seqs):

        def step(i, s=s):
            sl = cut(i, tile)
            total = dot(pre[0, s], wq[sl, :], NT) + dot(pre[1, s], wk[sl, :], NT)
            part[s, :, sl] = (total + dot(pre[2, s], wv[sl, :], NT)).astype(BF)

        loop(dm // tile, step)
        red[s].pair_send()
    for s in range(seqs):
        red[s].pair_add()
        red[s].slot(-1)
    for k, w in enumerate((wq, wk, wv)):

        def step(i, k=k, w=w):
            sl = cut(i, tile)
            lhs = x[:, :, sl].reshape(-1, tile)
            w[sl, :] = dot(lhs, pre[k].reshape(-1, wide), TN).astype(BF)

        loop(dm // tile, step)
        scat[k].start()
    scat[4].relay()
    for j in range(n - 1):
        if j == n - 2:
            scat[0].relay()
            scat[1].relay()
        for s in range(seqs):
            red[s].slot(j)
    scat[2].relay()
    gmine[...] = gx.finish()
    gx2 = Exchange(e, gmine, gin2, g2sem.at[0], g2sem.at[1], *Exchange.line(e))
    gx2.start()
    for s in range(seqs):
        for r, cl in zip(red[s].each, parts_of(dm)):
            r.result(y.at[:, cl])
        input_grad[s] = hidden_grad[s] + y[...]
    gains_out[...] = gx2.finish()
    for sc in scat:
        sc.wait()
        sc.drain()
    for s in range(seqs):
        red[s].drain()
        for k in range(3):
            from_heads_drain(e, dh.at[k, s], dsend.at[k, s], heads)


def tail_stage(sizes, *args):
    nf, nc, nt = sizes
    hidden_grad, up_part, wo_part = args[0], args[18], args[17]
    seqs, rows, dm = hidden_grad.shape
    half, wide = up_part.shape[1], wo_part.shape[1]
    heads = wide // HD
    full = 2 * nt * rows
    span = nt * rows
    sds = jax.ShapeDtypeStruct
    v, dma = pltpu.VMEM, pltpu.SemaphoreType.DMA
    small, small_terms = scatter_shapes(sizes, dm, wide)
    large, large_terms = scatter_shapes(sizes, dm, half)
    return pl.pallas_call(
        functools.partial(tail_kernel, sizes, seqs, rows),
        name="tail_stage",
        out_shape=(sds((seqs, rows, dm), F32), sds((8, dm), F32))
        + (sds(small_terms, BF),) * 4
        + (sds(large_terms, BF),),
        in_specs=[VMEM_SPEC] * 10 + [HBM_SPEC] * 9,
        out_specs=(VMEM_SPEC,) * 2 + (HBM_SPEC,) * 5,
        scratch_shapes=[
            v((seqs, nc, span, HD), BF),
            v((3, seqs, nc, span, HD), BF),
            v((seqs, nc, span, HD), BF),
            v((seqs, full, dm), BF),
            v((dm, wide), BF),
            v((dm, wide), BF),
            v((dm, wide), BF),
            v((3, seqs, nc, span, HD), BF),
            v((3, seqs, heads, full, HD), BF),
            v((nc * span, HD), F32),
            v((nc * span, HD), F32),
            v((2, seqs, full, wide), F32),
            v((3, seqs, full, wide), BF),
            v((seqs, full, dm), BF),
            v((seqs, nt * rows, dm), BF),
            v((seqs, nt - 1, rows, dm), BF),
            v((seqs, nt - 1, rows, dm), BF),
            v((rows, dm), F32),
            v((8, seqs * full), F32),
            v((2 * nt, 8, seqs * full), F32),
            v((128, seqs * full), F32),
            v((8, dm), F32),
            v((nf * nc, 8, dm), F32),
            v((nt, 8, dm), F32),
            v((dm, wide), BF),
            v((dm, half), BF),
            v(small, BF),
            v(small, BF),
            v(small, BF),
            v(small, BF),
            v(large, BF),
            dma((9,)),
            dma((3, seqs, nc)),
            dma((3, seqs)),
            dma((2, 2 * nt)),
            dma((seqs, SPLIT, 4, nt)),
            dma((5, 4)),
            dma((2, nf * nc)),
            dma((2, nt)),
        ],
        compiler_params=pltpu.CompilerParams(
            collective_id=3, has_side_effects=True, vmem_limit_bytes=63 << 20
        ),
    )(*args)


def add_kernel(count, *refs):
    for src, dst in zip(refs[:count], refs[count:]):
        total = src[0].astype(F32)
        for i in range(1, src.shape[0]):
            total += src[i].astype(F32)
        dst[...] = total


def add_terms(terms):
    steps = 4

    def rows(x):
        return x.shape[1] // steps

    return pl.pallas_call(
        functools.partial(add_kernel, len(terms)),
        name="add_terms",
        grid=(steps,),
        out_shape=tuple(jax.ShapeDtypeStruct(x.shape[1:], F32) for x in terms),
        in_specs=[
            pl.BlockSpec((x.shape[0], rows(x), x.shape[2]), lambda i: (0, i, 0)) for x in terms
        ],
        out_specs=tuple(pl.BlockSpec((rows(x), x.shape[2]), lambda i: (i, 0)) for x in terms),
    )(*terms)


def body(
    tokens, segments, positions, query_weight, key_weight, value_weight, output_weight,
    gate_weight, up_projection_weight, down_weight, query_gain, key_gain, attention_gain,
    feedforward_gain, cotangent,
):
    sizes = (lax.axis_size("fsdp"), lax.axis_size("ctx"), lax.axis_size("tensor"))
    seqs, rows, _ = tokens.shape
    span = sizes[2] * rows
    block_pos = lax.dynamic_slice_in_dim(positions, lax.axis_index("ctx") * span, span, 1)
    cosine, sine = rope_tables(block_pos)
    cos_own = jnp.concatenate([cosine, cosine], axis=-1)
    sin_own = jnp.concatenate([-sine, sine], axis=-1)
    seg_col = segments[:, :, None]
    seg_row = segments[:, None, :]
    qgain, kgain = query_gain[None], key_gain[None]
    (
        att, xs, wq, wk, wv, wo, gate, units, scales, angles, qkv_heads, att_heads, lse,
    ) = front_stage(
        sizes, tokens, cos_own, sin_own, qgain, kgain, seg_col, seg_row,
        query_weight, key_weight, value_weight, output_weight, gate_weight,
    )
    block_out, hidden_grad, agh, wo_part, gate_terms, up_part, down_terms, gains = ffn_stage(
        sizes, att, wo, gate, gate_weight, up_projection_weight, down_weight,
        tokens, cotangent, attention_gain[None], feedforward_gain[None],
    )
    input_grad, gain_sums, *terms, up_terms = tail_stage(
        sizes, hidden_grad, gains, units, scales, angles, qgain, kgain, seg_col, seg_row, lse,
        agh, qkv_heads, att_heads, xs, wq, wk, wv, wo_part, up_part,
    )
    weight_grads = add_terms((*terms, gate_terms, up_terms, down_terms))
    return (block_out, input_grad, *weight_grads, *(gain_sums[k] for k in range(4)))


def solution(mesh):
    in_specs = (
        P("fsdp", ("ctx", "tensor"), None),
        P("fsdp", None),
        P("fsdp", None),
        P(("fsdp", "ctx"), "tensor"),
        P(("fsdp", "ctx"), "tensor"),
        P(("fsdp", "ctx"), "tensor"),
        P(("fsdp", "ctx"), "tensor"),
        P(("fsdp", "ctx"), "tensor"),
        P(("fsdp", "ctx"), "tensor"),
        P(("fsdp", "ctx"), "tensor"),
        P(),
        P(),
        P(),
        P(),
        P("fsdp", ("ctx", "tensor"), None),
    )
    out_specs = (
        P("fsdp", ("ctx", "tensor"), None),
        P("fsdp", ("ctx", "tensor"), None),
        P(("fsdp", "ctx"), "tensor"),
        P(("fsdp", "ctx"), "tensor"),
        P(("fsdp", "ctx"), "tensor"),
        P(("fsdp", "ctx"), "tensor"),
        P(("fsdp", "ctx"), "tensor"),
        P(("fsdp", "ctx"), "tensor"),
        P(("fsdp", "ctx"), "tensor"),
        P(),
        P(),
        P(),
        P(),
    )
    return jax.shard_map(body, mesh=mesh, in_specs=in_specs, out_specs=out_specs, check_vma=False)
```
